32 devices in a mesh: dp: 1 (over z), tp: 32 (over y, x, core).
Axes of the slice: x: 4, y: 4, z: 1, core: 2. Of those that a mesh axis runs over, the one named last changes fastest.
The devices are a block of a 4x4x8 slice.
Arguments:
- q_hidden: bfloat16 [512, 8, 4096], P(('dp', 'tp'))
- d_hidden: bfloat16 [64, 32, 4096], P(('dp', 'tp'))
- q_mask: int32 [512, 8], P(('dp', 'tp'))
- d_mask: int32 [64, 32], P(('dp', 'tp'))
- positive: int32 [512], P(('dp', 'tp'))
- w_head: bfloat16 [4096, 32768], P(None, 'tp')
- b_head: float32 [32768], P('tp')
Outputs:
- output 1: float32 [1], P('dp')
- output 2: bfloat16 [4096, 32768], P('dp', 'tp')
- output 3: float32 [32768], P(('dp', 'tp'))
- output 4: bfloat16 [512, 8, 4096], P(('dp', 'tp'))
- output 5: bfloat16 [64, 32, 4096], P(('dp', 'tp'))
All inputs are finite; a program needn't handle non-finite values.
Results may differ from the reference program's by a relative error of at most 0.0125692.
Values are sent between devices in bfloat16 or wider.
A program may use at most 768 MiB of HBM per device.

```python
import math
import jax
import jax.numpy as jnp
from jax import lax

BQ = 512
BD = 64
LQ = 8
LD = 32
D = 4096
V = 32768

TEMPERATURE = LQ * math.sqrt(V * LD) / 16.0
LAM_Q = 4.0 / (V * LQ * LQ)
LAM_D = 4.0 / (V * LD * LD)


def draw_mask(mask_key, n_rows, length):
    row_lens = jax.random.randint(mask_key, (n_rows,), length // 2, length + 1)
    row_lens = row_lens.at[0].set(length)
    return (jnp.arange(length)[None, :] < row_lens[:, None]).astype(jnp.int32)


def setup_inputs(seed: int = 0, part: int = 0) -> dict:
    base_key = jax.random.key(seed)
    shared_key, part_root = jax.random.split(base_key)
    part_key = jax.random.fold_in(part_root, part)
    part_keys = jax.random.split(part_key, 5)
    shared_keys = jax.random.split(shared_key, 2)
    q_hidden = jax.random.normal(part_keys[0], (BQ, LQ, D), jnp.float32).astype(jnp.bfloat16)
    d_hidden = jax.random.normal(part_keys[1], (BD, LD, D), jnp.float32).astype(jnp.bfloat16)
    q_mask = draw_mask(part_keys[2], BQ, LQ)
    d_mask = draw_mask(part_keys[3], BD, LD)
    positive = jax.random.randint(part_keys[4], (BQ,), 0, BD)
    positive = positive.at[0].set(0).at[BQ - 1].set(BD - 1)
    w_head = (jax.random.normal(shared_keys[0], (D, V), jnp.float32) * D ** -0.5).astype(jnp.bfloat16)
    b_head = 0.5 * jax.random.normal(shared_keys[1], (V,), jnp.float32) - 0.25
    return dict(q_hidden=q_hidden, d_hidden=d_hidden, q_mask=q_mask, d_mask=d_mask,
                positive=positive, w_head=w_head, b_head=b_head)


def head_rows(hidden, mask_arr, w_head, b_head):
    def one_row(row_in):
        hid_row, mask_row = row_in
        logits = jnp.dot(hid_row, w_head, preferred_element_type=jnp.float32) + b_head
        active = jnp.log1p(jnp.maximum(logits, 0.0)) * mask_row[:, None].astype(jnp.float32)
        return jnp.sum(active, axis=0)
    return lax.map(one_row, (hidden, mask_arr))


def head_grads(hidden, mask_arr, grad_rep, w_head, b_head, acc_init):
    def one_row(acc_pair, row_in):
        acc_w, acc_b = acc_pair
        hid_row, mask_row, grad_row = row_in
        logits = jnp.dot(hid_row, w_head, preferred_element_type=jnp.float32) + b_head
        relu_slope = jnp.where(logits > 0.0, 1.0 / (1.0 + jnp.maximum(logits, 0.0)), 0.0)
        grad_logits = grad_row[None, :] * relu_slope * mask_row[:, None].astype(jnp.float32)
        grad_low = grad_logits.astype(jnp.bfloat16)
        acc_w = acc_w + jnp.dot(hid_row.T, grad_low, preferred_element_type=jnp.float32)
        acc_b = acc_b + jnp.sum(grad_logits, axis=0)
        grad_hid = jnp.dot(grad_low, w_head.T, preferred_element_type=jnp.float32).astype(jnp.bfloat16)
        return (acc_w, acc_b), grad_hid
    return lax.scan(one_row, acc_init, (hidden, mask_arr, grad_rep))


def reference(q_hidden, d_hidden, q_mask, d_mask, positive, w_head, b_head):
    q_rep = head_rows(q_hidden, q_mask, w_head, b_head)
    d_rep = head_rows(d_hidden, d_mask, w_head, b_head)
    scores = jnp.dot(q_rep, d_rep.T, preferred_element_type=jnp.float32) / TEMPERATURE
    log_norm = jax.nn.logsumexp(scores, axis=1)
    target = (positive[:, None] == jnp.arange(BD)[None, :]).astype(jnp.float32)
    q_mean = jnp.mean(q_rep, axis=0)
    d_mean = jnp.mean(d_rep, axis=0)
    loss_val = (jnp.mean(log_norm - jnp.sum(scores * target, axis=1))
                + LAM_Q * jnp.sum(q_mean * q_mean) + LAM_D * jnp.sum(d_mean * d_mean))
    grad_scores = (jnp.exp(scores - log_norm[:, None]) - target) / (BQ * TEMPERATURE)
    grad_q = jnp.dot(grad_scores, d_rep, preferred_element_type=jnp.float32) + (2.0 * LAM_Q / BQ) * q_mean
    grad_d = jnp.dot(grad_scores.T, q_rep, preferred_element_type=jnp.float32) + (2.0 * LAM_D / BD) * d_mean
    acc_init = (jnp.zeros((D, V), jnp.float32), jnp.zeros((V,), jnp.float32))
    acc_mid, grad_qh = head_grads(q_hidden, q_mask, grad_q, w_head, b_head, acc_init)
    (acc_w, acc_b), grad_dh = head_grads(d_hidden, d_mask, grad_d, w_head, b_head, acc_mid)
    return jnp.reshape(loss_val, (1,)), acc_w.astype(jnp.bfloat16), acc_b, grad_qh, grad_dh
```

```python
import functools
import math

import jax
import jax.numpy as jnp
from jax import lax
from jax.experimental import pallas as pl
from jax.experimental.pallas import tpu as pltpu
from jax.sharding import PartitionSpec as P

MESH = pl.DeviceIdType.MESH
F32 = jnp.float32
BF16 = jnp.bfloat16
VMEM_LIMIT = 67043328
HIGHEST = lax.Precision.HIGHEST


class Geometry:
    def __init__(self, n_group, rows, hidden, vocab, unit):
        self.side = math.isqrt(n_group // 2)
        self.nd = 2 * (self.side.bit_length() - 1)
        self.chips = 1 << self.nd
        assert self.side == 4 and self.chips * 2 == n_group
        self.rows = rows
        self.steps = rows + self.nd
        self.unit = unit
        self.slab = 2 * unit
        self.tokens = self.slab * self.chips
        self.half = hidden // 2
        self.width = self.half // self.nd
        self.vocab = vocab

    def hops(self, rel):
        return bin(rel).count("1")

    def slot(self, rel, lane):
        return ((rel >> lane) | (rel << (self.nd - lane))) & (self.chips - 1)

    def peer(self, me, dim, core):
        chip = lax.div(me, 2)
        x, y = lax.rem(chip, self.side), lax.div(chip, self.side)
        if dim == 0:
            x = x + 1 - 2 * lax.rem(x, 2)
        elif dim == 1:
            x = self.side - 1 - x
        elif dim == 2:
            y = y + 1 - 2 * lax.rem(y, 2)
        else:
            y = self.side - 1 - y
        return {"tp": (y * self.side + x) * 2 + core}


def entry_barrier(peers):
    barrier = pltpu.get_barrier_semaphore()
    for device in peers:
        pl.semaphore_signal(barrier, inc=1, device_id=device, device_id_type=MESH)
    pl.semaphore_wait(barrier, len(peers))


class Gather:
    def __init__(self, geo, me, xo, xs, stage, ownx, sems):
        (self.ici_send, self.ici_recv, self.share_send, self.share_recv, self.piece_send, self.piece_recv,
         self.free_ici, self.free_piece, self.free_xs) = sems
        self.geo, self.xo, self.xs, self.stage, self.ownx = geo, xo, xs, stage, ownx
        self.core = lax.rem(me, 2)
        self.sib = {"tp": me + 1 - 2 * self.core}
        self.cross = [geo.peer(me, dim, 1 - self.core) for dim in range(geo.nd)]

    def ici(self, lane, pos):
        count = (1 << pos) * self.geo.slab
        return pltpu.make_async_remote_copy(
            src_ref=self.xs.at[lane, pl.ds(0, count)], dst_ref=self.xo.at[lane, pl.ds(count, count)],
            send_sem=self.ici_send.at[lane, pos], recv_sem=self.ici_recv.at[lane, pos],
            device_id=self.cross[(lane + pos) % self.geo.nd], device_id_type=MESH)

    def share(self, lane):
        return pltpu.make_async_remote_copy(
            src_ref=self.xo.at[lane], dst_ref=self.xs.at[lane],
            send_sem=self.share_send.at[lane], recv_sem=self.share_recv.at[lane],
            device_id=self.sib, device_id_type=MESH)

    def piece(self, lane, row):
        width = self.geo.width
        return pltpu.make_async_remote_copy(
            src_ref=self.ownx.at[1, row, :, pl.ds(lane * width, width)], dst_ref=self.stage.at[lane],
            send_sem=self.piece_send.at[lane], recv_sem=self.piece_recv.at[lane],
            device_id=self.sib, device_id_type=MESH)

    def arrive(self, s, lane):
        geo = self.geo
        width = geo.width

        @pl.when(s < geo.rows)
        def _():
            self.piece(lane, s).wait()
            mine = self.ownx[0, s, :, lane * width:(lane + 1) * width].astype(F32)
            theirs = self.stage[lane].astype(F32)
            first = jnp.where(self.core == 0, mine, theirs)
            second = jnp.where(self.core == 0, theirs, mine)
            self.xo[lane, 0:geo.slab, :] = jnp.concatenate([first, second], axis=0).astype(BF16)

        @pl.when(s > 0)
        def _():
            for pos in range(geo.nd):
                self.ici(lane, pos).wait_recv()
            pl.semaphore_wait(self.free_xs.at[lane], 1)

        self.share(lane).start()

    def release_own(self, s, lane):
        geo = self.geo
        self.share(lane).wait_send()

        @pl.when(s < geo.steps - 1)
        def _():
            for pos in range(geo.nd):
                pl.semaphore_signal(self.free_ici.at[lane, pos], inc=1,
                                    device_id=self.cross[(lane + pos) % geo.nd], device_id_type=MESH)

        @pl.when(s < geo.rows - 1)
        def _():
            pl.semaphore_signal(self.free_piece.at[lane], inc=1, device_id=self.sib, device_id_type=MESH)

    def forward(self, s, lane):
        geo = self.geo

        @pl.when(s < geo.rows - 1)
        def _():
            pl.semaphore_wait(self.free_piece.at[lane], 1)
            self.piece(lane, s + 1).start()

        @pl.when(s < geo.steps - 1)
        def _():
            for pos in reversed(range(geo.nd)):
                pl.semaphore_wait(self.free_ici.at[lane, pos], 1)
                self.ici(lane, pos).start()

    def release_sib(self, s, lane):
        geo = self.geo

        @pl.when(s < geo.steps - 1)
        def _():
            for pos in range(geo.nd):
                self.ici(lane, pos).wait_send()
            pl.semaphore_signal(self.free_xs.at[lane], inc=1, device_id=self.sib, device_id_type=MESH)

    def tokens_of(self, ref, lane):
        geo = self.geo
        if lane == 0:
            return ref[lane]
        places = [geo.slot(rel, lane) * geo.slab for rel in range(geo.chips)]
        return jnp.concatenate([ref[lane, at:at + geo.slab, :] for at in places], axis=0)


def gather_scratch(geo):
    nd = geo.nd
    lane = pltpu.VMEM((nd, geo.tokens, geo.width), BF16)
    bufs = [lane, lane, pltpu.VMEM((nd, geo.unit, geo.width), BF16),
            pltpu.VMEM((2, geo.rows, geo.unit, geo.half), BF16)]
    dma, reg = pltpu.SemaphoreType.DMA, pltpu.SemaphoreType.REGULAR
    sems = [dma((nd, nd)), dma((nd, nd)), dma((nd,)), dma((nd,)), dma((nd,)), dma((nd,)),
            reg((nd, nd)), reg((nd,)), reg((nd,))]
    return bufs, sems


def start_loads(geo, core, q_hbm, d_hbm, w_hbm, ownx, wv, own_sem, w_sem):
    n_q, n_d = q_hbm.shape[0], d_hbm.shape[0]
    own_loads, w_loads = [], []
    for plane in range(2):
        column = pl.multiple_of((core if plane == 0 else 1 - core) * geo.half, geo.half)
        own_loads.append(pltpu.make_async_copy(
            q_hbm.at[:, :, pl.ds(column, geo.half)], ownx.at[plane, pl.ds(0, n_q)], own_sem.at[2 * plane]))
        own_loads.append(pltpu.make_async_copy(
            d_hbm.at[:, :, pl.ds(column, geo.half)], ownx.at[plane, pl.ds(n_q, n_d)], own_sem.at[2 * plane + 1]))
        for lane in range(geo.nd):
            w_loads.append(pltpu.make_async_copy(
                w_hbm.at[pl.ds(pl.multiple_of(column + lane * geo.width, geo.width), geo.width), :],
                wv.at[plane, lane], w_sem.at[plane, lane]))
    for copy in own_loads + w_loads:
        copy.start()
    return own_loads, w_loads


def loss_kernel(geo, q_hbm, d_hbm, w_hbm, bias, mask, rep, xo, xs, stage, ownx, wv, z, own_sem, w_sem, *sems):
    me = lax.axis_index("tp")
    net = Gather(geo, me, xo, xs, stage, ownx, sems)
    own_loads, w_loads = start_loads(geo, net.core, q_hbm, d_hbm, w_hbm, ownx, wv, own_sem, w_sem)
    xo[...] = jnp.zeros_like(xo)
    entry_barrier([net.sib] + net.cross)
    for copy in own_loads:
        copy.wait()
    for lane in range(geo.nd):
        net.piece(lane, 0).start()
    for copy in w_loads:
        copy.wait()

    def own_part(s, lane):
        net.arrive(s, lane)
        part = jnp.dot(net.tokens_of(xo, lane), wv[0, lane], preferred_element_type=F32)
        par = lax.rem(s, 2)
        if lane == 0:
            z[par] = part
        else:
            z[par] = z[par] + part

    def sib_part(s, lane):
        net.release_own(s, lane)
        net.share(lane).wait_recv()
        par = lax.rem(s, 2)
        z[par] = z[par] + jnp.dot(net.tokens_of(xs, lane), wv[1, lane], preferred_element_type=F32)

    def reps(s):
        par = lax.rem(s, 2)
        for rel in range(geo.chips):
            logits = z[par, rel * geo.slab:(rel + 1) * geo.slab, :] + bias[...]
            active = jnp.log1p(jnp.maximum(logits, 0.0))
            row = s + geo.nd - geo.hops(rel)
            for core in range(2):
                at = 2 * rel + core
                part = active[core * geo.unit:(core + 1) * geo.unit, :] * mask[s, :, at:at + 1]
                rep[row, at:at + 1, :] = jnp.sum(part, axis=0, keepdims=True)

    def body(s, carry):
        for lane in range(geo.nd):
            @pl.when(s > 0)
            def _():
                net.release_sib(s - 1, lane)

            own_part(s, lane)
            if lane == 0:
                @pl.when(s > 0)
                def _():
                    reps(s - 1)
                    net.forward(s - 1, geo.nd - 1)
            else:
                net.forward(s, lane - 1)
            sib_part(s, lane)
        return carry

    lax.fori_loop(0, geo.steps, body, 0)
    reps(geo.steps - 1)


def grad_kernel(geo, q_hbm, d_hbm, w_hbm, bias, mask, drep, gw_hbm, gb, gh_hbm,
                xo, xs, stage, ownx, wv, wt, acc, z, dz, dzt, dho, sibout, sibin, dlo, dhi, m1, m2, m3,
                r1, r2, r3, r4, ost, gout, own_sem, w_sem, sd_send, sd_recv, rs_send, rs_recv, out_send, out_recv,
                wout_sem, hout_sem, *sems):
    nd, slab, unit, width, steps, rows = geo.nd, geo.slab, geo.unit, geo.width, geo.steps, geo.rows
    me = lax.axis_index("tp")
    net = Gather(geo, me, xo, xs, stage, ownx, sems)
    core = net.core
    same = [geo.peer(me, dim, core) for dim in range(nd)]
    own_loads, w_loads = start_loads(geo, core, q_hbm, d_hbm, w_hbm, ownx, wv, own_sem, w_sem)
    xo[...] = jnp.zeros_like(xo)
    entry_barrier([net.sib] + net.cross + same)
    for copy in own_loads:
        copy.wait()
    for lane in range(nd):
        net.piece(lane, 0).start()
    gb[...] = jnp.zeros_like(gb)
    for copy in w_loads:
        copy.wait()

    def prepare(k, carry):
        acc[k] = jnp.zeros(acc.shape[1:], F32)
        wt[k] = wv[lax.div(k, nd), lax.rem(k, nd)].T
        return carry

    lax.fori_loop(0, 2 * nd, prepare, 0)

    def sib_dh(lane):
        return pltpu.make_async_remote_copy(
            src_ref=sibout.at[lane], dst_ref=sibin.at[lane], send_sem=sd_send.at[lane], recv_sem=sd_recv.at[lane],
            device_id=net.sib, device_id_type=MESH)

    def rs_copy(stage_no, lane, s):
        parity, ring = lax.rem(s, 2), lax.rem(s, 3)
        n_low = geo.tokens >> stage_no
        src = dhi.at[lane]
        if stage_no > 1:
            src = (m1, m2, m3)[stage_no - 2].at[ring, lane, pl.ds(n_low, n_low)]
        dst = (r1, r2, r3, r4)[stage_no - 1].at[parity, lane]
        return pltpu.make_async_remote_copy(
            src_ref=src, dst_ref=dst, send_sem=rs_send.at[stage_no - 1, lane],
            recv_sem=rs_recv.at[stage_no - 1, lane, parity],
            device_id=same[(lane + nd - stage_no) % nd], device_id_type=MESH)

    def out_copy(s):
        parity = lax.rem(s, 2)
        return pltpu.make_async_remote_copy(
            src_ref=ost.at[parity], dst_ref=gout.at[1, s - 9], send_sem=out_send.at[parity],
            recv_sem=out_recv.at[parity], device_id=net.sib, device_id_type=MESH)

    def scatter(s):
        ring, back, prev = lax.rem(s, 3), lax.rem(s + 1, 3), lax.rem(s + 2, 3)
        was = lax.rem(s + 1, 2)
        low1, low2, low3, low4 = (geo.tokens >> k for k in range(1, 5))
        for lane in range(nd):
            cols = slice(lane * width, (lane + 1) * width)

            @pl.when((s >= 3) & (s <= steps + 1))
            def _():
                rs_copy(1, lane, s - 1).wait()
                m1[ring, lane] = (r1[was, lane].astype(F32) + dlo[ring, lane].astype(F32)).astype(BF16)

            @pl.when((s >= 5) & (s <= steps + 2))
            def _():
                rs_copy(2, lane, s - 1).wait()
                m2[ring, lane] = (r2[was, lane].astype(F32) + m1[back, lane, 0:low2].astype(F32)).astype(BF16)

            @pl.when((s >= 7) & (s <= steps + 3))
            def _():
                rs_copy(3, lane, s - 1).wait()
                m3[ring, lane] = (r3[was, lane].astype(F32) + m2[back, lane, 0:low3].astype(F32)).astype(BF16)

            @pl.when((s >= 9) & (s <= steps + 4))
            def _():
                rs_copy(4, lane, s - 1).wait()
                done = r4[was, lane].astype(F32) + m3[back, lane, 0:low4].astype(F32)
                first, second = done[0:unit], done[unit:slab]
                gout[0, s - 9, :, cols] = jnp.where(core == 0, first, second).astype(BF16)
                ost[lax.rem(s, 2), :, cols] = jnp.where(core == 0, second, first).astype(BF16)

            @pl.when((s >= 1) & (s <= steps))
            def _():
                sib_dh(lane).wait()
                both = dho[lane] + sibin[lane].astype(F32)
                dlo[prev, lane] = both[0:low1].astype(BF16)
                dhi[lane] = both[low1:].astype(BF16)

            @pl.when((s >= 2) & (s <= steps))
            def _():
                rs_copy(1, lane, s).start()

            @pl.when((s >= 4) & (s <= steps + 1))
            def _():
                rs_copy(2, lane, s).start()

            @pl.when((s >= 6) & (s <= steps + 2))
            def _():
                rs_copy(3, lane, s).start()

            @pl.when((s >= 8) & (s <= steps + 3))
            def _():
                rs_copy(4, lane, s).start()

        @pl.when((s >= 10) & (s <= steps + 4))
        def _():
            out_copy(s - 1).wait()

        @pl.when((s >= 9) & (s <= steps + 4))
        def _():
            out_copy(s).start()

    def logits_grad(s):
        total = gb[...]
        for rel in range(geo.chips):
            logits = z[rel * slab:(rel + 1) * slab, :] + bias[...]
            slope = jnp.where(logits > 0.0, 1.0 / (1.0 + jnp.maximum(logits, 0.0)), 0.0)
            row = s + nd - geo.hops(rel)
            parts = []
            for cr in range(2):
                at = 2 * rel + cr
                grad_row = drep[row, at:at + 1, :]
                part = grad_row * slope[cr * unit:(cr + 1) * unit, :] * mask[s, :, at:at + 1]
                total = total + part
                parts.append(part)
            dz[rel * slab:(rel + 1) * slab, :] = jnp.concatenate(parts, axis=0).astype(BF16)
        gb[...] = total
        dzt[...] = dz[...].T

    def compute(s):
        def sib_part(lane):
            net.share(lane).wait_recv()
            z[...] += jnp.dot(net.tokens_of(xs, lane), wv[1, lane], preferred_element_type=F32)

        for lane in range(nd):
            @pl.when(s > 0)
            def _():
                net.release_sib(s - 1, lane)

            net.arrive(s, lane)
            part = jnp.dot(net.tokens_of(xo, lane), wv[0, lane], preferred_element_type=F32)
            if lane == 0:
                z[...] = part
            else:
                z[...] += part
                sib_part(lane - 1)
        sib_part(nd - 1)
        logits_grad(s)
        for lane in range(nd):
            acc[lane] += jnp.dot(dzt[...], net.tokens_of(xo, lane), preferred_element_type=F32)
            net.release_own(s, lane)
        for lane in range(nd):
            acc[nd + lane] += jnp.dot(dzt[...], net.tokens_of(xs, lane), preferred_element_type=F32)
            if lane >= 1:
                net.forward(s, lane - 1)
        for lane in range(nd):
            part = jnp.dot(dz[...], wt[nd + lane], preferred_element_type=F32)
            for rel in range(geo.chips):
                at = geo.slot(rel, lane) * slab
                sibout[lane, at:at + slab, :] = part[rel * slab:(rel + 1) * slab, :].astype(BF16)
            sib_dh(lane).start()
            if lane == 0:
                net.forward(s, nd - 1)
        for lane in range(nd):
            part = jnp.dot(dz[...], wt[lane], preferred_element_type=F32)
            for rel in range(geo.chips):
                at = geo.slot(rel, lane) * slab
                dho[lane, at:at + slab, :] = part[rel * slab:(rel + 1) * slab, :]

    def wout(plane, lane):
        column = (core if plane == 0 else 1 - core) * geo.half + lane * width
        return pltpu.make_async_copy(
            wv.at[plane, lane], gw_hbm.at[pl.ds(pl.multiple_of(column, width), width), :], wout_sem.at[plane, lane])

    def body(s, carry):
        scatter(s)

        @pl.when(s < steps)
        def _():
            compute(s)

        for plane in range(2):
            for lane in range(nd):
                k = plane * nd + lane

                @pl.when(s == steps + k // 2)
                def _():
                    wv[plane, lane] = acc[k].astype(BF16).T
                    wout(plane, lane).start()
        return carry

    lax.fori_loop(0, steps + 5, body, 0)
    out_copy(steps + 4).wait()
    stores = []
    for plane in range(2):
        column = pl.multiple_of((core if plane == 0 else 1 - core) * geo.half, geo.half)
        stores.append(pltpu.make_async_copy(gout.at[plane], gh_hbm.at[:, :, pl.ds(column, geo.half)],
                                            hout_sem.at[plane]))
    for copy in stores:
        copy.start()
    for copy in stores:
        copy.wait()
    for plane in range(2):
        for lane in range(nd):
            wout(plane, lane).wait()


def call_loss(geo, q_rows, d_rows, w_head, bias, mask):
    bufs, sems = gather_scratch(geo)
    dma = pltpu.SemaphoreType.DMA
    hbm, vmem = pl.BlockSpec(memory_space=pl.ANY), pl.BlockSpec(memory_space=pltpu.VMEM)
    slots = 2 * geo.chips
    return pl.pallas_call(
        functools.partial(loss_kernel, geo),
        name="loss_pass",
        out_shape=jax.ShapeDtypeStruct((geo.steps + geo.nd, slots, geo.vocab), F32),
        in_specs=[hbm, hbm, hbm, vmem, vmem],
        out_specs=vmem,
        scratch_shapes=bufs + [pltpu.VMEM((2, geo.nd, geo.width, geo.vocab), BF16),
                               pltpu.VMEM((2, geo.tokens, geo.vocab), F32), dma((4,)), dma((2, geo.nd))] + sems,
        compiler_params=pltpu.CompilerParams(collective_id=0, has_side_effects=True, vmem_limit_bytes=VMEM_LIMIT),
    )(q_rows, d_rows, w_head, bias, mask)


def call_grad(geo, q_rows, d_rows, w_head, bias, mask, drep):
    bufs, sems = gather_scratch(geo)
    dma = pltpu.SemaphoreType.DMA
    nd, tok, width, vocab = geo.nd, geo.tokens, geo.width, geo.vocab
    hbm, vmem = pl.BlockSpec(memory_space=pl.ANY), pl.BlockSpec(memory_space=pltpu.VMEM)
    lane_b = functools.partial(pltpu.VMEM, dtype=BF16)
    scratch = bufs + [
        pltpu.VMEM((2, nd, width, vocab), BF16), pltpu.VMEM((2 * nd, vocab, width), BF16),
        pltpu.VMEM((2 * nd, vocab, width), F32), pltpu.VMEM((tok, vocab), F32), pltpu.VMEM((tok, vocab), BF16),
        pltpu.VMEM((vocab, tok), BF16), pltpu.VMEM((nd, tok, width), F32), pltpu.VMEM((nd, tok, width), BF16),
        pltpu.VMEM((nd, tok, width), BF16), pltpu.VMEM((3, nd, tok // 2, width), BF16),
        pltpu.VMEM((nd, tok // 2, width), BF16), pltpu.VMEM((3, nd, tok // 2, width), BF16),
        pltpu.VMEM((3, nd, tok // 4, width), BF16), pltpu.VMEM((3, nd, tok // 8, width), BF16),
        pltpu.VMEM((2, nd, tok // 2, width), BF16), pltpu.VMEM((2, nd, tok // 4, width), BF16),
        pltpu.VMEM((2, nd, tok // 8, width), BF16), pltpu.VMEM((2, nd, tok // 16, width), BF16),
        pltpu.VMEM((2, geo.unit, geo.half), BF16), pltpu.VMEM((2, geo.rows, geo.unit, geo.half), BF16),
        dma((4,)), dma((2, nd)), dma((nd,)), dma((nd,)), dma((4, nd)), dma((4, nd, 2)), dma((2,)), dma((2,)),
        dma((2, nd)), dma((2,))] + sems
    return pl.pallas_call(
        functools.partial(grad_kernel, geo),
        name="grad_pass",
        out_shape=[jax.ShapeDtypeStruct(w_head.shape, BF16), jax.ShapeDtypeStruct((geo.unit, vocab), F32),
                   jax.ShapeDtypeStruct((geo.rows, geo.unit, 2 * geo.half), BF16)],
        in_specs=[hbm, hbm, hbm, vmem, vmem, vmem],
        out_specs=[hbm, vmem, hbm],
        scratch_shapes=scratch,
        compiler_params=pltpu.CompilerParams(collective_id=1, has_side_effects=True, vmem_limit_bytes=VMEM_LIMIT),
    )(q_rows, d_rows, w_head, bias, mask, drep)


def solution(mesh):
    n_group = mesh.shape['tp']
    row_spec = P(('dp', 'tp'))
    mask_spec = P(('dp', 'tp'), None)
    hid_spec = P(('dp', 'tp'), None, None)
    contract_first = (((0,), (0,)), ((), ()))
    contract_last = (((1,), (1,)), ((), ()))

    def local_step(q_hidden, d_hidden, q_mask, d_mask, positive, w_head, b_head):
        hidden_size, vocab_loc = w_head.shape
        vocab_size = vocab_loc * n_group
        n_q, q_len, _ = q_hidden.shape
        n_d, d_len, _ = d_hidden.shape
        pieces = d_len // q_len
        q_batch, d_batch = n_q * n_group, n_d * n_group
        tau = q_len * math.sqrt(vocab_size * d_len) / 16.0
        lam_q = 4.0 / (vocab_size * q_len * q_len)
        lam_d = 4.0 / (vocab_size * d_len * d_len)
        rows = n_q + n_d * pieces
        geo = Geometry(n_group, rows, hidden_size, vocab_loc, q_len)
        nd, side, slots = geo.nd, geo.side, 2 * geo.chips

        me = lax.axis_index('tp')
        rel = jnp.arange(geo.chips)
        flip = jnp.array([0, 1, 3, 2])
        chip = me // 2
        chip_of = ((chip // side) ^ flip[rel // side]) * side + ((chip % side) ^ flip[rel % side])
        device_of = (chip_of[:, None] * 2 + jnp.arange(2)[None, :]).reshape((slots,))
        place = (device_of[:, None] == jnp.arange(n_group)[None, :]).astype(F32)
        hop_of = [geo.hops(s // 2) for s in range(slots)]

        unit_mask = jnp.concatenate([q_mask, d_mask.reshape((n_d * pieces, q_len))], axis=0)
        own_ints = jnp.concatenate([unit_mask, positive.reshape((-1, q_len))], axis=0)
        all_ints = lax.all_gather(own_ints, 'tp')
        all_mask = all_ints[:, :rows].astype(F32).reshape((n_group, rows * q_len))
        pos_all = all_ints[:, rows:].reshape((q_batch,))
        slot_mask = jnp.dot(place, all_mask, precision=HIGHEST).reshape((slots, rows, q_len))
        padded = jnp.pad(slot_mask, ((0, 0), (nd, nd), (0, 0)))
        hop_vec = jnp.array(hop_of)[:, None, None]
        skewed = jnp.zeros((slots, geo.steps, q_len), F32)
        for h in range(nd + 1):
            skewed = jnp.where(hop_vec == h, padded[:, nd - h:nd - h + geo.steps, :], skewed)
        mask = jnp.pad(jnp.transpose(skewed, (1, 2, 0)), ((0, 0), (0, 0), (0, 128 - slots)))

        bias = b_head.reshape((1, vocab_loc))
        d_units = d_hidden.reshape((n_d * pieces, q_len, hidden_size))
        rep = call_loss(geo, q_hidden, d_units, w_head, bias, mask)
        q_rep = rep[nd:nd + n_q].reshape((n_q * slots, vocab_loc))
        d_rep = jnp.sum(rep[nd + n_q:nd + rows].reshape((n_d, pieces, slots, vocab_loc)), axis=1)
        d_rep = d_rep.reshape((n_d * slots, vocab_loc))

        q_mean = jnp.mean(q_rep, axis=0)
        d_mean = jnp.mean(d_rep, axis=0)
        part = lax.dot_general(q_rep, d_rep, contract_last, precision=HIGHEST, preferred_element_type=F32)
        part = part.reshape((n_q, slots, n_d, slots))
        score_part = jnp.einsum('rjik,je,kf->erfi', part, place, place, precision=HIGHEST)
        score_part = score_part.reshape((q_batch, d_batch))
        reg_part = jnp.stack([jnp.sum(q_mean * q_mean), jnp.sum(d_mean * d_mean)])
        reg_part = jnp.pad(reg_part[None, :], ((0, 7), (0, d_batch - 2)))
        summed = lax.psum(jnp.concatenate([score_part, reg_part], axis=0), 'tp')
        scores, reg_sum = summed[:q_batch] / tau, summed[q_batch]
        target = (pos_all[:, None] == jnp.arange(d_batch)[None, :]).astype(F32)
        log_norm = jax.nn.logsumexp(scores, axis=1)
        loss_val = (jnp.mean(log_norm - jnp.sum(scores * target, axis=1))
                    + lam_q * reg_sum[0] + lam_d * reg_sum[1])
        grad_scores = (jnp.exp(scores - log_norm[:, None]) - target) / (q_batch * tau)
        grad_part = grad_scores.reshape((n_group, n_q, n_group, n_d))
        grad_part = jnp.einsum('erfi,je,kf->rjik', grad_part, place, place, precision=HIGHEST)
        grad_part = grad_part.reshape((n_q * slots, n_d * slots))
        grad_q = (jnp.dot(grad_part, d_rep, precision=HIGHEST, preferred_element_type=F32)
                  + (2.0 * lam_q / q_batch) * q_mean).reshape((n_q, slots, vocab_loc))
        grad_d = (lax.dot_general(grad_part, q_rep, contract_first, precision=HIGHEST, preferred_element_type=F32)
                  + (2.0 * lam_d / d_batch) * d_mean).reshape((n_d, 1, slots, vocab_loc))
        grad_d = jnp.broadcast_to(grad_d, (n_d, pieces, slots, vocab_loc)).reshape((n_d * pieces, slots, vocab_loc))
        blank = jnp.zeros((nd, slots, vocab_loc), F32)
        drep = jnp.concatenate([blank, grad_q, grad_d, blank], axis=0)

        grad_w, grad_b, grad_h = call_grad(geo, q_hidden, d_units, w_head, bias, mask, drep)
        return (jnp.reshape(loss_val, (1,)), grad_w, jnp.sum(grad_b, axis=0), grad_h[:n_q],
                grad_h[n_q:].reshape(d_hidden.shape))

    return jax.shard_map(local_step, mesh=mesh,
                         in_specs=(hid_spec, hid_spec, mask_spec, mask_spec, row_spec, P(None, 'tp'), P('tp')),
                         out_specs=(P('dp'), P('dp', 'tp'), row_spec, hid_spec, hid_spec),
                         check_vma=False)
```

```python
import functools
import math

import jax
import jax.numpy as jnp
import numpy as np
from jax import lax
from jax.experimental import pallas as pl
from jax.experimental.pallas import tpu as pltpu
from jax.sharding import PartitionSpec as P

MESH = pl.DeviceIdType.MESH
F32 = jnp.float32
BF16 = jnp.bfloat16
VMEM_LIMIT = 67043328
HIGHEST = lax.Precision.HIGHEST


class Geometry:
    def __init__(self, n_group, rows, hidden, vocab, unit):
        self.side = math.isqrt(n_group // 2)
        self.nd = 2 * (self.side.bit_length() - 1)
        self.chips = 1 << self.nd
        assert self.side == 4 and self.chips * 2 == n_group
        self.rows = rows
        self.first = self.nd + rows
        self.steps = self.first + rows
        self.unit = unit
        self.slab = 2 * unit
        self.tokens = self.slab * self.chips
        self.half = hidden // 2
        self.width = self.half // self.nd
        self.vocab = vocab

    def hops(self, rel):
        return bin(rel).count("1")

    def slot(self, rel, lane):
        return ((rel >> lane) | (rel << (self.nd - lane))) & (self.chips - 1)

    def device(self, me, rel, core):
        chip = lax.div(me, 2)
        x, y = lax.rem(chip, self.side), lax.div(chip, self.side)
        if rel & 1:
            x = x + 1 - 2 * lax.rem(x, 2)
        if rel & 2:
            x = self.side - 1 - x
        if rel & 4:
            y = y + 1 - 2 * lax.rem(y, 2)
        if rel & 8:
            y = self.side - 1 - y
        return {"tp": (y * self.side + x) * 2 + core}

    def peer(self, me, dim, core):
        return self.device(me, 1 << dim, core)


def entry_barrier(peers):
    barrier = pltpu.get_barrier_semaphore()
    for device in peers:
        pl.semaphore_signal(barrier, inc=1, device_id=device, device_id_type=MESH)
    pl.semaphore_wait(barrier, len(peers))


class Gather:
    def __init__(self, geo, me, xo, xs, stage, ownx, sems):
        (self.ici_send, self.ici_recv, self.share_send, self.share_recv, self.piece_send, self.piece_recv,
         self.free_ici, self.free_piece, self.free_xs) = sems
        self.geo, self.xo, self.xs, self.stage, self.ownx = geo, xo, xs, stage, ownx
        self.core = lax.rem(me, 2)
        self.sib = {"tp": me + 1 - 2 * self.core}
        self.cross = [geo.peer(me, dim, 1 - self.core) for dim in range(geo.nd)]

    def ici(self, lane, pos):
        count = (1 << pos) * self.geo.slab
        return pltpu.make_async_remote_copy(
            src_ref=self.xs.at[lane, pl.ds(0, count)], dst_ref=self.xo.at[lane, pl.ds(count, count)],
            send_sem=self.ici_send.at[lane, pos], recv_sem=self.ici_recv.at[lane, pos],
            device_id=self.cross[(lane + pos) % self.geo.nd], device_id_type=MESH)

    def share(self, lane):
        return pltpu.make_async_remote_copy(
            src_ref=self.xo.at[lane], dst_ref=self.xs.at[lane],
            send_sem=self.share_send.at[lane], recv_sem=self.share_recv.at[lane],
            device_id=self.sib, device_id_type=MESH)

    def piece(self, lane, row):
        width = self.geo.width
        return pltpu.make_async_remote_copy(
            src_ref=self.ownx.at[1, row, :, pl.ds(lane * width, width)], dst_ref=self.stage.at[lane],
            send_sem=self.piece_send.at[lane], recv_sem=self.piece_recv.at[lane],
            device_id=self.sib, device_id_type=MESH)

    def arrive(self, s, lane):
        geo = self.geo
        width = geo.width

        row = lax.rem(s, geo.rows)
        self.piece(lane, row).wait()
        mine = self.ownx[0, row, :, lane * width:(lane + 1) * width].astype(F32)
        theirs = self.stage[lane].astype(F32)
        first = jnp.where(self.core == 0, mine, theirs)
        second = jnp.where(self.core == 0, theirs, mine)
        self.xo[lane, 0:geo.slab, :] = jnp.concatenate([first, second], axis=0).astype(BF16)

        @pl.when(s > 0)
        def _():
            for pos in range(geo.nd):
                self.ici(lane, pos).wait_recv()
            pl.semaphore_wait(self.free_xs.at[lane], 1)

        self.share(lane).start()

    def release_own(self, s, lane):
        geo = self.geo
        self.share(lane).wait_send()

        @pl.when(s < geo.steps - 1)
        def _():
            for pos in range(geo.nd):
                pl.semaphore_signal(self.free_ici.at[lane, pos], inc=1,
                                    device_id=self.cross[(lane + pos) % geo.nd], device_id_type=MESH)
            pl.semaphore_signal(self.free_piece.at[lane], inc=1, device_id=self.sib, device_id_type=MESH)

    def forward(self, s, lane):
        geo = self.geo

        @pl.when(s < geo.steps - 1)
        def _():
            pl.semaphore_wait(self.free_piece.at[lane], 1)
            self.piece(lane, lax.rem(s + 1, geo.rows)).start()
            for pos in reversed(range(geo.nd)):
                pl.semaphore_wait(self.free_ici.at[lane, pos], 1)
                self.ici(lane, pos).start()

    def release_sib(self, s, lane):
        geo = self.geo

        @pl.when(s < geo.steps - 1)
        def _():
            for pos in range(geo.nd):
                self.ici(lane, pos).wait_send()
            pl.semaphore_signal(self.free_xs.at[lane], inc=1, device_id=self.sib, device_id_type=MESH)

    def tokens_of(self, ref, lane):
        geo = self.geo
        if lane == 0:
            return ref[lane]
        places = [geo.slot(rel, lane) * geo.slab for rel in range(geo.chips)]
        return jnp.concatenate([ref[lane, at:at + geo.slab, :] for at in places], axis=0)


def gather_scratch(geo):
    nd = geo.nd
    lane = pltpu.VMEM((nd, geo.tokens, geo.width), BF16)
    bufs = [lane, lane, pltpu.VMEM((nd, geo.unit, geo.width), BF16),
            pltpu.VMEM((2, geo.rows, geo.unit, geo.half), BF16)]
    dma, reg = pltpu.SemaphoreType.DMA, pltpu.SemaphoreType.REGULAR
    sems = [dma((nd, nd)), dma((nd, nd)), dma((nd,)), dma((nd,)), dma((nd,)), dma((nd,)),
            reg((nd, nd)), reg((nd,)), reg((nd,))]
    return bufs, sems


def start_loads(geo, core, q_hbm, d_hbm, w_hbm, ownx, wv, own_sem, w_sem):
    n_q, n_d = q_hbm.shape[0], d_hbm.shape[0]
    own_loads, w_loads = [], []
    for plane in range(2):
        column = pl.multiple_of((core if plane == 0 else 1 - core) * geo.half, geo.half)
        own_loads.append(pltpu.make_async_copy(
            q_hbm.at[:, :, pl.ds(column, geo.half)], ownx.at[plane, pl.ds(0, n_q)], own_sem.at[2 * plane]))
        own_loads.append(pltpu.make_async_copy(
            d_hbm.at[:, :, pl.ds(column, geo.half)], ownx.at[plane, pl.ds(n_q, n_d)], own_sem.at[2 * plane + 1]))
        for lane in range(geo.nd):
            w_loads.append(pltpu.make_async_copy(
                w_hbm.at[pl.ds(pl.multiple_of(column + lane * geo.width, geo.width), geo.width), :],
                wv.at[plane, lane], w_sem.at[plane, lane]))
    for copy in own_loads + w_loads:
        copy.start()
    return own_loads, w_loads


def all_peers(geo, me):
    core = lax.rem(me, 2)
    found = [(0, 1 - core, geo.device(me, 0, 1 - core))]
    for rel in range(1, geo.chips):
        for other in range(2):
            found.append((rel, other, geo.device(me, rel, other)))
    return found


def fused_kernel(geo, const, q_hbm, d_hbm, w_hbm, bias, mrow, pos_ref, place, doc_place, pick,
                 loss_ref, gw_hbm, gb, gh_hbm,
                 xo, xs, stage, ownx, wv, wt, acc, z, dz, dzt, dho, sibout, sibin, dlo, dhi, m1, m2, m3,
                 r1, r2, r3, r4, ost, gout, early, rep, rd, drd, mall, mt, sbuf, pall, gmine, gall,
                 own_sem, w_sem, sd_send, sd_recv, rs_send, rs_recv, out_send, out_recv,
                 wout_sem, hout_sem, ex_send, ex_recv, *sems):
    nd, slab, unit, width, steps, rows, first = (geo.nd, geo.slab, geo.unit, geo.width, geo.steps, geo.rows,
                                                 geo.first)
    n_q, n_d, lam_q, lam_d, tau, q_batch, d_batch = const
    slots = 2 * geo.chips
    me = lax.axis_index("tp")
    net = Gather(geo, me, xo, xs, stage, ownx, sems)
    core = net.core
    same = [geo.peer(me, dim, core) for dim in range(nd)]
    peers = all_peers(geo, me)
    own_loads, w_loads = start_loads(geo, core, q_hbm, d_hbm, w_hbm, ownx, wv, own_sem, w_sem)
    xo[...] = jnp.zeros_like(xo)
    entry_barrier([device for _, _, device in peers])
    for copy in own_loads:
        copy.wait()
    for lane in range(nd):
        net.piece(lane, 0).start()

    def broadcast(kind, src_of, dst):
        return [pltpu.make_async_remote_copy(
            src_ref=src_of(2 * rel + other), dst_ref=dst.at[2 * rel + core],
            send_sem=ex_send.at[kind, i], recv_sem=ex_recv.at[kind, 2 * rel + core], device_id=device,
            device_id_type=MESH) for i, (rel, other, device) in enumerate(peers)]

    def arrivals(kind, dst):
        return [pltpu.make_async_remote_copy(
            src_ref=dst.at[2 * rel + other], dst_ref=dst.at[2 * rel + other],
            send_sem=ex_send.at[kind, i], recv_sem=ex_recv.at[kind, 2 * rel + other], device_id=device,
            device_id_type=MESH) for i, (rel, other, device) in enumerate(peers)]

    masks_out = broadcast(0, lambda slot: mrow, mall)
    for copy in masks_out:
        copy.start()
    mall[core] = mrow[...]
    gb[...] = jnp.zeros_like(gb)
    for ref in (dlo, m1, m2, m3):
        ref[...] = jnp.zeros_like(ref)

    def sib_dh(lane):
        return pltpu.make_async_remote_copy(
            src_ref=sibout.at[lane], dst_ref=sibin.at[lane], send_sem=sd_send.at[lane], recv_sem=sd_recv.at[lane],
            device_id=net.sib, device_id_type=MESH)

    def rs_copy(stage_no, lane, s):
        parity, ring = lax.rem(s, 2), lax.rem(s, 3)
        n_low = geo.tokens >> stage_no
        src = dhi.at[lane]
        if stage_no > 1:
            src = (m1, m2, m3)[stage_no - 2].at[ring, lane, pl.ds(n_low, n_low)]
        dst = (r1, r2, r3, r4)[stage_no - 1].at[parity, lane]
        return pltpu.make_async_remote_copy(
            src_ref=src, dst_ref=dst, send_sem=rs_send.at[stage_no - 1, lane],
            recv_sem=rs_recv.at[stage_no - 1, lane, parity],
            device_id=same[(lane + nd - stage_no) % nd], device_id_type=MESH)

    def out_copy(s):
        parity = lax.rem(s, 2)
        return pltpu.make_async_remote_copy(
            src_ref=ost.at[parity], dst_ref=gout.at[1, lax.rem(s - 9, rows)], send_sem=out_send.at[parity],
            recv_sem=out_recv.at[parity], device_id=net.sib, device_id_type=MESH)

    def merge(stage_no, lane, s, last, low):
        @pl.when(s < last)
        def _():
            rs_copy(stage_no, lane, s - 1).wait()
        got = (r1, r2, r3, r4)[stage_no - 1][lax.rem(s + 1, 2), lane].astype(F32)
        return jnp.where(s < last, got, 0.0) + low.astype(F32)

    def scatter(s):
        ring, back, prev = lax.rem(s, 3), lax.rem(s + 1, 3), lax.rem(s + 2, 3)
        low1, low2, low3, low4 = (geo.tokens >> k for k in range(1, 5))
        for lane in range(nd):
            cols = slice(lane * width, (lane + 1) * width)

            @pl.when((s >= first + 2) & (s <= steps + 2))
            def _():
                m1[ring, lane] = merge(1, lane, s, steps + 2, dlo[ring, lane]).astype(BF16)

            @pl.when((s >= first + 3) & (s <= steps + 4))
            def _():
                m2[ring, lane] = merge(2, lane, s, steps + 4, m1[back, lane, 0:low2]).astype(BF16)

            @pl.when((s >= first + 4) & (s <= steps + 6))
            def _():
                m3[ring, lane] = merge(3, lane, s, steps + 6, m2[back, lane, 0:low3]).astype(BF16)

            @pl.when((s >= first + 5) & (s <= steps + 8))
            def _():
                done = merge(4, lane, s, steps + 8, m3[back, lane, 0:low4])
                kept = lax.rem(s - first - 5, nd)

                @pl.when(s < first + 9)
                def _():
                    early[kept, lane] = done

                @pl.when(s >= first + 9)
                def _():
                    total = done + jnp.where(s >= steps + 5, early[kept, lane], 0.0)
                    one, two = total[0:unit], total[unit:slab]
                    gout[0, lax.rem(s - 9, rows), :, cols] = jnp.where(core == 0, one, two).astype(BF16)
                    ost[lax.rem(s, 2), :, cols] = jnp.where(core == 0, two, one).astype(BF16)

            @pl.when((s > first) & (s <= steps))
            def _():
                sib_dh(lane).wait()
                both = dho[lane] + sibin[lane].astype(F32)
                dlo[prev, lane] = both[0:low1].astype(BF16)
                dhi[lane] = both[low1:].astype(BF16)
                rs_copy(1, lane, s).start()

            @pl.when((s >= first + 2) & (s <= steps + 2))
            def _():
                rs_copy(2, lane, s).start()

            @pl.when((s >= first + 3) & (s <= steps + 4))
            def _():
                rs_copy(3, lane, s).start()

            @pl.when((s >= first + 4) & (s <= steps + 6))
            def _():
                rs_copy(4, lane, s).start()

        @pl.when((s >= first + 10) & (s <= steps + 8))
        def _():
            out_copy(s - 1).wait()

        @pl.when((s >= first + 9) & (s <= steps + 8))
        def _():
            out_copy(s).start()

    def own_part(s, lane):
        net.arrive(s, lane)

        @pl.when(s >= nd)
        def _():
            part = jnp.dot(net.tokens_of(xo, lane), wv[0, lane], preferred_element_type=F32)
            par = lax.rem(s, 2)
            if lane == 0:
                z[par] = part
            else:
                z[par] = z[par] + part

    def sib_part(s, lane):
        net.release_own(s, lane)
        net.share(lane).wait_recv()

        @pl.when(s >= nd)
        def _():
            par = lax.rem(s, 2)
            z[par] = z[par] + jnp.dot(net.tokens_of(xs, lane), wv[1, lane], preferred_element_type=F32)

    def reps(s):
        par = lax.rem(s, 2)
        for rel in range(geo.chips):
            logits = z[par, rel * slab:(rel + 1) * slab, :] + bias[...]
            active = jnp.log1p(jnp.maximum(logits, 0.0))
            row = lax.rem(s - geo.hops(rel), rows)
            for cr in range(2):
                at = 2 * rel + cr
                part = active[cr * unit:(cr + 1) * unit, :] * mt[row, :, at:at + 1]
                rep[at, pl.ds(row, 1), :] = jnp.sum(part, axis=0, keepdims=True)

    def prepare(s):
        @pl.when(s == 1)
        def _():
            for copy in w_loads:
                copy.wait()
            for copy in arrivals(0, mall):
                copy.wait_recv()
            for copy in masks_out:
                copy.wait_send()
            table = jnp.concatenate([mall[i] for i in range(slots)], axis=0)
            table = jnp.concatenate([table, jnp.zeros((128 - slots, table.shape[1]), F32)], axis=0)
            mt[...] = table.T.reshape(mt.shape)

        @pl.when((s >= 1) & (s <= nd))
        def _():
            def turn(k, carry):
                acc[k] = jnp.zeros(acc.shape[1:], F32)
                wt[k] = wv[lax.div(k, nd), lax.rem(k, nd)].T
                return carry

            lax.fori_loop(2 * (s - 1), 2 * s, turn, 0)

    def loss_step(s, carry):
        prepare(s)
        for lane in range(nd):
            @pl.when(s > 0)
            def _():
                net.release_sib(s - 1, lane)

            own_part(s, lane)
            if lane == 0:
                @pl.when(s > 0)
                def _():
                    net.forward(s - 1, nd - 1)

                @pl.when(s > nd)
                def _():
                    reps(s - 1)
            else:
                net.forward(s, lane - 1)
            sib_part(s, lane)
        return carry

    def softmax():
        chunk = 8
        parts = slots // chunk
        pieces = rep[:, n_q:rows, :].reshape((slots * (rows - n_q), geo.vocab))
        rd[...] = jnp.dot(pick[...], pieces, precision=HIGHEST, preferred_element_type=F32)

        def score(c, q_sum):
            at = pl.ds(c * chunk, chunk)
            reps_c = rep[at, 0:n_q, :].reshape((chunk * n_q, geo.vocab))
            part = lax.dot_general(reps_c, rd[...], (((1,), (1,)), ((), ())), precision=HIGHEST,
                                   preferred_element_type=F32)
            part = jnp.dot(part, doc_place[...], precision=HIGHEST, preferred_element_type=F32)
            sbuf[at] = part.reshape((chunk, n_q, part.shape[1]))
            return q_sum + jnp.sum(reps_c, axis=0, keepdims=True)

        q_sum = lax.fori_loop(0, parts, score, jnp.zeros((1, geo.vocab), F32))
        scores_out = broadcast(1, lambda slot: sbuf.at[slot], pall)
        for copy in scores_out:
            copy.start()
        pall[core] = sbuf[core]
        q_mean = q_sum / q_batch
        d_mean = jnp.sum(rd[...], axis=0, keepdims=True) / d_batch
        reg = (lam_q * jnp.sum(q_mean * q_mean, axis=1, keepdims=True)
               + lam_d * jnp.sum(d_mean * d_mean, axis=1, keepdims=True))
        for copy in arrivals(1, pall):
            copy.wait_recv()
        total = pall[0]
        for i in range(1, slots):
            total = total + pall[i]
        scores = total / tau
        lane_no = lax.broadcasted_iota(jnp.int32, scores.shape, 1)
        target = lane_no == pos_ref[...]
        masked = jnp.where(lane_no < d_batch, scores, -jnp.inf)
        top = jnp.max(masked, axis=1, keepdims=True)
        log_norm = jnp.log(jnp.sum(jnp.exp(masked - top), axis=1, keepdims=True)) + top
        hit = jnp.sum(jnp.where(target, scores, 0.0), axis=1, keepdims=True)
        mine = jnp.sum(log_norm - hit, axis=0, keepdims=True) / q_batch + reg
        grad = (jnp.exp(masked - log_norm) - target.astype(F32)) / (q_batch * tau)
        gmine[0:n_q, :] = grad
        gmine[n_q:, :] = jnp.broadcast_to(mine, (gmine.shape[0] - n_q, grad.shape[1]))
        grads_out = broadcast(2, lambda slot: gmine, gall)
        for copy in grads_out:
            copy.start()
        gall[core] = gmine[...]
        drd[...] = jnp.broadcast_to((2.0 * lam_d / d_batch) * d_mean, drd.shape)
        for copy in arrivals(2, gall):
            copy.wait_recv()
        by_device = jnp.zeros((1, place.shape[1]), F32)
        for i in range(slots):
            by_device = by_device + gall[i, n_q:n_q + 1, :] * place[i:i + 1, :]
        loss_ref[...] = jnp.broadcast_to(jnp.sum(by_device, axis=1, keepdims=True), loss_ref.shape)

        def back(c, carry):
            at = pl.ds(c * chunk, chunk)
            grad_c = gall[at, 0:n_q, :].reshape((chunk * n_q, gall.shape[2]))
            grad_c = lax.dot_general(grad_c, doc_place[...], (((1,), (1,)), ((), ())), precision=HIGHEST,
                                     preferred_element_type=F32)
            reps_c = rep[at, 0:n_q, :].reshape((chunk * n_q, geo.vocab))
            drd[...] += lax.dot_general(grad_c, reps_c, (((0,), (0,)), ((), ())), precision=HIGHEST,
                                        preferred_element_type=F32)
            drq = jnp.dot(grad_c, rd[...], precision=HIGHEST, preferred_element_type=F32)
            drq = drq + (2.0 * lam_q / q_batch) * q_mean
            rep[at, 0:n_q, :] = drq.reshape((chunk, n_q, geo.vocab))
            return carry

        lax.fori_loop(0, parts, back, 0)
        spread = lax.dot_general(pick[...], drd[...], (((0,), (0,)), ((), ())), precision=HIGHEST,
                                 preferred_element_type=F32)
        rep[:, n_q:rows, :] = spread.reshape((slots, rows - n_q, geo.vocab))
        for copy in scores_out + grads_out:
            copy.wait_send()

    def logits_grad(s):
        total = gb[...]
        for rel in range(geo.chips):
            logits = z[0, rel * slab:(rel + 1) * slab, :] + bias[...]
            slope = jnp.where(logits > 0.0, 1.0 / (1.0 + jnp.maximum(logits, 0.0)), 0.0)
            row = lax.rem(s - geo.hops(rel), rows)
            parts = []
            for cr in range(2):
                at = 2 * rel + cr
                grad_row = rep[at, pl.ds(row, 1), :]
                part = grad_row * slope[cr * unit:(cr + 1) * unit, :] * mt[row, :, at:at + 1]
                total = total + part
                parts.append(part)
            dz[rel * slab:(rel + 1) * slab, :] = jnp.concatenate(parts, axis=0).astype(BF16)
        gb[...] = total
        dzt[...] = dz[...].T

    def grad_step(s):
        def sib_dot(lane):
            net.share(lane).wait_recv()
            z[0] += jnp.dot(net.tokens_of(xs, lane), wv[1, lane], preferred_element_type=F32)

        for lane in range(nd):
            net.release_sib(s - 1, lane)
            net.arrive(s, lane)
            part = jnp.dot(net.tokens_of(xo, lane), wv[0, lane], preferred_element_type=F32)
            if lane == 0:
                z[0] = part
            else:
                z[0] += part
                sib_dot(lane - 1)
        sib_dot(nd - 1)
        logits_grad(s)
        for lane in range(nd):
            acc[lane] += jnp.dot(dzt[...], net.tokens_of(xo, lane), preferred_element_type=F32)
            net.release_own(s, lane)
        for lane in range(nd):
            acc[nd + lane] += jnp.dot(dzt[...], net.tokens_of(xs, lane), preferred_element_type=F32)
            if lane >= 1:
                net.forward(s, lane - 1)
        for lane in range(nd):
            part = jnp.dot(dz[...], wt[nd + lane], preferred_element_type=F32)
            for rel in range(geo.chips):
                at = geo.slot(rel, lane) * slab
                sibout[lane, at:at + slab, :] = part[rel * slab:(rel + 1) * slab, :].astype(BF16)
            sib_dh(lane).start()
            if lane == 0:
                net.forward(s, nd - 1)
        for lane in range(nd):
            part = jnp.dot(dz[...], wt[lane], preferred_element_type=F32)
            for rel in range(geo.chips):
                at = geo.slot(rel, lane) * slab
                dho[lane, at:at + slab, :] = part[rel * slab:(rel + 1) * slab, :]

    def wout(k):
        plane, lane = lax.div(k, nd), lax.rem(k, nd)
        half_no = core + plane - 2 * core * plane
        column = half_no * geo.half + lane * width
        return pltpu.make_async_copy(
            wv.at[plane, lane], gw_hbm.at[pl.ds(pl.multiple_of(column, width), width), :], wout_sem.at[k])

    def body(s, carry):
        scatter(s)

        @pl.when(s < steps)
        def _():
            grad_step(s)

        @pl.when((s >= steps) & (s < steps + 2 * nd))
        def _():
            k = s - steps
            wv[lax.div(k, nd), lax.rem(k, nd)] = acc[k].astype(BF16).T
            wout(k).start()
        return carry

    lax.fori_loop(0, first, loss_step, 0)
    net.forward(first - 1, nd - 1)
    reps(first - 1)
    softmax()
    lax.fori_loop(first, steps + 9, body, 0)
    out_copy(steps + 8).wait()
    stores = []
    for plane in range(2):
        column = pl.multiple_of((core if plane == 0 else 1 - core) * geo.half, geo.half)
        stores.append(pltpu.make_async_copy(gout.at[plane], gh_hbm.at[:, :, pl.ds(column, geo.half)],
                                            hout_sem.at[plane]))
    for copy in stores:
        copy.start()
    for copy in stores:
        copy.wait()
    for k in range(2 * nd):
        wout(k).wait()


def call_fused(geo, const, q_rows, d_rows, w_head, bias, mrow, positive, place, doc_place, pick):
    bufs, sems = gather_scratch(geo)
    dma = pltpu.SemaphoreType.DMA
    nd, tok, width, vocab, rows = geo.nd, geo.tokens, geo.width, geo.vocab, geo.rows
    n_q, docs, slots = const[0], doc_place.shape[0], 2 * geo.chips
    lanes = doc_place.shape[1]
    tile = n_q + 8
    hbm, vmem = pl.BlockSpec(memory_space=pl.ANY), pl.BlockSpec(memory_space=pltpu.VMEM)
    scratch = bufs + [
        pltpu.VMEM((2, nd, width, vocab), BF16), pltpu.VMEM((2 * nd, vocab, width), BF16),
        pltpu.VMEM((2 * nd, vocab, width), F32), pltpu.VMEM((2, tok, vocab), F32), pltpu.VMEM((tok, vocab), BF16),
        pltpu.VMEM((vocab, tok), BF16), pltpu.VMEM((nd, tok, width), F32), pltpu.VMEM((nd, tok, width), BF16),
        pltpu.VMEM((nd, tok, width), BF16), pltpu.VMEM((3, nd, tok // 2, width), BF16),
        pltpu.VMEM((nd, tok // 2, width), BF16), pltpu.VMEM((3, nd, tok // 2, width), BF16),
        pltpu.VMEM((3, nd, tok // 4, width), BF16), pltpu.VMEM((3, nd, tok // 8, width), BF16),
        pltpu.VMEM((2, nd, tok // 2, width), BF16), pltpu.VMEM((2, nd, tok // 4, width), BF16),
        pltpu.VMEM((2, nd, tok // 8, width), BF16), pltpu.VMEM((2, nd, tok // 16, width), BF16),
        pltpu.VMEM((2, geo.unit, geo.half), BF16), pltpu.VMEM((2, rows, geo.unit, geo.half), BF16),
        pltpu.VMEM((nd, nd, geo.slab, width), F32),
        pltpu.VMEM((slots, rows, vocab), F32), pltpu.VMEM((docs, vocab), F32), pltpu.VMEM((docs, vocab), F32),
        pltpu.VMEM((slots,) + mrow.shape, F32), pltpu.VMEM((mrow.shape[1] // geo.unit, geo.unit, 128), F32),
        pltpu.VMEM((slots, n_q, lanes), F32), pltpu.VMEM((slots, n_q, lanes), F32),
        pltpu.VMEM((tile, lanes), F32), pltpu.VMEM((slots, tile, lanes), F32),
        dma((4,)), dma((2, nd)), dma((nd,)), dma((nd,)), dma((4, nd)), dma((4, nd, 2)), dma((2,)), dma((2,)),
        dma((2 * nd,)), dma((2,)), dma((3, slots)), dma((3, slots))] + sems
    return pl.pallas_call(
        functools.partial(fused_kernel, geo, const),
        name="lexical_head",
        out_shape=[jax.ShapeDtypeStruct((1, 128), F32), jax.ShapeDtypeStruct(w_head.shape, BF16),
                   jax.ShapeDtypeStruct((geo.unit, vocab), F32),
                   jax.ShapeDtypeStruct((rows, geo.unit, 2 * geo.half), BF16)],
        in_specs=[hbm, hbm, hbm] + [vmem] * 6,
        out_specs=[vmem, hbm, vmem, hbm],
        scratch_shapes=scratch,
        compiler_params=pltpu.CompilerParams(collective_id=0, has_side_effects=True, vmem_limit_bytes=VMEM_LIMIT),
    )(q_rows, d_rows, w_head, bias, mrow, positive, place, doc_place, pick)


def solution(mesh):
    n_group = mesh.shape['tp']
    row_spec = P(('dp', 'tp'))
    mask_spec = P(('dp', 'tp'), None)
    hid_spec = P(('dp', 'tp'), None, None)

    def local_step(q_hidden, d_hidden, q_mask, d_mask, positive, w_head, b_head):
        hidden_size, vocab_loc = w_head.shape
        vocab_size = vocab_loc * n_group
        n_q, q_len, _ = q_hidden.shape
        n_d, d_len, _ = d_hidden.shape
        pieces = d_len // q_len
        q_batch, d_batch = n_q * n_group, n_d * n_group
        tau = q_len * math.sqrt(vocab_size * d_len) / 16.0
        lam_q = 4.0 / (vocab_size * q_len * q_len)
        lam_d = 4.0 / (vocab_size * d_len * d_len)
        rows = n_q + n_d * pieces
        geo = Geometry(n_group, rows, hidden_size, vocab_loc, q_len)
        side, slots = geo.side, 2 * geo.chips
        lanes = max(128, d_batch)

        me = lax.axis_index('tp')
        slot = jnp.arange(slots)
        chip, rel = me // 2, slot // 2
        step_x, step_y = rel % side, rel // side
        chip_of = (((chip // side) ^ step_y ^ (step_y >> 1)) * side + ((chip % side) ^ step_x ^ (step_x >> 1)))
        device_of = chip_of * 2 + slot % 2
        place = (device_of[:, None] == jnp.arange(lanes)[None, :]).astype(F32)
        doc_of = (device_of[None, :] * n_d + jnp.arange(n_d)[:, None]).reshape((n_d * slots,))
        doc_place = (doc_of[:, None] == jnp.arange(lanes)[None, :]).astype(F32)
        doc_row = np.arange(n_d * slots)
        unit_row = np.arange(slots * n_d * pieces)
        pick = ((doc_row[:, None] % slots == unit_row[None, :] // (n_d * pieces))
                & (doc_row[:, None] // slots == unit_row[None, :] % (n_d * pieces) // pieces)).astype(np.float32)

        own_mask = jnp.concatenate([q_mask.reshape((-1,)), d_mask.reshape((-1,))]).astype(F32)
        mrow = jnp.pad(own_mask, (0, -own_mask.shape[0] % 128)).reshape((1, -1))
        const = (n_q, n_d, lam_q, lam_d, tau, float(q_batch), float(d_batch))
        loss, grad_w, grad_b, grad_h = call_fused(
            geo, const, q_hidden, d_hidden.reshape((n_d * pieces, q_len, hidden_size)), w_head,
            b_head.reshape((1, vocab_loc)), mrow, positive.reshape((n_q, 1)), place, doc_place, jnp.asarray(pick))
        return (loss[0, 0:1], grad_w, jnp.sum(grad_b, axis=0), grad_h[:n_q], grad_h[n_q:].reshape(d_hidden.shape))

    return jax.shard_map(local_step, mesh=mesh,
                         in_specs=(hid_spec, hid_spec, mask_spec, mask_spec, row_spec, P(None, 'tp'), P('tp')),
                         out_specs=(P('dp'), P('dp', 'tp'), row_spec, hid_spec, hid_spec),
                         check_vma=False)
```

```python
import functools
import math

import jax
import jax.numpy as jnp
import numpy as np
from jax import lax
from jax.experimental import pallas as pl
from jax.experimental.pallas import tpu as pltpu
from jax.sharding import PartitionSpec as P

MESH = pl.DeviceIdType.MESH
F32 = jnp.float32
BF16 = jnp.bfloat16
VMEM_LIMIT = 67043328
HIGHEST = lax.Precision.HIGHEST


class Geometry:
    def __init__(self, n_group, rows, hidden, vocab, unit):
        self.side = math.isqrt(n_group // 2)
        self.nd = 2 * (self.side.bit_length() - 1)
        self.chips = 1 << self.nd
        assert self.side == 4 and self.chips * 2 == n_group
        self.rows = rows
        self.first = self.nd + rows
        self.steps = self.first + rows
        self.unit = unit
        self.slab = 2 * unit
        self.tokens = self.slab * self.chips
        self.half = hidden // 2
        self.width = self.half // self.nd
        self.vocab = vocab

    def hops(self, rel):
        return bin(rel).count("1")

    def slot(self, rel, lane):
        return ((rel >> lane) | (rel << (self.nd - lane))) & (self.chips - 1)

    def device(self, me, rel, core):
        chip = lax.div(me, 2)
        x, y = lax.rem(chip, self.side), lax.div(chip, self.side)
        if rel & 1:
            x = x + 1 - 2 * lax.rem(x, 2)
        if rel & 2:
            x = self.side - 1 - x
        if rel & 4:
            y = y + 1 - 2 * lax.rem(y, 2)
        if rel & 8:
            y = self.side - 1 - y
        return {"tp": (y * self.side + x) * 2 + core}

    def peer(self, me, dim, core):
        return self.device(me, 1 << dim, core)


def entry_barrier(peers):
    barrier = pltpu.get_barrier_semaphore()
    for device in peers:
        pl.semaphore_signal(barrier, inc=1, device_id=device, device_id_type=MESH)
    pl.semaphore_wait(barrier, len(peers))


class Gather:
    def __init__(self, geo, me, x, stage, ownx, sems):
        (self.ici_send, self.ici_recv, self.piece_send, self.piece_recv, self.free_ici, self.free_piece) = sems
        self.geo, self.x, self.stage, self.ownx = geo, x, stage, ownx
        self.core = lax.rem(me, 2)
        self.sib = {"tp": me + 1 - 2 * self.core}
        self.same = [geo.peer(me, dim, self.core) for dim in range(geo.nd)]

    def ici(self, s, lane, pos):
        count = (1 << pos) * self.geo.slab
        here, there = lax.rem(s, 2), lax.rem(s + 1, 2)
        return pltpu.make_async_remote_copy(
            src_ref=self.x.at[here, lane, pl.ds(0, count)], dst_ref=self.x.at[there, lane, pl.ds(count, count)],
            send_sem=self.ici_send.at[lane, pos, there], recv_sem=self.ici_recv.at[lane, pos, there],
            device_id=self.same[(lane + pos) % self.geo.nd], device_id_type=MESH)

    def piece(self, s, lane):
        width, parity = self.geo.width, lax.rem(s, 2)
        return pltpu.make_async_remote_copy(
            src_ref=self.ownx.at[1, lax.rem(s, self.geo.rows), :, pl.ds(lane * width, width)],
            dst_ref=self.stage.at[parity, lane], send_sem=self.piece_send.at[lane, parity],
            recv_sem=self.piece_recv.at[lane, parity], device_id=self.sib, device_id_type=MESH)

    def arrive(self, s, lane):
        geo = self.geo
        width, parity = geo.width, lax.rem(s, 2)
        self.piece(s, lane).wait()
        mine = self.ownx[0, lax.rem(s, geo.rows), :, lane * width:(lane + 1) * width].astype(F32)
        theirs = self.stage[parity, lane].astype(F32)
        first = jnp.where(self.core == 0, mine, theirs)
        second = jnp.where(self.core == 0, theirs, mine)
        self.x[parity, lane, 0:geo.slab, :] = jnp.concatenate([first, second], axis=0).astype(BF16)

        @pl.when(s > 0)
        def _():
            for pos in range(geo.nd):
                self.ici(s - 1, lane, pos).wait_recv()

        @pl.when((s > 0) & (s < geo.steps - 1))
        def _():
            pl.semaphore_wait(self.free_piece.at[lane], 1)
            for pos in range(geo.nd):
                pl.semaphore_wait(self.free_ici.at[lane, pos], 1)

        @pl.when(s < geo.steps - 1)
        def _():
            for pos in reversed(range(geo.nd)):
                self.ici(s, lane, pos).start()
            self.piece(s + 1, lane).start()

    def release(self, s, lane):
        geo = self.geo

        @pl.when(s < geo.steps - 1)
        def _():
            for pos in range(geo.nd):
                self.ici(s, lane, pos).wait_send()

        @pl.when(s < geo.steps - 2)
        def _():
            for pos in range(geo.nd):
                pl.semaphore_signal(self.free_ici.at[lane, pos], inc=1,
                                    device_id=self.same[(lane + pos) % geo.nd], device_id_type=MESH)
            pl.semaphore_signal(self.free_piece.at[lane], inc=1, device_id=self.sib, device_id_type=MESH)

    def tokens(self, s, lane):
        geo, parity = self.geo, lax.rem(s, 2)
        if lane == 0:
            return self.x[parity, lane]
        places = [geo.slot(rel, lane) * geo.slab for rel in range(geo.chips)]
        return jnp.concatenate([self.x[parity, lane, at:at + geo.slab, :] for at in places], axis=0)


def gather_scratch(geo):
    nd = geo.nd
    bufs = [pltpu.VMEM((2, nd, geo.tokens, geo.width), BF16), pltpu.VMEM((2, nd, geo.unit, geo.width), BF16),
            pltpu.VMEM((2, geo.rows, geo.unit, geo.half), BF16)]
    dma, reg = pltpu.SemaphoreType.DMA, pltpu.SemaphoreType.REGULAR
    sems = [dma((nd, nd, 2)), dma((nd, nd, 2)), dma((nd, 2)), dma((nd, 2)), reg((nd, nd)), reg((nd,))]
    return bufs, sems


def all_peers(geo, me):
    core = lax.rem(me, 2)
    found = [(0, 1 - core, geo.device(me, 0, 1 - core))]
    for rel in range(1, geo.chips):
        for other in range(2):
            found.append((rel, other, geo.device(me, rel, other)))
    return found


def fused_kernel(geo, const, q_hbm, d_hbm, w_hbm, bias, mrow, pos_ref, place, doc_place, pick,
                 loss_ref, gw_hbm, gb, gh_hbm,
                 x, stage, ownx, wv, wt, acc, zo, zs, zr, dz, dzt, dlo, dhi, m1, m2, m3,
                 r1, r2, r3, r4, ost, gout, early, rep, rd, drd, mall, mt, sbuf, pall, gmine, gall,
                 own_sem, w_sem, wx_send, wx_recv, z_send, z_recv, dz_send, dz_recv, rs_send, rs_recv,
                 out_send, out_recv, wout_sem, wo_send, wo_recv, hout_sem, ex_send, ex_recv, *sems):
    nd, slab, unit, width, steps, rows, first = (geo.nd, geo.slab, geo.unit, geo.width, geo.steps, geo.rows,
                                                 geo.first)
    n_q, n_d, lam_q, lam_d, tau, q_batch, d_batch = const
    slots, vocab = 2 * geo.chips, geo.vocab
    me = lax.axis_index("tp")
    net = Gather(geo, me, x, stage, ownx, sems)
    core, same = net.core, net.same
    peers = all_peers(geo, me)
    half_at = [pl.multiple_of(core * geo.half, geo.half), pl.multiple_of((1 - core) * geo.half, geo.half)]

    n_dp = d_hbm.shape[0]
    own_loads = []
    for half in range(2):
        cols = pl.ds(half_at[half], geo.half)
        own_loads.append(pltpu.make_async_copy(q_hbm.at[:, :, cols], ownx.at[half, pl.ds(0, n_q)],
                                               own_sem.at[2 * half]))
        own_loads.append(pltpu.make_async_copy(d_hbm.at[:, :, cols], ownx.at[half, pl.ds(n_q, n_dp)],
                                               own_sem.at[2 * half + 1]))
    w_loads, w_cross = [], []
    for lane in range(nd):
        here = pl.ds(pl.multiple_of(half_at[0] + lane * width, width), width)
        there = pl.ds(pl.multiple_of(half_at[1] + lane * width, width), width)
        w_loads.append(pltpu.make_async_copy(w_hbm.at[here, :], wv.at[lane, :, pl.ds(0, vocab)], w_sem.at[lane]))
        w_cross.append(pltpu.make_async_remote_copy(
            src_ref=w_hbm.at[there, :], dst_ref=wv.at[lane, :, pl.ds(vocab, vocab)], send_sem=wx_send.at[lane],
            recv_sem=wx_recv.at[lane], device_id=net.sib, device_id_type=MESH))
    for copy in own_loads + w_loads:
        copy.start()
    x[...] = jnp.zeros_like(x)
    entry_barrier([device for _, _, device in peers])
    for copy in own_loads:
        copy.wait()
    for lane in range(nd):
        net.piece(0, lane).start()

    def broadcast(kind, src_of, dst):
        return [pltpu.make_async_remote_copy(
            src_ref=src_of(2 * rel + other), dst_ref=dst.at[2 * rel + core],
            send_sem=ex_send.at[kind, i], recv_sem=ex_recv.at[kind, 2 * rel + core], device_id=device,
            device_id_type=MESH) for i, (rel, other, device) in enumerate(peers)]

    def arrivals(kind, dst):
        return [pltpu.make_async_remote_copy(
            src_ref=dst.at[2 * rel + other], dst_ref=dst.at[2 * rel + other],
            send_sem=ex_send.at[kind, i], recv_sem=ex_recv.at[kind, 2 * rel + other], device_id=device,
            device_id_type=MESH) for i, (rel, other, device) in enumerate(peers)]

    masks_out = broadcast(0, lambda slot: mrow, mall)
    for copy in masks_out:
        copy.start()
    mall[core] = mrow[...]
    gb[...] = jnp.zeros_like(gb)
    for copy in w_cross:
        copy.start()
    for ref in (dlo, m1, m2, m3):
        ref[...] = jnp.zeros_like(ref)

    def z_copy(s):
        parity = lax.rem(s, 2)
        return pltpu.make_async_remote_copy(
            src_ref=zs.at[parity], dst_ref=zr.at[parity], send_sem=z_send.at[parity], recv_sem=z_recv.at[parity],
            device_id=net.sib, device_id_type=MESH)

    def dz_copies():
        return [pltpu.make_async_remote_copy(
            src_ref=dzt.at[pl.ds(0, vocab)], dst_ref=dzt.at[pl.ds(vocab, vocab)], send_sem=dz_send.at[0],
            recv_sem=dz_recv.at[0], device_id=net.sib, device_id_type=MESH),
            pltpu.make_async_remote_copy(
                src_ref=dz.at[:, pl.ds(0, vocab)], dst_ref=dz.at[:, pl.ds(vocab, vocab)], send_sem=dz_send.at[1],
                recv_sem=dz_recv.at[1], device_id=net.sib, device_id_type=MESH)]

    def rs_copy(stage_no, lane, s):
        parity, ring = lax.rem(s, 2), lax.rem(s, 3)
        n_low = geo.tokens >> stage_no
        src = dhi.at[lane]
        if stage_no > 1:
            src = (m1, m2, m3)[stage_no - 2].at[ring, lane, pl.ds(n_low, n_low)]
        dst = (r1, r2, r3, r4)[stage_no - 1].at[parity, lane]
        return pltpu.make_async_remote_copy(
            src_ref=src, dst_ref=dst, send_sem=rs_send.at[stage_no - 1, lane],
            recv_sem=rs_recv.at[stage_no - 1, lane, parity],
            device_id=same[(lane + nd - stage_no) % nd], device_id_type=MESH)

    def out_copy(s):
        parity = lax.rem(s, 2)
        return pltpu.make_async_remote_copy(
            src_ref=ost.at[parity], dst_ref=gout.at[1, lax.rem(s - 9, rows)], send_sem=out_send.at[parity],
            recv_sem=out_recv.at[parity], device_id=net.sib, device_id_type=MESH)

    def merge(stage_no, lane, s, last, low):
        @pl.when(s < last)
        def _():
            rs_copy(stage_no, lane, s - 1).wait()
        got = (r1, r2, r3, r4)[stage_no - 1][lax.rem(s + 1, 2), lane].astype(F32)
        return jnp.where(s < last, got, 0.0) + low.astype(F32)

    def scatter(s):
        ring, back = lax.rem(s, 3), lax.rem(s + 1, 3)
        low1, low2, low3, low4 = (geo.tokens >> k for k in range(1, 5))
        for lane in range(nd):
            cols = slice(lane * width, (lane + 1) * width)

            @pl.when((s >= first + 2) & (s <= steps + 2))
            def _():
                m1[ring, lane] = merge(1, lane, s, steps + 2, dlo[ring, lane]).astype(BF16)

            @pl.when((s >= first + 3) & (s <= steps + 4))
            def _():
                m2[ring, lane] = merge(2, lane, s, steps + 4, m1[back, lane, 0:low2]).astype(BF16)

            @pl.when((s >= first + 4) & (s <= steps + 6))
            def _():
                m3[ring, lane] = merge(3, lane, s, steps + 6, m2[back, lane, 0:low3]).astype(BF16)

            @pl.when((s >= first + 5) & (s <= steps + 8))
            def _():
                done = merge(4, lane, s, steps + 8, m3[back, lane, 0:low4])
                @pl.when(s < first + 9)
                def _():
                    early[lax.rem(s - first - 5, nd), lane] = done

                @pl.when(s >= first + 9)
                def _():
                    kept = lax.rem(s - first - 5 + nd - rows % nd, nd)
                    total = done + jnp.where(s >= steps + 5, early[kept, lane], 0.0)
                    one, two = total[0:unit], total[unit:slab]
                    gout[0, lax.rem(s - 9, rows), :, cols] = jnp.where(core == 0, one, two).astype(BF16)
                    ost[lax.rem(s, 2), :, cols] = jnp.where(core == 0, two, one).astype(BF16)

            @pl.when((s >= first + 2) & (s <= steps + 2))
            def _():
                rs_copy(2, lane, s).start()

            @pl.when((s >= first + 3) & (s <= steps + 4))
            def _():
                rs_copy(3, lane, s).start()

            @pl.when((s >= first + 4) & (s <= steps + 6))
            def _():
                rs_copy(4, lane, s).start()

        @pl.when((s >= first + 10) & (s <= steps + 8))
        def _():
            out_copy(s - 1).wait()

        @pl.when((s >= first + 9) & (s <= steps + 8))
        def _():
            out_copy(s).start()

    def logits_part(s, lane):
        parity = lax.rem(s, 2)
        tokens = net.tokens(s, lane)
        for ref, at in ((zs, vocab), (zo, 0)):
            part = jnp.dot(tokens, wv[lane, :, at:at + vocab], preferred_element_type=F32)
            if lane == 0:
                ref[parity] = part
            else:
                ref[parity] = ref[parity] + part

    def reps(s):
        parity = lax.rem(s, 2)
        z_copy(s).wait()
        for rel in range(geo.chips):
            span = slice(rel * slab, (rel + 1) * slab)
            logits = zo[parity, span, :] + zr[parity, span, :] + bias[...]
            active = jnp.log1p(jnp.maximum(logits, 0.0))
            row = lax.rem(s - geo.hops(rel), rows)
            for cr in range(2):
                at = 2 * rel + cr
                part = active[cr * unit:(cr + 1) * unit, :] * mt[row, :, at:at + 1]
                rep[at, pl.ds(row, 1), :] = jnp.sum(part, axis=0, keepdims=True)

    def prepare(s):
        @pl.when(s == 1)
        def _():
            for copy in w_loads:
                copy.wait()
            for copy in arrivals(0, mall):
                copy.wait_recv()
            for copy in masks_out:
                copy.wait_send()
            table = jnp.concatenate([mall[i] for i in range(slots)], axis=0)
            table = jnp.concatenate([table, jnp.zeros((128 - slots, table.shape[1]), F32)], axis=0)
            mt[...] = table.T.reshape(mt.shape)

        @pl.when(s == 2)
        def _():
            for copy in w_cross:
                copy.wait()

        @pl.when((s >= 2) & (s < 2 + nd))
        def _():
            def turn(part, carry):
                span = pl.ds(pl.multiple_of(part * vocab, vocab), vocab)
                acc[s - 2, span, :] = jnp.zeros((vocab, width), F32)
                wt[s - 2, span, :] = wv[s - 2, :, span].T
                return carry

            lax.fori_loop(0, 2, turn, 0)

    def loss_step(s, carry):
        prepare(s)
        for lane in range(nd):
            net.arrive(s, lane)

            @pl.when(s >= nd)
            def _():
                logits_part(s, lane)

            if lane >= 2:
                net.release(s, lane - 2)
            else:
                @pl.when(s > 0)
                def _():
                    net.release(s - 1, lane + nd - 2)
            if lane == 1:
                @pl.when(s > nd)
                def _():
                    reps(s - 1)

        @pl.when(s >= nd)
        def _():
            z_copy(s).start()
        return carry

    def softmax():
        chunk = 8
        parts = slots // chunk
        pieces = rep[:, n_q:rows, :].reshape((slots * (rows - n_q), geo.vocab))
        rd[...] = jnp.dot(pick[...], pieces, precision=HIGHEST, preferred_element_type=F32)

        def score(c, q_sum):
            at = pl.ds(c * chunk, chunk)
            reps_c = rep[at, 0:n_q, :].reshape((chunk * n_q, geo.vocab))
            part = lax.dot_general(reps_c, rd[...], (((1,), (1,)), ((), ())), precision=HIGHEST,
                                   preferred_element_type=F32)
            part = jnp.dot(part, doc_place[...], precision=HIGHEST, preferred_element_type=F32)
            sbuf[at] = part.reshape((chunk, n_q, part.shape[1]))
            return q_sum + jnp.sum(reps_c, axis=0, keepdims=True)

        q_sum = lax.fori_loop(0, parts, score, jnp.zeros((1, geo.vocab), F32))
        scores_out = broadcast(1, lambda slot: sbuf.at[slot], pall)
        for copy in scores_out:
            copy.start()
        pall[core] = sbuf[core]
        q_mean = q_sum / q_batch
        d_mean = jnp.sum(rd[...], axis=0, keepdims=True) / d_batch
        reg = (lam_q * jnp.sum(q_mean * q_mean, axis=1, keepdims=True)
               + lam_d * jnp.sum(d_mean * d_mean, axis=1, keepdims=True))
        for copy in arrivals(1, pall):
            copy.wait_recv()
        total = pall[0]
        for i in range(1, slots):
            total = total + pall[i]
        scores = total / tau
        lane_no = lax.broadcasted_iota(jnp.int32, scores.shape, 1)
        target = lane_no == pos_ref[...]
        masked = jnp.where(lane_no < d_batch, scores, -jnp.inf)
        top = jnp.max(masked, axis=1, keepdims=True)
        log_norm = jnp.log(jnp.sum(jnp.exp(masked - top), axis=1, keepdims=True)) + top
        hit = jnp.sum(jnp.where(target, scores, 0.0), axis=1, keepdims=True)
        mine = jnp.sum(log_norm - hit, axis=0, keepdims=True) / q_batch + reg
        grad = (jnp.exp(masked - log_norm) - target.astype(F32)) / (q_batch * tau)
        gmine[0:n_q, :] = grad
        gmine[n_q:, :] = jnp.broadcast_to(mine, (gmine.shape[0] - n_q, grad.shape[1]))
        grads_out = broadcast(2, lambda slot: gmine, gall)
        for copy in grads_out:
            copy.start()
        gall[core] = gmine[...]
        drd[...] = jnp.broadcast_to((2.0 * lam_d / d_batch) * d_mean, drd.shape)
        for copy in arrivals(2, gall):
            copy.wait_recv()
        by_device = jnp.zeros((1, place.shape[1]), F32)
        for i in range(slots):
            by_device = by_device + gall[i, n_q:n_q + 1, :] * place[i:i + 1, :]
        loss_ref[...] = jnp.broadcast_to(jnp.sum(by_device, axis=1, keepdims=True), loss_ref.shape)

        def back(c, carry):
            at = pl.ds(c * chunk, chunk)
            grad_c = gall[at, 0:n_q, :].reshape((chunk * n_q, gall.shape[2]))
            grad_c = lax.dot_general(grad_c, doc_place[...], (((1,), (1,)), ((), ())), precision=HIGHEST,
                                     preferred_element_type=F32)
            reps_c = rep[at, 0:n_q, :].reshape((chunk * n_q, geo.vocab))
            drd[...] += lax.dot_general(grad_c, reps_c, (((0,), (0,)), ((), ())), precision=HIGHEST,
                                        preferred_element_type=F32)
            drq = jnp.dot(grad_c, rd[...], precision=HIGHEST, preferred_element_type=F32)
            drq = drq + (2.0 * lam_q / q_batch) * q_mean
            rep[at, 0:n_q, :] = drq.reshape((chunk, n_q, geo.vocab))
            return carry

        lax.fori_loop(0, parts, back, 0)
        spread = lax.dot_general(pick[...], drd[...], (((0,), (0,)), ((), ())), precision=HIGHEST,
                                 preferred_element_type=F32)
        rep[:, n_q:rows, :] = spread.reshape((slots, rows - n_q, geo.vocab))
        for copy in scores_out + grads_out:
            copy.wait_send()

    def logits_grad(s):
        parity = lax.rem(s, 2)
        z_copy(s).wait()
        total = gb[...]
        for rel in range(geo.chips):
            span = slice(rel * slab, (rel + 1) * slab)
            logits = zo[parity, span, :] + zr[parity, span, :] + bias[...]
            inverse = 1.0 / (1.0 + logits)
            row = lax.rem(s - geo.hops(rel), rows)
            parts = []
            for cr in range(2):
                at = 2 * rel + cr
                part = slice(cr * unit, (cr + 1) * unit)
                grad_row = rep[at, pl.ds(row, 1), :] * inverse[part, :]
                grad_row = jnp.where(logits[part, :] > 0.0, grad_row, 0.0) * mt[row, :, at:at + 1]
                total = total + grad_row
                parts.append(grad_row)
            dz[span, 0:vocab] = jnp.concatenate(parts, axis=0).astype(BF16)
        gb[...] = total
        dzt[0:vocab, :] = dz[:, 0:vocab].T

    def grad_step(s, carry):
        for lane in range(nd):
            net.arrive(s, lane)
            logits_part(s, lane)
        z_copy(s).start()
        scatter(s + 1)
        logits_grad(s)
        copies = dz_copies()
        for copy in copies:
            copy.start()
        for lane in range(nd):
            acc[lane, 0:vocab, :] += jnp.dot(dzt[0:vocab, :], net.tokens(s, lane), preferred_element_type=F32)
        for copy in copies:
            copy.wait()
        for lane in range(nd):
            acc[lane, vocab:, :] += jnp.dot(dzt[vocab:, :], net.tokens(s, lane), preferred_element_type=F32)
        ring = lax.rem(s, 3)
        for lane in range(nd):
            part = jnp.dot(dz[...], wt[lane], preferred_element_type=F32)
            for rel in range(geo.chips):
                at = geo.slot(rel, lane) * slab
                block = part[rel * slab:(rel + 1) * slab, :].astype(BF16)
                if at < geo.tokens // 2:
                    dlo[ring, lane, at:at + slab, :] = block
                else:
                    dhi[lane, at - geo.tokens // 2:at - geo.tokens // 2 + slab, :] = block
            rs_copy(1, lane, s + 1).start()
            if lane >= 2:
                net.release(s, 2 * lane - 4)
                net.release(s, 2 * lane - 3)
        return carry

    def wout(lane):
        return pltpu.make_async_copy(
            wv.at[lane, :, pl.ds(0, vocab)],
            gw_hbm.at[pl.ds(pl.multiple_of(half_at[0] + lane * width, width), width), :], wout_sem.at[lane])

    def wout_cross(lane):
        return pltpu.make_async_remote_copy(
            src_ref=wv.at[lane, :, pl.ds(vocab, vocab)],
            dst_ref=gw_hbm.at[pl.ds(pl.multiple_of(half_at[0] + lane * width, width), width), :],
            send_sem=wo_send.at[lane], recv_sem=wo_recv.at[lane], device_id=net.sib, device_id_type=MESH)

    def tail_step(s, carry):
        scatter(s)

        @pl.when(s <= steps + nd)
        def _():
            lane = s - steps - 1
            for part in range(2):
                span = slice(part * vocab, (part + 1) * vocab)
                wv[lane, :, span] = acc[lane, span, :].astype(BF16).T
            wout(lane).start()
            wout_cross(lane).start()
        return carry

    lax.fori_loop(0, first, loss_step, 0)
    for lane in range(2, nd):
        net.release(first - 1, lane)
    reps(first - 1)
    softmax()
    lax.fori_loop(first, steps, grad_step, 0)
    lax.fori_loop(steps + 1, steps + 9, tail_step, 0)
    out_copy(steps + 8).wait()
    stores = [pltpu.make_async_copy(gout.at[half], gh_hbm.at[:, :, pl.ds(half_at[half], geo.half)], hout_sem.at[half])
              for half in range(2)]
    for copy in stores:
        copy.start()
    for copy in stores:
        copy.wait()
    for lane in range(nd):
        wout(lane).wait()
        wout_cross(lane).wait()


def call_fused(geo, const, q_rows, d_rows, w_head, bias, mrow, positive, place, doc_place, pick):
    bufs, sems = gather_scratch(geo)
    dma = pltpu.SemaphoreType.DMA
    nd, tok, width, vocab, rows = geo.nd, geo.tokens, geo.width, geo.vocab, geo.rows
    n_q, docs, slots = const[0], doc_place.shape[0], 2 * geo.chips
    lanes = doc_place.shape[1]
    tile = n_q + 8
    hbm, vmem = pl.BlockSpec(memory_space=pl.ANY), pl.BlockSpec(memory_space=pltpu.VMEM)
    logit = pltpu.VMEM((2, tok, vocab), F32)
    scratch = bufs + [
        pltpu.VMEM((nd, width, 2 * vocab), BF16), pltpu.VMEM((nd, 2 * vocab, width), BF16),
        pltpu.VMEM((nd, 2 * vocab, width), F32), logit, logit, logit,
        pltpu.VMEM((tok, 2 * vocab), BF16), pltpu.VMEM((2 * vocab, tok), BF16),
        pltpu.VMEM((3, nd, tok // 2, width), BF16), pltpu.VMEM((nd, tok // 2, width), BF16),
        pltpu.VMEM((3, nd, tok // 2, width), BF16), pltpu.VMEM((3, nd, tok // 4, width), BF16),
        pltpu.VMEM((3, nd, tok // 8, width), BF16),
        pltpu.VMEM((2, nd, tok // 2, width), BF16), pltpu.VMEM((2, nd, tok // 4, width), BF16),
        pltpu.VMEM((2, nd, tok // 8, width), BF16), pltpu.VMEM((2, nd, tok // 16, width), BF16),
        pltpu.VMEM((2, geo.unit, geo.half), BF16), pltpu.VMEM((2, rows, geo.unit, geo.half), BF16),
        pltpu.VMEM((nd, nd, geo.slab, width), F32),
        pltpu.VMEM((slots, rows, vocab), F32), pltpu.VMEM((docs, vocab), F32), pltpu.VMEM((docs, vocab), F32),
        pltpu.VMEM((slots,) + mrow.shape, F32), pltpu.VMEM((mrow.shape[1] // geo.unit, geo.unit, 128), F32),
        pltpu.VMEM((slots, n_q, lanes), F32), pltpu.VMEM((slots, n_q, lanes), F32),
        pltpu.VMEM((tile, lanes), F32), pltpu.VMEM((slots, tile, lanes), F32),
        dma((4,)), dma((nd,)), dma((nd,)), dma((nd,)), dma((2,)), dma((2,)), dma((2,)), dma((2,)),
        dma((4, nd)), dma((4, nd, 2)), dma((2,)), dma((2,)), dma((nd,)), dma((nd,)), dma((nd,)), dma((2,)),
        dma((3, slots)), dma((3, slots))] + sems
    return pl.pallas_call(
        functools.partial(fused_kernel, geo, const),
        name="lexical_head",
        out_shape=[jax.ShapeDtypeStruct((1, 128), F32), jax.ShapeDtypeStruct(w_head.shape, BF16),
                   jax.ShapeDtypeStruct((geo.unit, vocab), F32),
                   jax.ShapeDtypeStruct((rows, geo.unit, 2 * geo.half), BF16)],
        in_specs=[hbm, hbm, hbm] + [vmem] * 6,
        out_specs=[vmem, hbm, vmem, hbm],
        scratch_shapes=scratch,
        compiler_params=pltpu.CompilerParams(collective_id=0, has_side_effects=True, vmem_limit_bytes=VMEM_LIMIT),
    )(q_rows, d_rows, w_head, bias, mrow, positive, place, doc_place, pick)


def solution(mesh):
    n_group = mesh.shape['tp']
    row_spec = P(('dp', 'tp'))
    mask_spec = P(('dp', 'tp'), None)
    hid_spec = P(('dp', 'tp'), None, None)

    def local_step(q_hidden, d_hidden, q_mask, d_mask, positive, w_head, b_head):
        hidden_size, vocab_loc = w_head.shape
        vocab_size = vocab_loc * n_group
        n_q, q_len, _ = q_hidden.shape
        n_d, d_len, _ = d_hidden.shape
        pieces = d_len // q_len
        q_batch, d_batch = n_q * n_group, n_d * n_group
        tau = q_len * math.sqrt(vocab_size * d_len) / 16.0
        lam_q = 4.0 / (vocab_size * q_len * q_len)
        lam_d = 4.0 / (vocab_size * d_len * d_len)
        rows = n_q + n_d * pieces
        geo = Geometry(n_group, rows, hidden_size, vocab_loc, q_len)
        side, slots = geo.side, 2 * geo.chips
        lanes = max(128, d_batch)

        me = lax.axis_index('tp')
        slot = jnp.arange(slots)
        chip, rel = me // 2, slot // 2
        step_x, step_y = rel % side, rel // side
        chip_of = (((chip // side) ^ step_y ^ (step_y >> 1)) * side + ((chip % side) ^ step_x ^ (step_x >> 1)))
        device_of = chip_of * 2 + slot % 2
        place = (device_of[:, None] == jnp.arange(lanes)[None, :]).astype(F32)
        doc_of = (device_of[None, :] * n_d + jnp.arange(n_d)[:, None]).reshape((n_d * slots,))
        doc_place = (doc_of[:, None] == jnp.arange(lanes)[None, :]).astype(F32)
        doc_row = np.arange(n_d * slots)
        unit_row = np.arange(slots * n_d * pieces)
        pick = ((doc_row[:, None] % slots == unit_row[None, :] // (n_d * pieces))
                & (doc_row[:, None] // slots == unit_row[None, :] % (n_d * pieces) // pieces)).astype(np.float32)

        own_mask = jnp.concatenate([q_mask.reshape((-1,)), d_mask.reshape((-1,))]).astype(F32)
        mrow = jnp.pad(own_mask, (0, -own_mask.shape[0] % 128)).reshape((1, -1))
        const = (n_q, n_d, lam_q, lam_d, tau, float(q_batch), float(d_batch))
        loss, grad_w, grad_b, grad_h = call_fused(
            geo, const, q_hidden, d_hidden.reshape((n_d * pieces, q_len, hidden_size)), w_head,
            b_head.reshape((1, vocab_loc)), mrow, positive.reshape((n_q, 1)), place, doc_place, jnp.asarray(pick))
        return (loss[0, 0:1], grad_w, jnp.sum(grad_b, axis=0), grad_h[:n_q], grad_h[n_q:].reshape(d_hidden.shape))

    return jax.shard_map(local_step, mesh=mesh,
                         in_specs=(hid_spec, hid_spec, mask_spec, mask_spec, row_spec, P(None, 'tp'), P('tp')),
                         out_specs=(P('dp'), P('dp', 'tp'), row_spec, hid_spec, hid_spec),
                         check_vma=False)
```

```python
import functools
import math

import jax
import jax.numpy as jnp
import numpy as np
from jax import lax
from jax.experimental import pallas as pl
from jax.experimental.pallas import tpu as pltpu
from jax.sharding import PartitionSpec as P

MESH = pl.DeviceIdType.MESH
F32 = jnp.float32
BF16 = jnp.bfloat16
VMEM_LIMIT = 67043328
HIGHEST = lax.Precision.HIGHEST


class Geometry:
    def __init__(self, n_group, rows, hidden, vocab, unit):
        self.side = math.isqrt(n_group // 2)
        self.nd = 2 * (self.side.bit_length() - 1)
        self.chips = 1 << self.nd
        assert self.side == 4 and self.chips * 2 == n_group
        self.rows = rows
        self.first = self.nd + rows
        self.steps = self.first + rows
        self.unit = unit
        self.slab = 2 * unit
        self.tokens = self.slab * self.chips
        self.half = hidden // 2
        self.width = self.half // self.nd
        self.vocab = vocab

    def hops(self, rel):
        return bin(rel).count("1")

    def slot(self, rel, lane):
        return ((rel >> lane) | (rel << (self.nd - lane))) & (self.chips - 1)

    def device(self, me, rel, core):
        chip = lax.div(me, 2)
        x, y = lax.rem(chip, self.side), lax.div(chip, self.side)
        if rel & 1:
            x = x + 1 - 2 * lax.rem(x, 2)
        if rel & 2:
            x = self.side - 1 - x
        if rel & 4:
            y = y + 1 - 2 * lax.rem(y, 2)
        if rel & 8:
            y = self.side - 1 - y
        return {"tp": (y * self.side + x) * 2 + core}

    def peer(self, me, dim, core):
        return self.device(me, 1 << dim, core)


def entry_barrier(peers):
    barrier = pltpu.get_barrier_semaphore()
    for device in peers:
        pl.semaphore_signal(barrier, inc=1, device_id=device, device_id_type=MESH)
    pl.semaphore_wait(barrier, len(peers))


class Gather:
    def __init__(self, geo, me, x, stage, ownx, sems):
        (self.ici_send, self.ici_recv, self.piece_send, self.piece_recv, self.free_ici, self.free_piece) = sems
        self.geo, self.x, self.stage, self.ownx = geo, x, stage, ownx
        self.core = lax.rem(me, 2)
        self.sib = {"tp": me + 1 - 2 * self.core}
        dims = [geo.peer(me, dim, self.core)["tp"] for dim in range(geo.nd)]
        turn = geo.nd // 2
        self.same = [{"tp": dims[d] + self.core * (dims[(d + turn) % geo.nd] - dims[d])} for d in range(geo.nd)]

    def place(self, rel, lane):
        geo = self.geo
        one = geo.slot(rel, lane) * geo.slab
        two = geo.slot(rel, (lane + geo.nd // 2) % geo.nd) * geo.slab
        if one == two:
            return pl.ds(one, geo.slab)
        return pl.ds(pl.multiple_of(one + self.core * (two - one), geo.slab), geo.slab)

    def ici(self, s, lane, pos):
        count = (1 << pos) * self.geo.slab
        here, there = lax.rem(s, 2), lax.rem(s + 1, 2)
        return pltpu.make_async_remote_copy(
            src_ref=self.x.at[here, lane, pl.ds(0, count)], dst_ref=self.x.at[there, lane, pl.ds(count, count)],
            send_sem=self.ici_send.at[lane, pos, there], recv_sem=self.ici_recv.at[lane, pos, there],
            device_id=self.same[(lane + pos) % self.geo.nd], device_id_type=MESH)

    def piece(self, s, lane):
        width, parity = self.geo.width, lax.rem(s, 2)
        return pltpu.make_async_remote_copy(
            src_ref=self.ownx.at[1, lax.rem(s, self.geo.rows), :, pl.ds(lane * width, width)],
            dst_ref=self.stage.at[parity, lane], send_sem=self.piece_send.at[lane, parity],
            recv_sem=self.piece_recv.at[lane, parity], device_id=self.sib, device_id_type=MESH)

    def inject(self, s, lane):
        geo = self.geo
        width, parity = geo.width, lax.rem(s, 2)
        self.piece(s, lane).wait()
        mine = self.ownx[0, lax.rem(s, geo.rows), :, lane * width:(lane + 1) * width].astype(F32)
        theirs = self.stage[parity, lane].astype(F32)
        first = jnp.where(self.core == 0, mine, theirs)
        second = jnp.where(self.core == 0, theirs, mine)
        self.x[parity, lane, 0:geo.slab, :] = jnp.concatenate([first, second], axis=0).astype(BF16)

    def begin(self):
        geo = self.geo

        def first(lane, pos):
            return pltpu.make_async_remote_copy(
                src_ref=self.x.at[0, lane, pl.ds(0, geo.slab)],
                dst_ref=self.x.at[1, lane, pl.ds((1 << pos) * geo.slab, geo.slab)],
                send_sem=self.ici_send.at[lane, pos, 1], recv_sem=self.ici_recv.at[lane, pos, 1],
                device_id=self.same[(lane + pos) % geo.nd], device_id_type=MESH)

        for lane in range(geo.nd):
            self.inject(0, lane)
            for pos in range(geo.nd):
                first(lane, pos).start()
            self.piece(1, lane).start()
        for lane in range(geo.nd):
            for pos in range(geo.nd):
                first(lane, pos).wait_send()
            self.grant(lane)
        for lane in range(geo.nd):
            for pos in range(geo.nd):
                first(lane, pos).wait_recv()

    def arrive(self, s, lane, loss):
        geo = self.geo
        self.inject(s, lane)

        def receive():
            for pos in range(geo.nd):
                self.ici(s - 1, lane, pos).wait_recv()

        def send():
            pl.semaphore_wait(self.free_piece.at[lane], 1)
            for pos in range(geo.nd):
                pl.semaphore_wait(self.free_ici.at[lane, pos], 1)
            for pos in reversed(range(geo.nd)):
                self.ici(s, lane, pos).start()
            self.piece(s + 1, lane).start()

        if loss:
            @pl.when(s > 1)
            def _():
                receive()

            send()
        else:
            receive()

            @pl.when(s < geo.steps - 1)
            def _():
                send()

    def grant(self, lane):
        geo = self.geo
        for pos in range(geo.nd):
            pl.semaphore_signal(self.free_ici.at[lane, pos], inc=1,
                                device_id=self.same[(lane + pos) % geo.nd], device_id_type=MESH)
        pl.semaphore_signal(self.free_piece.at[lane], inc=1, device_id=self.sib, device_id_type=MESH)

    def release(self, s, lane, loss):
        geo = self.geo

        def sent():
            for pos in range(geo.nd):
                self.ici(s, lane, pos).wait_send()

        if loss:
            sent()
            self.grant(lane)
        else:
            @pl.when(s < geo.steps - 1)
            def _():
                sent()

            @pl.when(s < geo.steps - 2)
            def _():
                self.grant(lane)

    def tokens(self, s, lane):
        geo, parity = self.geo, lax.rem(s, 2)
        return jnp.concatenate([self.x[parity, lane, self.place(rel, lane), :] for rel in range(geo.chips)], axis=0)


def gather_scratch(geo):
    nd = geo.nd
    bufs = [pltpu.VMEM((2, nd, geo.tokens, geo.width), BF16), pltpu.VMEM((2, nd, geo.unit, geo.width), BF16),
            pltpu.VMEM((2, geo.rows, geo.unit, geo.half), BF16)]
    dma, reg = pltpu.SemaphoreType.DMA, pltpu.SemaphoreType.REGULAR
    sems = [dma((nd, nd, 2)), dma((nd, nd, 2)), dma((nd, 2)), dma((nd, 2)), reg((nd, nd)), reg((nd,))]
    return bufs, sems


def all_peers(geo, me):
    core = lax.rem(me, 2)
    found = [(0, 1 - core, geo.device(me, 0, 1 - core))]
    for rel in range(1, geo.chips):
        for other in range(2):
            found.append((rel, other, geo.device(me, rel, other)))
    return found


def fused_kernel(geo, const, q_hbm, d_hbm, w_hbm, bias, mrow, pos_ref, place, doc_place, pick,
                 loss_ref, gw_hbm, gb, gh_hbm,
                 x, stage, ownx, wv, wt, acc, zo, zs, zr, dz, dzt, dsum, m1, m2, m3,
                 r1, r2, r3, r4, ost, gout, early, rep, rd, drd, mall, mt, sbuf, pall, gmine, gall,
                 own_sem, w_sem, wx_send, wx_recv, z_send, z_recv, dz_send, dz_recv, rs_send, rs_recv,
                 out_send, out_recv, wout_sem, wo_send, wo_recv, hout_sem, ex_send, ex_recv, *sems):
    nd, slab, unit, width, steps, rows, first = (geo.nd, geo.slab, geo.unit, geo.width, geo.steps, geo.rows,
                                                 geo.first)
    n_q, n_d, lam_q, lam_d, tau, q_batch, d_batch = const
    slots, vocab = 2 * geo.chips, geo.vocab
    me = lax.axis_index("tp")
    net = Gather(geo, me, x, stage, ownx, sems)
    core, same = net.core, net.same
    peers = all_peers(geo, me)
    half_at = [pl.multiple_of(core * geo.half, geo.half), pl.multiple_of((1 - core) * geo.half, geo.half)]

    n_dp = d_hbm.shape[0]
    own_loads = []
    for half in range(2):
        cols = pl.ds(half_at[half], geo.half)
        own_loads.append(pltpu.make_async_copy(q_hbm.at[:, :, cols], ownx.at[half, pl.ds(0, n_q)],
                                               own_sem.at[2 * half]))
        own_loads.append(pltpu.make_async_copy(d_hbm.at[:, :, cols], ownx.at[half, pl.ds(n_q, n_dp)],
                                               own_sem.at[2 * half + 1]))
    w_loads, w_cross = [], []
    for lane in range(nd):
        here = pl.ds(pl.multiple_of(half_at[0] + lane * width, width), width)
        there = pl.ds(pl.multiple_of(half_at[1] + lane * width, width), width)
        w_loads.append(pltpu.make_async_copy(w_hbm.at[here, :], wv.at[lane, :, pl.ds(0, vocab)], w_sem.at[lane]))
        w_cross.append(pltpu.make_async_remote_copy(
            src_ref=w_hbm.at[there, :], dst_ref=wv.at[lane, :, pl.ds(vocab, vocab)], send_sem=wx_send.at[lane],
            recv_sem=wx_recv.at[lane], device_id=net.sib, device_id_type=MESH))
    for copy in own_loads + w_loads:
        copy.start()
    x[...] = jnp.zeros_like(x)
    entry_barrier([device for _, _, device in peers])
    for copy in own_loads:
        copy.wait()
    for lane in range(nd):
        net.piece(0, lane).start()

    def broadcast(kind, src_of, dst):
        return [pltpu.make_async_remote_copy(
            src_ref=src_of(2 * rel + other), dst_ref=dst.at[2 * rel + core],
            send_sem=ex_send.at[kind, i], recv_sem=ex_recv.at[kind, 2 * rel + core], device_id=device,
            device_id_type=MESH) for i, (rel, other, device) in enumerate(peers)]

    def arrivals(kind, dst):
        return [pltpu.make_async_remote_copy(
            src_ref=dst.at[2 * rel + other], dst_ref=dst.at[2 * rel + other],
            send_sem=ex_send.at[kind, i], recv_sem=ex_recv.at[kind, 2 * rel + other], device_id=device,
            device_id_type=MESH) for i, (rel, other, device) in enumerate(peers)]

    masks_out = broadcast(0, lambda slot: mrow, mall)
    for copy in masks_out:
        copy.start()
    mall[core] = mrow[...]
    gb[...] = jnp.zeros_like(gb)
    for copy in w_cross:
        copy.start()
    for ref in (dsum, m1, m2, m3):
        ref[...] = jnp.zeros_like(ref)

    part = vocab // 2

    def z_copy(s, half):
        parity, cols = lax.rem(s, 2), pl.ds(half * part, part)
        return pltpu.make_async_remote_copy(
            src_ref=zs.at[parity, :, cols], dst_ref=zr.at[parity, :, cols], send_sem=z_send.at[parity, half],
            recv_sem=z_recv.at[parity, half], device_id=net.sib, device_id_type=MESH)

    def dz_copy(half, turned):
        here, there = pl.ds(half * part, part), pl.ds(vocab + half * part, part)
        src, dst = (dzt.at[here], dzt.at[there]) if turned else (dz.at[:, here], dz.at[:, there])
        return pltpu.make_async_remote_copy(
            src_ref=src, dst_ref=dst, send_sem=dz_send.at[half, int(turned)], recv_sem=dz_recv.at[half, int(turned)],
            device_id=net.sib, device_id_type=MESH)

    def rs_copy(stage_no, lane, s):
        parity, ring = lax.rem(s, 2), lax.rem(s, 3)
        n_low = geo.tokens >> stage_no
        src = dsum.at[lax.rem(s + 2, 3), lane, pl.ds(n_low, n_low)]
        if stage_no > 1:
            src = (m1, m2, m3)[stage_no - 2].at[ring, lane, pl.ds(n_low, n_low)]
        dst = (r1, r2, r3, r4)[stage_no - 1].at[parity, lane]
        return pltpu.make_async_remote_copy(
            src_ref=src, dst_ref=dst, send_sem=rs_send.at[stage_no - 1, lane],
            recv_sem=rs_recv.at[stage_no - 1, lane, parity],
            device_id=same[(lane + nd - stage_no) % nd], device_id_type=MESH)

    def out_copy(s):
        parity = lax.rem(s, 2)
        return pltpu.make_async_remote_copy(
            src_ref=ost.at[parity], dst_ref=gout.at[1, lax.rem(s - 9, rows)], send_sem=out_send.at[parity],
            recv_sem=out_recv.at[parity], device_id=net.sib, device_id_type=MESH)

    def merge(stage_no, lane, s, last, low):
        @pl.when(s < last)
        def _():
            rs_copy(stage_no, lane, s - 1).wait()
        got = (r1, r2, r3, r4)[stage_no - 1][lax.rem(s + 1, 2), lane].astype(F32)
        return jnp.where(s < last, got, 0.0) + low.astype(F32)

    def scatter(s):
        ring, back = lax.rem(s, 3), lax.rem(s + 1, 3)
        low1, low2, low3, low4 = (geo.tokens >> k for k in range(1, 5))
        for lane in range(nd):
            cols = slice(lane * width, (lane + 1) * width)

            @pl.when((s >= first + 2) & (s <= steps + 2))
            def _():
                m1[ring, lane] = merge(1, lane, s, steps + 2, dsum[ring, lane, 0:low1]).astype(BF16)

            @pl.when((s >= first + 3) & (s <= steps + 4))
            def _():
                m2[ring, lane] = merge(2, lane, s, steps + 4, m1[back, lane, 0:low2]).astype(BF16)

            @pl.when((s >= first + 4) & (s <= steps + 6))
            def _():
                m3[ring, lane] = merge(3, lane, s, steps + 6, m2[back, lane, 0:low3]).astype(BF16)

            @pl.when((s >= first + 5) & (s <= steps + 8))
            def _():
                done = merge(4, lane, s, steps + 8, m3[back, lane, 0:low4])
                @pl.when(s < first + 9)
                def _():
                    early[lax.rem(s - first - 5, nd), lane] = done

                @pl.when(s >= first + 9)
                def _():
                    kept = lax.rem(s - first - 5 + nd - rows % nd, nd)
                    total = done + jnp.where(s >= steps + 5, early[kept, lane], 0.0)
                    one, two = total[0:unit], total[unit:slab]
                    gout[0, lax.rem(s - 9, rows), :, cols] = jnp.where(core == 0, one, two).astype(BF16)
                    ost[lax.rem(s, 2), :, cols] = jnp.where(core == 0, two, one).astype(BF16)

            @pl.when((s >= first + 2) & (s <= steps + 2))
            def _():
                rs_copy(2, lane, s).start()

            @pl.when((s >= first + 3) & (s <= steps + 4))
            def _():
                rs_copy(3, lane, s).start()

            @pl.when((s >= first + 4) & (s <= steps + 6))
            def _():
                rs_copy(4, lane, s).start()

        @pl.when((s >= first + 10) & (s <= steps + 8))
        def _():
            out_copy(s - 1).wait()

        @pl.when((s >= first + 9) & (s <= steps + 8))
        def _():
            out_copy(s).start()

    def logits_part(s, lane):
        parity = lax.rem(s, 2)
        tokens = net.tokens(s, lane)
        for ref, at in ((zs, vocab), (zo, 0)):
            part = jnp.dot(tokens, wv[lane, :, at:at + vocab], preferred_element_type=F32)
            if lane == 0:
                ref[parity] = part
            else:
                ref[parity] = ref[parity] + part

    def reps(s):
        parity = lax.rem(s, 2)
        for half in range(2):
            z_copy(s, half).wait()
        for rel in range(geo.chips):
            span = slice(rel * slab, (rel + 1) * slab)
            logits = zo[parity, span, :] + zr[parity, span, :] + bias[...]
            active = jnp.log1p(jnp.maximum(logits, 0.0))
            row = lax.rem(s - geo.hops(rel), rows)
            for cr in range(2):
                at = 2 * rel + cr
                part = active[cr * unit:(cr + 1) * unit, :] * mt[row, :, at:at + 1]
                rep[at, pl.ds(row, 1), :] = jnp.sum(part, axis=0, keepdims=True)

    def prepare(s):
        @pl.when(s == 1)
        def _():
            for copy in w_loads:
                copy.wait()
            for copy in arrivals(0, mall):
                copy.wait_recv()
            for copy in masks_out:
                copy.wait_send()
            table = jnp.concatenate([mall[i] for i in range(slots)], axis=0)
            table = jnp.concatenate([table, jnp.zeros((128 - slots, table.shape[1]), F32)], axis=0)
            mt[...] = table.T.reshape(mt.shape)

        @pl.when(s == 2)
        def _():
            for copy in w_cross:
                copy.wait()

        @pl.when((s >= 2) & (s < 2 + nd))
        def _():
            def turn(half, carry):
                span = pl.ds(pl.multiple_of(half * vocab, vocab), vocab)
                acc[s - 2, span, :] = jnp.zeros((vocab, width), F32)
                wt[s - 2, span, :] = wv[s - 2, :, span].T
                return carry

            lax.fori_loop(0, 2, turn, 0)

    def loss_step(s, carry):
        prepare(s)
        for lane in range(nd):
            if lane == nd - 1:
                net.release(s, 0, True)
            else:
                @pl.when(s > 1)
                def _():
                    net.release(s - 1, lane + 1, True)

            net.arrive(s, lane, True)

            @pl.when(s >= nd)
            def _():
                logits_part(s, lane)

            if lane == 1:
                @pl.when(s > nd)
                def _():
                    reps(s - 1)

        @pl.when(s >= nd)
        def _():
            for half in range(2):
                z_copy(s, half).start()
        return carry

    def softmax():
        chunk = 8
        parts = slots // chunk
        pieces = rep[:, n_q:rows, :].reshape((slots * (rows - n_q), geo.vocab))
        rd[...] = jnp.dot(pick[...], pieces, precision=HIGHEST, preferred_element_type=F32)

        def score(c, q_sum):
            at = pl.ds(c * chunk, chunk)
            reps_c = rep[at, 0:n_q, :].reshape((chunk * n_q, geo.vocab))
            part = lax.dot_general(reps_c, rd[...], (((1,), (1,)), ((), ())), precision=HIGHEST,
                                   preferred_element_type=F32)
            part = jnp.dot(part, doc_place[...], precision=HIGHEST, preferred_element_type=F32)
            sbuf[at] = part.reshape((chunk, n_q, part.shape[1]))
            return q_sum + jnp.sum(reps_c, axis=0, keepdims=True)

        q_sum = lax.fori_loop(0, parts, score, jnp.zeros((1, geo.vocab), F32))
        scores_out = broadcast(1, lambda slot: sbuf.at[slot], pall)
        for copy in scores_out:
            copy.start()
        pall[core] = sbuf[core]
        q_mean = q_sum / q_batch
        d_mean = jnp.sum(rd[...], axis=0, keepdims=True) / d_batch
        reg = (lam_q * jnp.sum(q_mean * q_mean, axis=1, keepdims=True)
               + lam_d * jnp.sum(d_mean * d_mean, axis=1, keepdims=True))
        for copy in arrivals(1, pall):
            copy.wait_recv()
        total = pall[0]
        for i in range(1, slots):
            total = total + pall[i]
        scores = total / tau
        lane_no = lax.broadcasted_iota(jnp.int32, scores.shape, 1)
        target = lane_no == pos_ref[...]
        masked = jnp.where(lane_no < d_batch, scores, -jnp.inf)
        top = jnp.max(masked, axis=1, keepdims=True)
        log_norm = jnp.log(jnp.sum(jnp.exp(masked - top), axis=1, keepdims=True)) + top
        hit = jnp.sum(jnp.where(target, scores, 0.0), axis=1, keepdims=True)
        mine = jnp.sum(log_norm - hit, axis=0, keepdims=True) / q_batch + reg
        grad = (jnp.exp(masked - log_norm) - target.astype(F32)) / (q_batch * tau)
        gmine[0:n_q, :] = grad
        gmine[n_q:, :] = jnp.broadcast_to(mine, (gmine.shape[0] - n_q, grad.shape[1]))
        grads_out = broadcast(2, lambda slot: gmine, gall)
        for copy in grads_out:
            copy.start()
        gall[core] = gmine[...]
        drd[...] = jnp.broadcast_to((2.0 * lam_d / d_batch) * d_mean, drd.shape)
        for copy in arrivals(2, gall):
            copy.wait_recv()
        by_device = jnp.zeros((1, place.shape[1]), F32)
        for i in range(slots):
            by_device = by_device + gall[i, n_q:n_q + 1, :] * place[i:i + 1, :]
        loss_ref[...] = jnp.broadcast_to(jnp.sum(by_device, axis=1, keepdims=True), loss_ref.shape)

        def back(c, carry):
            at = pl.ds(c * chunk, chunk)
            grad_c = gall[at, 0:n_q, :].reshape((chunk * n_q, gall.shape[2]))
            grad_c = lax.dot_general(grad_c, doc_place[...], (((1,), (1,)), ((), ())), precision=HIGHEST,
                                     preferred_element_type=F32)
            reps_c = rep[at, 0:n_q, :].reshape((chunk * n_q, geo.vocab))
            drd[...] += lax.dot_general(grad_c, reps_c, (((0,), (0,)), ((), ())), precision=HIGHEST,
                                        preferred_element_type=F32)
            drq = jnp.dot(grad_c, rd[...], precision=HIGHEST, preferred_element_type=F32)
            drq = drq + (2.0 * lam_q / q_batch) * q_mean
            rep[at, 0:n_q, :] = drq.reshape((chunk, n_q, geo.vocab))
            return carry

        lax.fori_loop(0, parts, back, 0)
        spread = lax.dot_general(pick[...], drd[...], (((0,), (0,)), ((), ())), precision=HIGHEST,
                                 preferred_element_type=F32)
        rep[:, n_q:rows, :] = spread.reshape((slots, rows - n_q, geo.vocab))
        for copy in scores_out + grads_out:
            copy.wait_send()

    def logit_sum(s, at):
        total = jnp.dot(net.tokens(s, 0), wv[0, :, at:at + part], preferred_element_type=F32)
        for lane in range(1, nd):
            total += jnp.dot(net.tokens(s, lane), wv[lane, :, at:at + part], preferred_element_type=F32)
        return total

    def logits_grad(s, half):
        parity = lax.rem(s, 2)
        cols = slice(half * part, (half + 1) * part)
        total = gb[:, cols]
        for rel in range(geo.chips):
            span = slice(rel * slab, (rel + 1) * slab)
            logits = zo[parity, span, cols] + zr[parity, span, cols] + bias[:, cols]
            inverse = 1.0 / (1.0 + logits)
            row = lax.rem(s - geo.hops(rel), rows)
            parts = []
            for cr in range(2):
                at = 2 * rel + cr
                tok = slice(cr * unit, (cr + 1) * unit)
                grad_row = rep[at, pl.ds(row, 1), cols] * inverse[tok, :]
                grad_row = jnp.where(logits[tok, :] > 0.0, grad_row, 0.0) * mt[row, :, at:at + 1]
                total = total + grad_row
                parts.append(grad_row)
            dz[span, cols] = jnp.concatenate(parts, axis=0).astype(BF16)
        gb[:, cols] = total
        dzt[cols, :] = dz[:, cols].T

    def accumulate(s, at, count):
        for lane in range(nd):
            acc[lane, at:at + count, :] += jnp.dot(dzt[at:at + count, :], net.tokens(s, lane),
                                                   preferred_element_type=F32)

    def grad_step(s, carry):
        parity = lax.rem(s, 2)
        for lane in range(nd):
            net.arrive(s, lane, False)
        for half in range(2):
            zs[parity, :, half * part:(half + 1) * part] = logit_sum(s, vocab + half * part)
            z_copy(s, half).start()
        zo[parity, :, 0:part] = logit_sum(s, 0)
        z_copy(s, 0).wait()
        logits_grad(s, 0)
        zo[parity, :, part:vocab] = logit_sum(s, part)
        dz_copy(0, True).start()
        dz_copy(0, False).start()
        z_copy(s, 1).wait()
        logits_grad(s, 1)
        accumulate(s, 0, part)
        dz_copy(1, True).start()
        dz_copy(1, False).start()
        scatter(s + 1)
        accumulate(s, part, part)
        for half in range(2):
            dz_copy(half, True).wait()
        accumulate(s, vocab, vocab)
        for half in range(2):
            dz_copy(half, False).wait()
        ring = lax.rem(s, 3)
        for lane in range(nd):
            block = jnp.dot(dz[...], wt[lane], preferred_element_type=F32).astype(BF16)
            for rel in range(geo.chips):
                dsum[ring, lane, net.place(rel, lane), :] = block[rel * slab:(rel + 1) * slab, :]
            rs_copy(1, lane, s + 1).start()
            if lane >= 2:
                net.release(s, 2 * lane - 4, False)
                net.release(s, 2 * lane - 3, False)
        return carry

    def wout(lane):
        return pltpu.make_async_copy(
            wv.at[lane, :, pl.ds(0, vocab)],
            gw_hbm.at[pl.ds(pl.multiple_of(half_at[0] + lane * width, width), width), :], wout_sem.at[lane])

    def wout_cross(lane):
        return pltpu.make_async_remote_copy(
            src_ref=wv.at[lane, :, pl.ds(vocab, vocab)],
            dst_ref=gw_hbm.at[pl.ds(pl.multiple_of(half_at[0] + lane * width, width), width), :],
            send_sem=wo_send.at[lane], recv_sem=wo_recv.at[lane], device_id=net.sib, device_id_type=MESH)

    def tail_step(s, carry):
        scatter(s)

        @pl.when(s <= steps + nd)
        def _():
            lane = s - steps - 1
            for half in range(2):
                span = slice(half * vocab, (half + 1) * vocab)
                wv[lane, :, span] = acc[lane, span, :].astype(BF16).T
            wout(lane).start()
            wout_cross(lane).start()
        return carry

    net.begin()
    lax.fori_loop(1, first, loss_step, 0)
    for lane in range(1, nd):
        net.release(first - 1, lane, True)
    reps(first - 1)
    softmax()
    lax.fori_loop(first, steps, grad_step, 0)
    lax.fori_loop(steps + 1, steps + 9, tail_step, 0)
    out_copy(steps + 8).wait()
    stores = [pltpu.make_async_copy(gout.at[half], gh_hbm.at[:, :, pl.ds(half_at[half], geo.half)], hout_sem.at[half])
              for half in range(2)]
    for copy in stores:
        copy.start()
    for copy in stores:
        copy.wait()
    for lane in range(nd):
        wout(lane).wait()
        wout_cross(lane).wait()


def call_fused(geo, const, q_rows, d_rows, w_head, bias, mrow, positive, place, doc_place, pick):
    bufs, sems = gather_scratch(geo)
    dma = pltpu.SemaphoreType.DMA
    nd, tok, width, vocab, rows = geo.nd, geo.tokens, geo.width, geo.vocab, geo.rows
    n_q, docs, slots = const[0], doc_place.shape[0], 2 * geo.chips
    lanes = doc_place.shape[1]
    tile = n_q + 8
    hbm, vmem = pl.BlockSpec(memory_space=pl.ANY), pl.BlockSpec(memory_space=pltpu.VMEM)
    logit = pltpu.VMEM((2, tok, vocab), F32)
    scratch = bufs + [
        pltpu.VMEM((nd, width, 2 * vocab), BF16), pltpu.VMEM((nd, 2 * vocab, width), BF16),
        pltpu.VMEM((nd, 2 * vocab, width), F32), logit, logit, logit,
        pltpu.VMEM((tok, 2 * vocab), BF16), pltpu.VMEM((2 * vocab, tok), BF16),
        pltpu.VMEM((3, nd, tok, width), BF16),
        pltpu.VMEM((3, nd, tok // 2, width), BF16), pltpu.VMEM((3, nd, tok // 4, width), BF16),
        pltpu.VMEM((3, nd, tok // 8, width), BF16),
        pltpu.VMEM((2, nd, tok // 2, width), BF16), pltpu.VMEM((2, nd, tok // 4, width), BF16),
        pltpu.VMEM((2, nd, tok // 8, width), BF16), pltpu.VMEM((2, nd, tok // 16, width), BF16),
        pltpu.VMEM((2, geo.unit, geo.half), BF16), pltpu.VMEM((2, rows, geo.unit, geo.half), BF16),
        pltpu.VMEM((nd, nd, geo.slab, width), F32),
        pltpu.VMEM((slots, rows, vocab), F32), pltpu.VMEM((docs, vocab), F32), pltpu.VMEM((docs, vocab), F32),
        pltpu.VMEM((slots,) + mrow.shape, F32), pltpu.VMEM((mrow.shape[1] // geo.unit, geo.unit, 128), F32),
        pltpu.VMEM((slots, n_q, lanes), F32), pltpu.VMEM((slots, n_q, lanes), F32),
        pltpu.VMEM((tile, lanes), F32), pltpu.VMEM((slots, tile, lanes), F32),
        dma((4,)), dma((nd,)), dma((nd,)), dma((nd,)), dma((2, 2)), dma((2, 2)), dma((2, 2)), dma((2, 2)),
        dma((4, nd)), dma((4, nd, 2)), dma((2,)), dma((2,)), dma((nd,)), dma((nd,)), dma((nd,)), dma((2,)),
        dma((3, slots)), dma((3, slots))] + sems
    return pl.pallas_call(
        functools.partial(fused_kernel, geo, const),
        name="lexical_head",
        out_shape=[jax.ShapeDtypeStruct((1, 128), F32), jax.ShapeDtypeStruct(w_head.shape, BF16),
                   jax.ShapeDtypeStruct((geo.unit, vocab), F32),
                   jax.ShapeDtypeStruct((rows, geo.unit, 2 * geo.half), BF16)],
        in_specs=[hbm, hbm, hbm] + [vmem] * 6,
        out_specs=[vmem, hbm, vmem, hbm],
        scratch_shapes=scratch,
        compiler_params=pltpu.CompilerParams(collective_id=0, has_side_effects=True, vmem_limit_bytes=VMEM_LIMIT),
    )(q_rows, d_rows, w_head, bias, mrow, positive, place, doc_place, pick)


def solution(mesh):
    n_group = mesh.shape['tp']
    row_spec = P(('dp', 'tp'))
    mask_spec = P(('dp', 'tp'), None)
    hid_spec = P(('dp', 'tp'), None, None)

    def local_step(q_hidden, d_hidden, q_mask, d_mask, positive, w_head, b_head):
        hidden_size, vocab_loc = w_head.shape
        vocab_size = vocab_loc * n_group
        n_q, q_len, _ = q_hidden.shape
        n_d, d_len, _ = d_hidden.shape
        pieces = d_len // q_len
        q_batch, d_batch = n_q * n_group, n_d * n_group
        tau = q_len * math.sqrt(vocab_size * d_len) / 16.0
        lam_q = 4.0 / (vocab_size * q_len * q_len)
        lam_d = 4.0 / (vocab_size * d_len * d_len)
        rows = n_q + n_d * pieces
        geo = Geometry(n_group, rows, hidden_size, vocab_loc, q_len)
        side, slots = geo.side, 2 * geo.chips
        lanes = max(128, d_batch)

        me = lax.axis_index('tp')
        slot = jnp.arange(slots)
        chip, rel = me // 2, slot // 2
        step_x, step_y = rel % side, rel // side
        chip_of = (((chip // side) ^ step_y ^ (step_y >> 1)) * side + ((chip % side) ^ step_x ^ (step_x >> 1)))
        device_of = chip_of * 2 + slot % 2
        place = (device_of[:, None] == jnp.arange(lanes)[None, :]).astype(F32)
        doc_of = (device_of[None, :] * n_d + jnp.arange(n_d)[:, None]).reshape((n_d * slots,))
        doc_place = (doc_of[:, None] == jnp.arange(lanes)[None, :]).astype(F32)
        doc_row = np.arange(n_d * slots)
        unit_row = np.arange(slots * n_d * pieces)
        pick = ((doc_row[:, None] % slots == unit_row[None, :] // (n_d * pieces))
                & (doc_row[:, None] // slots == unit_row[None, :] % (n_d * pieces) // pieces)).astype(np.float32)

        own_mask = jnp.concatenate([q_mask.reshape((-1,)), d_mask.reshape((-1,))]).astype(F32)
        mrow = jnp.pad(own_mask, (0, -own_mask.shape[0] % 128)).reshape((1, -1))
        const = (n_q, n_d, lam_q, lam_d, tau, float(q_batch), float(d_batch))
        loss, grad_w, grad_b, grad_h = call_fused(
            geo, const, q_hidden, d_hidden.reshape((n_d * pieces, q_len, hidden_size)), w_head,
            b_head.reshape((1, vocab_loc)), mrow, positive.reshape((n_q, 1)), place, doc_place, jnp.asarray(pick))
        return (loss[0, 0:1], grad_w, jnp.sum(grad_b, axis=0), grad_h[:n_q], grad_h[n_q:].reshape(d_hidden.shape))

    return jax.shard_map(local_step, mesh=mesh,
                         in_specs=(hid_spec, hid_spec, mask_spec, mask_spec, row_spec, P(None, 'tp'), P('tp')),
                         out_specs=(P('dp'), P('dp', 'tp'), row_spec, hid_spec, hid_spec),
                         check_vma=False)
```

```python
import functools
import math

import jax
import jax.numpy as jnp
import numpy as np
from jax import lax
from jax.experimental import pallas as pl
from jax.experimental.pallas import tpu as pltpu
from jax.sharding import PartitionSpec as P

MESH = pl.DeviceIdType.MESH
F32 = jnp.float32
BF16 = jnp.bfloat16
VMEM_LIMIT = 67043328
PAIR = range(2)
HIGHEST = lax.Precision.HIGHEST


def parity(s):
    return lax.rem(s, 2)


def ring(s):
    return lax.rem(s, 3)


def sum_rows(x):
    return jnp.sum(x, axis=0, keepdims=True)


def sum_lanes(x):
    return jnp.sum(x, axis=1, keepdims=True)


def exact_dot(a, b, dims=(((1,), (0,)), ((), ()))):
    return lax.dot_general(a, b, dims, precision=HIGHEST, preferred_element_type=F32)


TURNED = (((1,), (1,)), ((), ()))
FIRST = (((0,), (0,)), ((), ()))


class Geometry:
    def __init__(self, n_group, rows, hidden, vocab, unit):
        self.side = math.isqrt(n_group // 2)
        self.nd = 2 * (self.side.bit_length() - 1)
        self.chips = 1 << self.nd
        assert self.side == 4 and self.chips * 2 == n_group
        self.rows = rows
        self.first = self.nd + rows
        self.steps = self.first + rows
        self.unit = unit
        self.slab = 2 * unit
        self.tokens = self.slab * self.chips
        self.half = hidden // 2
        self.width = self.half // self.nd
        self.vocab = vocab

    def hops(self, rel):
        return bin(rel).count("1")

    def slot(self, rel, lane):
        return ((rel >> lane) | (rel << (self.nd - lane))) & (self.chips - 1)

    def device(self, me, rel, core):
        chip = lax.div(me, 2)
        x, y = lax.rem(chip, self.side), lax.div(chip, self.side)
        at = [x, y]
        for dim in range(self.nd):
            if rel >> dim & 1:
                axis, wide = divmod(dim, len(at))
                at[axis] = self.side - 1 - at[axis] if wide else at[axis] + 1 - 2 * lax.rem(at[axis], 2)
        x, y = at
        return {"tp": (y * self.side + x) * 2 + core}

    def peer(self, me, dim, core):
        return self.device(me, 1 << dim, core)


def entry_barrier(peers):
    barrier = pltpu.get_barrier_semaphore()
    for device in peers:
        pl.semaphore_signal(barrier, inc=1, device_id=device, device_id_type=MESH)
    pl.semaphore_wait(barrier, len(peers))


class Gather:
    def __init__(self, geo, me, x, stage, ownx, sems):
        (self.ici_send, self.ici_recv, self.piece_send, self.piece_recv, self.free_ici, self.free_piece) = sems
        self.geo, self.x, self.stage, self.ownx = geo, x, stage, ownx
        self.core = lax.rem(me, 2)
        self.sib = {"tp": me + 1 - 2 * self.core}
        dims = [geo.peer(me, dim, self.core)["tp"] for dim in range(geo.nd)]
        turn = geo.nd // 2
        self.same = [{"tp": dims[d] + self.core * (dims[(d + turn) % geo.nd] - dims[d])} for d in range(geo.nd)]

    def place(self, rel, lane):
        geo = self.geo
        one = geo.slot(rel, lane) * geo.slab
        two = geo.slot(rel, (lane + geo.nd // 2) % geo.nd) * geo.slab
        if one == two:
            return pl.ds(one, geo.slab)
        return pl.ds(pl.multiple_of(one + self.core * (two - one), geo.slab), geo.slab)

    def ici(self, s, lane, pos):
        count = (1 << pos) * self.geo.slab
        here, there = parity(s), parity(s + 1)
        return pltpu.make_async_remote_copy(
            src_ref=self.x.at[here, lane, pl.ds(0, count)], dst_ref=self.x.at[there, lane, pl.ds(count, count)],
            send_sem=self.ici_send.at[lane, pos, there], recv_sem=self.ici_recv.at[lane, pos, there],
            device_id=self.same[(lane + pos) % self.geo.nd], device_id_type=MESH)

    def piece(self, s, lane):
        width = self.geo.width
        return pltpu.make_async_remote_copy(
            src_ref=self.ownx.at[1, lax.rem(s, self.geo.rows), :, pl.ds(lane * width, width)],
            dst_ref=self.stage.at[parity(s), lane], send_sem=self.piece_send.at[lane, parity(s)],
            recv_sem=self.piece_recv.at[lane, parity(s)], device_id=self.sib, device_id_type=MESH)

    def inject(self, s, lane):
        geo = self.geo
        width = geo.width
        self.piece(s, lane).wait()
        mine = self.ownx[0, lax.rem(s, geo.rows), :, lane * width:(lane + 1) * width].astype(F32)
        theirs = self.stage[parity(s), lane].astype(F32)
        first = jnp.where(self.core == 0, mine, theirs)
        second = jnp.where(self.core == 0, theirs, mine)
        self.x[parity(s), lane, :geo.slab, :] = jnp.concatenate([first, second], axis=0).astype(BF16)

    def begin(self):
        geo = self.geo
        for lane in range(geo.nd):
            self.inject(0, lane)
            for pos in range(geo.nd):
                self.first(lane, pos).start()
            self.piece(1, lane).start()

    def begun(self):
        geo = self.geo
        for lane in range(geo.nd):
            for pos in range(geo.nd):
                self.first(lane, pos).wait_send()
            self.grant(lane)
        for lane in range(geo.nd):
            for pos in range(geo.nd):
                self.first(lane, pos).wait_recv()

    def first(self, lane, pos):
        geo = self.geo
        return pltpu.make_async_remote_copy(
            src_ref=self.x.at[0, lane, pl.ds(0, geo.slab)],
            dst_ref=self.x.at[1, lane, pl.ds((1 << pos) * geo.slab, geo.slab)],
            send_sem=self.ici_send.at[lane, pos, 1], recv_sem=self.ici_recv.at[lane, pos, 1],
            device_id=self.same[(lane + pos) % geo.nd], device_id_type=MESH)

    def arrive(self, s, lane, loss):
        geo = self.geo
        self.inject(s, lane)

        def receive():
            for pos in range(geo.nd):
                self.ici(s - 1, lane, pos).wait_recv()

        def credits():
            pl.semaphore_wait(self.free_piece.at[lane], 1)
            for pos in range(geo.nd):
                pl.semaphore_wait(self.free_ici.at[lane, pos], 1)

        def send():
            for pos in reversed(range(geo.nd)):
                self.ici(s, lane, pos).start()
            self.piece(s + 1, lane).start()

        if loss:
            @pl.when(s > 1)
            def _():
                receive()

            credits()
            send()
        else:
            receive()
            credits()

            @pl.when(s < geo.steps - 1)
            def _():
                send()

    def grant(self, lane):
        geo = self.geo
        for pos in range(geo.nd):
            pl.semaphore_signal(self.free_ici.at[lane, pos], inc=1,
                                device_id=self.same[(lane + pos) % geo.nd], device_id_type=MESH)
        pl.semaphore_signal(self.free_piece.at[lane], inc=1, device_id=self.sib, device_id_type=MESH)

    def release(self, s, lane, loss):
        geo = self.geo

        def sent():
            for pos in range(geo.nd):
                self.ici(s, lane, pos).wait_send()

        if loss:
            sent()
            self.grant(lane)
        else:
            @pl.when(s < geo.steps - 1)
            def _():
                sent()
                self.grant(lane)

    def tokens(self, s, lane):
        geo = self.geo
        return jnp.concatenate([self.x[parity(s), lane, self.place(rel, lane), :] for rel in range(geo.chips)], axis=0)


def gather_scratch(geo):
    nd = geo.nd
    bufs = [pltpu.VMEM((2, nd, geo.tokens, geo.width), BF16), pltpu.VMEM((2, nd, geo.unit, geo.width), BF16),
            pltpu.VMEM((2, geo.rows, geo.unit, geo.half), BF16)]
    dma, reg = pltpu.SemaphoreType.DMA, pltpu.SemaphoreType.REGULAR
    sems = [dma((nd, nd, 2)), dma((nd, nd, 2)), dma((nd, 2)), dma((nd, 2)), reg((nd, nd)), reg((nd,))]
    return bufs, sems


def all_peers(geo, me):
    core = lax.rem(me, 2)
    found = [(0, 1 - core, geo.device(me, 0, 1 - core))]
    for rel in range(1, geo.chips):
        for other in PAIR:
            found.append((rel, other, geo.device(me, rel, other)))
    return found


def fused_kernel(geo, const, q_hbm, d_hbm, w_hbm, bias, mrow, pos_ref, place, doc_place, pick,
                 loss_ref, gw_hbm, gb_ref, gq_hbm, gd_hbm,
                 x, stage, ownx, wv, wt, acc, zo, zs, zr, dz, dzt, dsum, m1, m2, m3,
                 r1, r2, r3, r4, x2, x3, x4, ost, gout, early, last, gb, rep, rd, drd, mall, mt, sbuf, pall, gmine, gall,
                 lmine, lall,
                 own_sem, w_sem, wx_send, wx_recv, z_send, z_recv, dz_send, dz_recv, rs_send, rs_recv, fl_send, fl_recv,
                 out_send, out_recv, wout_sem, wo_send, wo_recv, hout_sem, ex_send, ex_recv, *sems):
    nd, slab, unit, width, steps, rows, first = (geo.nd, geo.slab, geo.unit, geo.width, geo.steps, geo.rows,
                                                 geo.first)
    n_q, n_d, lam_q, lam_d, tau, q_batch, d_batch = const
    slots, vocab = 2 * geo.chips, geo.vocab
    me = lax.axis_index("tp")
    net = Gather(geo, me, x, stage, ownx, sems)
    core, same = net.core, net.same
    peers = all_peers(geo, me)
    half_at = [pl.multiple_of(core * geo.half, geo.half), pl.multiple_of((1 - core) * geo.half, geo.half)]

    n_dp = d_hbm.shape[0]
    own_loads = []
    for half in PAIR:
        cols = pl.ds(half_at[half], geo.half)
        own_loads.append(pltpu.make_async_copy(q_hbm.at[:, :, cols], ownx.at[half, pl.ds(0, n_q)],
                                               own_sem.at[2 * half]))
        own_loads.append(pltpu.make_async_copy(d_hbm.at[:, :, cols], ownx.at[half, pl.ds(n_q, n_dp)],
                                               own_sem.at[2 * half + 1]))
    w_loads, w_cross = [], []
    for lane in range(nd):
        here = pl.ds(pl.multiple_of(half_at[0] + lane * width, width), width)
        there = pl.ds(pl.multiple_of(half_at[1] + lane * width, width), width)
        w_loads.append(pltpu.make_async_copy(w_hbm.at[here, :], wv.at[lane, :, pl.ds(0, vocab)], w_sem.at[lane]))
        w_cross.append(pltpu.make_async_remote_copy(
            src_ref=w_hbm.at[there, :], dst_ref=wv.at[lane, :, pl.ds(vocab, vocab)], send_sem=wx_send.at[lane],
            recv_sem=wx_recv.at[lane], device_id=net.sib, device_id_type=MESH))
    for copy in own_loads + w_loads:
        copy.start()
    entry_barrier([device for _, _, device in peers])
    for copy in own_loads:
        copy.wait()
    for lane in range(nd):
        net.piece(0, lane).start()
    net.begin()

    def broadcast(kind, src_of, dst):
        return [pltpu.make_async_remote_copy(
            src_ref=src_of(2 * rel + other), dst_ref=dst.at[2 * rel + core],
            send_sem=ex_send.at[kind, i], recv_sem=ex_recv.at[kind, 2 * rel + core], device_id=device,
            device_id_type=MESH) for i, (rel, other, device) in enumerate(peers)]

    def arrivals(kind, dst):
        return [pltpu.make_async_remote_copy(
            src_ref=dst.at[2 * rel + other], dst_ref=dst.at[2 * rel + other],
            send_sem=ex_send.at[kind, i], recv_sem=ex_recv.at[kind, 2 * rel + other], device_id=device,
            device_id_type=MESH) for i, (rel, other, device) in enumerate(peers)]

    masks_out = broadcast(0, lambda slot: mrow, mall)
    for copy in masks_out:
        copy.start()
    mall[core] = mrow[...]
    for copy in w_cross:
        copy.start()
    gb[...] = jnp.zeros_like(gb)
    for ref in (dsum, m1, m2, m3, dz):
        ref[...] = jnp.zeros_like(ref)

    part = vocab // 2

    def z_copy(s, half):
        cols = pl.ds(half * part, part)
        return pltpu.make_async_remote_copy(
            src_ref=zs.at[parity(s), :, cols], dst_ref=zr.at[parity(s), :, cols], send_sem=z_send.at[parity(s), half],
            recv_sem=z_recv.at[parity(s), half], device_id=net.sib, device_id_type=MESH)

    def dz_copy(s, half, turned):
        here, there = pl.ds(half * part, part), pl.ds(vocab + half * part, part)
        src, dst = dzt.at[here], dzt.at[there]
        if not turned:
            src, dst = dz.at[parity(s), :, here], dz.at[parity(s), :, there]
        return pltpu.make_async_remote_copy(
            src_ref=src, dst_ref=dst, send_sem=dz_send.at[half, int(turned)], recv_sem=dz_recv.at[half, int(turned)],
            device_id=net.sib, device_id_type=MESH)

    def rs_copy(stage_no, lane, s):
        n_low = geo.tokens >> stage_no
        src = dsum.at[ring(s + 2), lane, pl.ds(n_low, n_low)]
        if stage_no > 1:
            src = (m1, m2, m3)[stage_no - 2].at[ring(s), lane, pl.ds(n_low, n_low)]
        dst = (r1, r2, r3, r4)[stage_no - 1].at[parity(s), lane]
        return pltpu.make_async_remote_copy(
            src_ref=src, dst_ref=dst, send_sem=rs_send.at[stage_no - 1, lane, parity(s)],
            recv_sem=rs_recv.at[stage_no - 1, lane, parity(s)],
            device_id=same[(lane + nd - stage_no) % nd], device_id_type=MESH)

    low = [geo.tokens >> k for k in range(5)]
    deep = (low[2] + low[4], low[2] + low[3], low[2] + low[3] + low[4])
    later = (2, 3, 4)
    tail, spare = (steps - 1) % 3, steps % 3

    def flush_copy(i, lane):
        src, dst, stage_no = (
            (dsum.at[tail, lane, pl.ds(low[2], low[2])], x2.at[lane], 2),
            (dsum.at[spare, lane, pl.ds(low[3], low[3])], x3.at[0, lane], 3),
            (dsum.at[tail, lane, pl.ds(low[3], low[3])], x3.at[1, lane], 3),
            (dsum.at[spare, lane, pl.ds(deep[0], low[4])], x4.at[0, lane], 4),
            (dsum.at[spare, lane, pl.ds(deep[2], low[4])], x4.at[1, lane], 4),
            (dsum.at[tail, lane, pl.ds(low[4], low[4])], x4.at[2, lane], 4))[i]
        return pltpu.make_async_remote_copy(
            src_ref=src, dst_ref=dst, send_sem=fl_send.at[i, lane], recv_sem=fl_recv.at[i, lane],
            device_id=same[(lane + nd - stage_no) % nd], device_id_type=MESH)

    def out_copy(s, at):
        return pltpu.make_async_remote_copy(
            src_ref=ost.at[at], dst_ref=gout.at[1, lax.rem(s - 9, rows)], send_sem=out_send.at[at],
            recv_sem=out_recv.at[at], device_id=net.sib, device_id_type=MESH)

    def emit(lane, s, total, at):
        cols = slice(lane * width, (lane + 1) * width)
        one, two = total[:unit], total[unit:slab]
        gout[0, lax.rem(s - 9, rows), :, cols] = jnp.where(core == 0, one, two).astype(BF16)
        ost[at, :, cols] = jnp.where(core == 0, two, one).astype(BF16)

    def merged(stage_no, lane, s, mine):
        got = (r1, r2, r3, r4)[stage_no - 1][parity(s + 1), lane].astype(F32)
        return got + mine.astype(F32)

    def merge_first(s):
        for lane in range(nd):
            rs_copy(1, lane, s - 1).wait()
        for lane in range(nd):
            m1[ring(s), lane] = merged(1, lane, s, dsum[ring(s), lane, :low[1]]).astype(BF16)

    def merge_rest(s):
        back = ring(s + 1)
        for lane in range(nd):
            for stage_no in later:
                rs_copy(stage_no, lane, s - 1).wait()
        for lane in range(nd):
            m2[ring(s), lane] = merged(2, lane, s, m1[back, lane, :low[2]]).astype(BF16)
            m3[ring(s), lane] = merged(3, lane, s, m2[back, lane, :low[3]]).astype(BF16)
            last[lane] = merged(4, lane, s, m3[back, lane, :low[4]])

    def finish(s):
        @pl.when((s >= first + 5) & (s < first + 9))
        def _():
            early[lax.rem(s - first - 5, nd)] = last[...]

        @pl.when(s >= first + 9)
        def _():
            for lane in range(nd):
                emit(lane, s, last[lane], parity(s))

        @pl.when(s >= first + 10)
        def _():
            out_copy(s - 1, parity(s + 1)).wait()

        @pl.when(s >= first + 9)
        def _():
            out_copy(s, parity(s)).start()

    def start_rest(s):
        for lane in range(nd):
            rs_copy(3, lane, s).start()
            rs_copy(4, lane, s).start()

    def logits_part(s, lane):
        tokens = net.tokens(s, lane)
        for ref, at in ((zs, vocab), (zo, 0)):
            part = jnp.dot(tokens, wv[lane, :, at:at + vocab], preferred_element_type=F32)
            if lane == 0:
                ref[parity(s)] = part
            else:
                ref[parity(s)] = ref[parity(s)] + part

    def reps(s):
        for half in PAIR:
            z_copy(s, half).wait()
        for rel in range(geo.chips):
            span = slice(rel * slab, (rel + 1) * slab)
            logits = zo[parity(s), span, :] + zr[parity(s), span, :] + bias[...]
            active = jnp.log1p(jnp.maximum(logits, 0.0))
            row = lax.rem(s - geo.hops(rel), rows)
            for cr in PAIR:
                at = 2 * rel + cr
                part = active[cr * unit:(cr + 1) * unit, :] * mt[row, :, at:at + 1]
                rep[at, pl.ds(row, 1), :] = sum_rows(part)

    def prepare(s):
        @pl.when(s == 1)
        def _():
            for copy in w_loads:
                copy.wait()
            for copy in arrivals(0, mall):
                copy.wait_recv()
            for copy in masks_out:
                copy.wait_send()
            table = jnp.concatenate([mall[i] for i in range(slots)], axis=0)
            table = jnp.concatenate([table, jnp.zeros((128 - slots, table.shape[1]), F32)], axis=0)
            mt[...] = table.T.reshape(mt.shape)

        @pl.when(s == 2)
        def _():
            for copy in w_cross:
                copy.wait()

        @pl.when((s >= 2) & (s < 2 + nd))
        def _():
            def turn(half, carry):
                span = pl.ds(pl.multiple_of(half * vocab, vocab), vocab)
                acc[s - 2, span, :] = jnp.zeros((vocab, width), F32)
                wt[s - 2, span, :] = wv[s - 2, :, span].T
                return carry

            lax.fori_loop(0, 2, turn, 0)

    def loss_step(s, carry):
        prepare(s)
        for lane in range(nd):
            if lane == nd - 1:
                net.release(s, 0, True)
            else:
                @pl.when(s > 1)
                def _():
                    net.release(s - 1, lane + 1, True)

            net.arrive(s, lane, True)

            @pl.when(s >= nd)
            def _():
                logits_part(s, lane)

            if lane == 1:
                @pl.when(s > nd)
                def _():
                    reps(s - 1)

        @pl.when(s >= nd)
        def _():
            for half in PAIR:
                z_copy(s, half).start()
        return carry

    def softmax():
        chunk = 16
        hq = n_q // 2
        shift = loss_ref.shape[1] // 2
        parts = slots // chunk
        pieces = rep[:, n_q:rows, :].reshape((slots * (rows - n_q), geo.vocab))
        rd[...] = exact_dot(pick[...], pieces)

        def score(c, q_sum):
            at = pl.ds(c * chunk, chunk)
            reps_c = rep[at, :n_q, :].reshape((chunk * n_q, geo.vocab))
            part = exact_dot(reps_c, rd[...], TURNED)
            part = exact_dot(part, doc_place[...])
            part = part.reshape((chunk, n_q, part.shape[1]))
            sbuf[at] = part[:, :hq] + pltpu.roll(part[:, hq:], shift, 2)
            return q_sum + sum_rows(reps_c)

        q_sum = lax.fori_loop(0, parts, score, jnp.zeros((1, geo.vocab), F32))
        scores_out = broadcast(1, lambda slot: sbuf.at[slot], pall)
        for copy in scores_out:
            copy.start()
        pall[core] = sbuf[core]
        q_mean = q_sum / q_batch
        d_mean = sum_rows(rd[...]) / d_batch
        reg = (lam_q * sum_lanes(q_mean * q_mean)
               + lam_d * sum_lanes(d_mean * d_mean))
        for copy in arrivals(1, pall):
            copy.wait_recv()
        total = pall[0]
        for i in range(1, slots):
            total = total + pall[i]
        scores = jnp.concatenate([total, pltpu.roll(total, shift, 1)], axis=0) / tau
        lane_no = lax.broadcasted_iota(jnp.int32, scores.shape, 1)
        target = lane_no == pos_ref[...]
        masked = jnp.where(lane_no < d_batch, scores, -jnp.inf)
        top = jnp.max(masked, axis=1, keepdims=True)
        log_norm = jnp.log(sum_lanes(jnp.exp(masked - top))) + top
        hit = sum_lanes(jnp.where(target, scores, 0.0))
        mine = sum_rows(log_norm - hit) / q_batch + reg
        grad = (jnp.exp(masked - log_norm) - target.astype(F32)) / (q_batch * tau)
        gmine[...] = grad[:hq] + pltpu.roll(grad[hq:], shift, 1)
        lmine[...] = jnp.broadcast_to(mine, lmine.shape)
        grads_out = broadcast(2, lambda slot: gmine, gall)
        for copy in grads_out:
            copy.start()
        losses_out = broadcast(3, lambda slot: lmine, lall)
        for copy in losses_out:
            copy.start()
        gall[core] = gmine[...]
        lall[core] = lmine[...]
        drd[...] = jnp.broadcast_to((2.0 * lam_d / d_batch) * d_mean, drd.shape)
        for copy in arrivals(2, gall):
            copy.wait_recv()

        def back(c, carry):
            at = pl.ds(c * chunk, chunk)
            grad_c = gall[at]
            grad_c = jnp.concatenate([grad_c, pltpu.roll(grad_c, shift, 2)], axis=1).reshape((chunk * n_q, 2 * shift))
            grad_c = exact_dot(grad_c, doc_place[...], TURNED)
            reps_c = rep[at, :n_q, :].reshape((chunk * n_q, geo.vocab))
            drd[...] += exact_dot(grad_c, reps_c, FIRST)
            drq = exact_dot(grad_c, rd[...])
            drq = drq + (2.0 * lam_q / q_batch) * q_mean
            rep[at, :n_q, :] = drq.reshape((chunk, n_q, geo.vocab))
            return carry

        lax.fori_loop(0, parts, back, 0)
        spread = exact_dot(pick[...], drd[...], FIRST)
        rep[:, n_q:rows, :] = spread.reshape((slots, rows - n_q, geo.vocab))
        for copy in arrivals(3, lall):
            copy.wait_recv()
        by_device = jnp.zeros((1, place.shape[1]), F32)
        for i in range(slots):
            by_device = by_device + lall[i] * place[i:i + 1, :]
        loss_ref[...] = jnp.broadcast_to(sum_lanes(by_device), loss_ref.shape)
        for copy in scores_out + grads_out + losses_out:
            copy.wait_send()

    def logit_sum(s, at):
        total = jnp.dot(net.tokens(s, 0), wv[0, :, at:at + part], preferred_element_type=F32)
        for lane in range(1, nd):
            total += jnp.dot(net.tokens(s, lane), wv[lane, :, at:at + part], preferred_element_type=F32)
        return total

    def logits_grad(s, half):
        cols = slice(half * part, (half + 1) * part)
        total = gb[:, cols]
        for rel in range(geo.chips):
            span = slice(rel * slab, (rel + 1) * slab)
            logits = zo[parity(s), span, cols] + zr[parity(s), span, cols] + bias[:, cols]
            inverse = 1.0 / (1.0 + logits)
            row = lax.rem(s - geo.hops(rel), rows)
            parts = []
            for cr in PAIR:
                at = 2 * rel + cr
                tok = slice(cr * unit, (cr + 1) * unit)
                grad_row = rep[at, pl.ds(row, 1), cols] * inverse[tok, :]
                grad_row = jnp.where(logits[tok, :] > 0.0, grad_row, 0.0) * mt[row, :, at:at + 1]
                total = total + grad_row
                parts.append(grad_row)
            dz[parity(s), span, cols] = jnp.concatenate(parts, axis=0).astype(BF16)
        gb[:, cols] = total
        dzt[cols, :] = dz[parity(s), :, cols].T

    def accumulate(s, at, count):
        for lane in range(nd):
            acc[lane, at:at + count, :] += jnp.dot(dzt[at:at + count, :], net.tokens(s, lane),
                                                   preferred_element_type=F32)

    def hidden_grad(s, lane):
        block = jnp.dot(dz[parity(s)], wt[lane], preferred_element_type=F32).astype(BF16)
        for rel in range(geo.chips):
            dsum[ring(s), lane, net.place(rel, lane), :] = block[rel * slab:(rel + 1) * slab, :]
        rs_copy(1, lane, s + 1).start()

    def grad_step(s, carry):
        for lane in range(nd):
            net.arrive(s, lane, False)
        for half in PAIR:
            zs[parity(s), :, half * part:(half + 1) * part] = logit_sum(s, vocab + half * part)
            z_copy(s, half).start()
        hidden_grad(s - 1, 0)
        zo[parity(s), :, :part] = logit_sum(s, 0)
        z_copy(s, 0).wait()
        logits_grad(s, 0)
        zo[parity(s), :, part:vocab] = logit_sum(s, part)
        dz_copy(s, 0, True).start()
        dz_copy(s, 0, False).start()
        z_copy(s, 1).wait()
        logits_grad(s, 1)
        accumulate(s, 0, part)
        dz_copy(s, 1, True).start()
        dz_copy(s, 1, False).start()
        hidden_grad(s - 1, 1)
        merge_rest(s)
        accumulate(s, part, part)
        finish(s)
        start_rest(s)
        for half in PAIR:
            dz_copy(s, half, True).wait()
        merge_first(s)
        accumulate(s, vocab, vocab)
        for lane in range(nd):
            net.release(s, lane, False)
            rs_copy(2, lane, s).start()
        for lane in range(2, nd):
            hidden_grad(s - 1, lane)
        for half in PAIR:
            dz_copy(s, half, False).wait()
        return carry

    def wout(lane):
        return pltpu.make_async_copy(
            wv.at[lane, :, pl.ds(0, vocab)],
            gw_hbm.at[pl.ds(pl.multiple_of(half_at[0] + lane * width, width), width), :], wout_sem.at[lane])

    def wout_cross(lane):
        return pltpu.make_async_remote_copy(
            src_ref=wv.at[lane, :, pl.ds(vocab, vocab)],
            dst_ref=gw_hbm.at[pl.ds(pl.multiple_of(half_at[0] + lane * width, width), width), :],
            send_sem=wo_send.at[lane], recv_sem=wo_recv.at[lane], device_id=net.sib, device_id_type=MESH)

    def store_weights(lane):
        for half in PAIR:
            span = slice(half * vocab, (half + 1) * vocab)
            wv[lane, :, span] = acc[lane, span, :].astype(BF16).T
        wout(lane).start()
        wout_cross(lane).start()

    def flush():
        end = steps
        merge_rest(end)
        finish(end)
        start_rest(end)
        merge_first(end)
        for lane in range(nd):
            rs_copy(2, lane, end).start()
            hidden_grad(end - 1, lane)
        store_weights(0)

        end += 1
        merge_rest(end)
        finish(end)
        start_rest(end)
        merge_first(end)
        for lane in range(nd):
            rs_copy(2, lane, end).start()
            flush_copy(0, lane).start()

        end += 1
        for lane in range(nd):
            for stage_no in later:
                rs_copy(stage_no, lane, end - 1).wait()
            flush_copy(0, lane).wait()
        for lane in range(nd):
            m3[ring(end), lane] = merged(3, lane, end, m2[ring(end + 1), lane, :low[3]]).astype(BF16)
            m2[ring(end), lane] = merged(2, lane, end, m1[ring(end + 1), lane, :low[2]]).astype(BF16)
            last[lane] = merged(4, lane, end, m3[ring(end + 1), lane, :low[4]])
            dsum[spare, lane, :low[2], :] = (x2[lane].astype(F32)
                                          + m1[ring(end + 2), lane, :low[2]].astype(F32)).astype(BF16)
            rs_copy(3, lane, end).start()
            rs_copy(4, lane, end).start()
            flush_copy(1, lane).start()
            flush_copy(2, lane).start()
        finish(end)
        store_weights(1)

        end += 1
        for lane in range(nd):
            for stage_no in range(3, 5):
                rs_copy(stage_no, lane, end - 1).wait()
            flush_copy(1, lane).wait()
            flush_copy(2, lane).wait()
        for lane in range(nd):
            last[lane] = merged(4, lane, end, m3[ring(end + 1), lane, :low[4]])
            m3[ring(end), lane] = merged(3, lane, end, m2[ring(end + 1), lane, :low[3]]).astype(BF16)
            dsum[spare, lane, low[2]:deep[1], :] = (
                x3[0, lane].astype(F32) + m2[ring(end + 2), lane, :low[3]].astype(F32)).astype(BF16)
            dsum[spare, lane, deep[1]:low[1], :] = (
                x3[1, lane].astype(F32) + dsum[spare, lane, :low[3], :].astype(F32)).astype(BF16)
            rs_copy(4, lane, end).start()
            for i in range(3, 6):
                flush_copy(i, lane).start()
        finish(end)
        store_weights(2)

        end += 1
        for lane in range(nd):
            rs_copy(4, lane, end - 1).wait()
            for i in range(3, 6):
                flush_copy(i, lane).wait()
        for lane in range(nd):
            own3 = (m3[ring(end + 1), lane, :low[4]], m3[ring(end + 2), lane, :low[4]],
                    dsum[spare, lane, low[2]:deep[0], :],
                    dsum[spare, lane, deep[1]:deep[2], :])
            got4 = (r4[parity(end + 1), lane], x4[0, lane], x4[1, lane], x4[2, lane])
            for i in range(nd + 1):
                total = dsum[tail, lane, :low[4], :].astype(F32)
                if i < nd:
                    total = got4[i].astype(F32) + own3[i].astype(F32)
                if i > 0:
                    total = total + early[i - 1, lane]
                emit(lane, end + i, total, 2 + i)
        out_copy(end - 1, parity(end - 1)).wait()
        for i in range(nd + 1):
            out_copy(end + i, 2 + i).start()
        store_weights(3)
        for i in range(nd + 1):
            out_copy(end + i, 2 + i).wait()

    net.begun()
    lax.fori_loop(1, first, loss_step, 0)
    for lane in range(1, nd):
        net.release(first - 1, lane, True)
    for lane in range(nd):
        for stage_no in range(1, 5):
            rs_copy(stage_no, lane, first - 1).start()
    reps(first - 1)
    softmax()
    lax.fori_loop(first, steps, grad_step, 0)
    flush()
    gb_ref[...] = sum_rows(gb[...])
    stores = []
    for half in PAIR:
        cols = pl.ds(half_at[half], geo.half)
        stores.append(pltpu.make_async_copy(gout.at[half, pl.ds(0, n_q)], gq_hbm.at[:, :, cols], hout_sem.at[half, 0]))
        stores.append(pltpu.make_async_copy(gout.at[half, pl.ds(n_q, n_dp)], gd_hbm.at[:, :, cols],
                                            hout_sem.at[half, 1]))
    for copy in stores:
        copy.start()
    for copy in stores:
        copy.wait()
    for lane in range(nd):
        wout(lane).wait()
        wout_cross(lane).wait()


def call_fused(geo, const, q_rows, d_rows, w_head, bias, mrow, positive, place, doc_place, pick):
    bufs, sems = gather_scratch(geo)
    dma = pltpu.SemaphoreType.DMA
    nd, tok, width, vocab, rows = geo.nd, geo.tokens, geo.width, geo.vocab, geo.rows
    n_q, docs, slots = const[0], doc_place.shape[0], 2 * geo.chips
    lanes = doc_place.shape[1]
    hq = n_q // 2
    hbm, vmem = pl.BlockSpec(memory_space=pl.ANY), pl.BlockSpec(memory_space=pltpu.VMEM)
    logit = pltpu.VMEM((2, tok, vocab), F32)
    scratch = bufs + [
        pltpu.VMEM((nd, width, 2 * vocab), BF16), pltpu.VMEM((nd, 2 * vocab, width), BF16),
        pltpu.VMEM((nd, 2 * vocab, width), F32), logit, logit, logit,
        pltpu.VMEM((2, tok, 2 * vocab), BF16), pltpu.VMEM((2 * vocab, tok), BF16),
        pltpu.VMEM((3, nd, tok, width), BF16),
        pltpu.VMEM((3, nd, tok // 2, width), BF16), pltpu.VMEM((3, nd, tok // 4, width), BF16),
        pltpu.VMEM((3, nd, tok // 8, width), BF16),
        pltpu.VMEM((2, nd, tok // 2, width), BF16), pltpu.VMEM((2, nd, tok // 4, width), BF16),
        pltpu.VMEM((2, nd, tok // 8, width), BF16), pltpu.VMEM((2, nd, tok // 16, width), BF16),
        pltpu.VMEM((nd, tok // 4, width), BF16), pltpu.VMEM((2, nd, tok // 8, width), BF16),
        pltpu.VMEM((3, nd, tok // 16, width), BF16),
        pltpu.VMEM((nd + 3, geo.unit, geo.half), BF16), pltpu.VMEM((2, rows, geo.unit, geo.half), BF16),
        pltpu.VMEM((nd, nd, geo.slab, width), F32), pltpu.VMEM((nd, geo.slab, width), F32),
        pltpu.VMEM((geo.unit, vocab), F32),
        pltpu.VMEM((slots, rows, vocab), F32), pltpu.VMEM((docs, vocab), F32), pltpu.VMEM((docs, vocab), F32),
        pltpu.VMEM((slots,) + mrow.shape, F32), pltpu.VMEM((mrow.shape[1] // geo.unit, geo.unit, 128), F32),
        pltpu.VMEM((slots, hq, lanes), F32), pltpu.VMEM((slots, hq, lanes), F32),
        pltpu.VMEM((hq, lanes), F32), pltpu.VMEM((slots, hq, lanes), F32),
        pltpu.VMEM((1, lanes), F32), pltpu.VMEM((slots, 1, lanes), F32),
        dma((4,)), dma((nd,)), dma((nd,)), dma((nd,)), dma((2, 2)), dma((2, 2)), dma((2, 2)), dma((2, 2)),
        dma((4, nd, 2)), dma((4, nd, 2)), dma((6, nd)), dma((6, nd)), dma((nd + 3,)), dma((nd + 3,)), dma((nd,)), dma((nd,)),
        dma((nd,)), dma((2, 2)), dma((4, slots)), dma((4, slots))] + sems
    return pl.pallas_call(
        functools.partial(fused_kernel, geo, const),
        name="lexical_head",
        out_shape=[jax.ShapeDtypeStruct((1, lanes), F32), jax.ShapeDtypeStruct(w_head.shape, BF16),
                   jax.ShapeDtypeStruct((1, vocab), F32), jax.ShapeDtypeStruct(q_rows.shape, BF16),
                   jax.ShapeDtypeStruct(d_rows.shape, BF16)],
        in_specs=[hbm, hbm, hbm] + [vmem] * 6,
        out_specs=[vmem, hbm, vmem, hbm, hbm],
        scratch_shapes=scratch,
        compiler_params=pltpu.CompilerParams(collective_id=0, has_side_effects=True, vmem_limit_bytes=VMEM_LIMIT),
    )(q_rows, d_rows, w_head, bias, mrow, positive, place, doc_place, pick)


def solution(mesh):
    n_group = mesh.shape['tp']
    row_spec = P(('dp', 'tp'))
    mask_spec = P(('dp', 'tp'), None)
    hid_spec = P(('dp', 'tp'), None, None)

    def local_step(q_hidden, d_hidden, q_mask, d_mask, positive, w_head, b_head):
        hidden_size, vocab_loc = w_head.shape
        vocab_size = vocab_loc * n_group
        n_q, q_len, _ = q_hidden.shape
        n_d, d_len, _ = d_hidden.shape
        pieces = d_len // q_len
        q_batch, d_batch = n_q * n_group, n_d * n_group
        tau = q_len * math.sqrt(vocab_size * d_len) / 16.0
        lam_q = 4.0 / (vocab_size * q_len * q_len)
        lam_d = 4.0 / (vocab_size * d_len * d_len)
        rows = n_q + n_d * pieces
        geo = Geometry(n_group, rows, hidden_size, vocab_loc, q_len)
        side, slots = geo.side, 2 * geo.chips
        lanes = max(128, 2 * d_batch)

        me = lax.axis_index('tp')
        slot = jnp.arange(slots)
        chip, rel = me // 2, slot // 2
        step_x, step_y = rel % side, rel // side
        chip_of = (((chip // side) ^ step_y ^ (step_y >> 1)) * side + ((chip % side) ^ step_x ^ (step_x >> 1)))
        device_of = chip_of * 2 + slot % 2
        place = jax.nn.one_hot(device_of, lanes, dtype=F32)
        doc_of = jnp.add.outer(jnp.arange(n_d), device_of * n_d).reshape((n_d * slots,))
        doc_place = jax.nn.one_hot(doc_of, lanes, dtype=F32)
        pick = np.concatenate([np.kron(np.eye(slots), np.repeat(row, pieces)) for row in np.eye(n_d)])

        own_mask = jnp.concatenate([q_mask.reshape((-1,)), d_mask.reshape((-1,))]).astype(F32)
        mrow = jnp.pad(own_mask, (0, -own_mask.shape[0] % 128)).reshape((1, -1))
        const = (n_q, n_d, lam_q, lam_d, tau, float(q_batch), float(d_batch))
        loss, grad_w, grad_b, grad_q, grad_d = call_fused(
            geo, const, q_hidden, d_hidden.reshape((n_d * pieces, q_len, hidden_size)), w_head,
            b_head.reshape((1, vocab_loc)), mrow, positive.reshape((n_q, 1)), place, doc_place, jnp.asarray(pick, F32))
        return (loss[0, 0:1], grad_w, grad_b.reshape((vocab_loc,)), grad_q, grad_d.reshape(d_hidden.shape))

    return jax.shard_map(local_step, mesh=mesh,
                         in_specs=(hid_spec, hid_spec, mask_spec, mask_spec, row_spec, P(None, 'tp'), P('tp')),
                         out_specs=(P('dp'), P('dp', 'tp'), row_spec, hid_spec, hid_spec),
                         check_vma=False)
```

```python
import functools
import math

import jax
import jax.numpy as jnp
import numpy as np
from jax import lax
from jax.experimental import pallas as pl
from jax.experimental.pallas import tpu as pltpu
from jax.sharding import PartitionSpec as P

MESH = pl.DeviceIdType.MESH
F32 = jnp.float32
BF16 = jnp.bfloat16
VMEM_LIMIT = 67043328
PAIR = range(2)
HIGHEST = lax.Precision.HIGHEST


def parity(s):
    return lax.rem(s, 2)


def ring(s):
    return lax.rem(s, 3)


def sum_rows(x):
    return jnp.sum(x, axis=0, keepdims=True)


def sum_lanes(x):
    return jnp.sum(x, axis=1, keepdims=True)


def exact_dot(a, b, dims=(((1,), (0,)), ((), ()))):
    return lax.dot_general(a, b, dims, precision=HIGHEST, preferred_element_type=F32)


TURNED = (((1,), (1,)), ((), ()))
FIRST = (((0,), (0,)), ((), ()))


class Geometry:
    def __init__(self, n_group, rows, hidden, vocab, unit):
        self.side = math.isqrt(n_group // 2)
        self.nd = 2 * (self.side.bit_length() - 1)
        self.chips = 1 << self.nd
        assert self.side == 4 and self.chips * 2 == n_group
        self.rows = rows
        self.first = self.nd + rows
        self.steps = self.first + rows
        self.unit = unit
        self.slab = 2 * unit
        self.tokens = self.slab * self.chips
        self.half = hidden // 2
        self.width = self.half // self.nd
        self.vocab = vocab

    def hops(self, rel):
        return bin(rel).count("1")

    def slot(self, rel, lane):
        return ((rel >> lane) | (rel << (self.nd - lane))) & (self.chips - 1)

    def device(self, me, rel, core):
        chip = lax.div(me, 2)
        x, y = lax.rem(chip, self.side), lax.div(chip, self.side)
        at = [x, y]
        for dim in range(self.nd):
            if rel >> dim & 1:
                axis, wide = divmod(dim, len(at))
                at[axis] = self.side - 1 - at[axis] if wide else at[axis] + 1 - 2 * lax.rem(at[axis], 2)
        x, y = at
        return {"tp": (y * self.side + x) * 2 + core}

    def peer(self, me, dim, core):
        return self.device(me, 1 << dim, core)


def entry_barrier(peers):
    barrier = pltpu.get_barrier_semaphore()
    for device in peers:
        pl.semaphore_signal(barrier, inc=1, device_id=device, device_id_type=MESH)
    pl.semaphore_wait(barrier, len(peers))


class Gather:
    def __init__(self, geo, me, x, stage, ownx, sems):
        (self.ici_send, self.ici_recv, self.piece_send, self.piece_recv, self.free_ici, self.free_piece) = sems
        self.geo, self.x, self.stage, self.ownx = geo, x, stage, ownx
        self.core = lax.rem(me, 2)
        self.sib = {"tp": me + 1 - 2 * self.core}
        dims = [geo.peer(me, dim, self.core)["tp"] for dim in range(geo.nd)]
        turn = geo.nd // 2
        self.same = [{"tp": dims[d] + self.core * (dims[(d + turn) % geo.nd] - dims[d])} for d in range(geo.nd)]

    def place(self, rel, lane):
        geo = self.geo
        one = geo.slot(rel, lane) * geo.slab
        two = geo.slot(rel, (lane + geo.nd // 2) % geo.nd) * geo.slab
        if one == two:
            return pl.ds(one, geo.slab)
        return pl.ds(pl.multiple_of(one + self.core * (two - one), geo.slab), geo.slab)

    def ici(self, s, lane, pos):
        count = (1 << pos) * self.geo.slab
        here, there = parity(s), parity(s + 1)
        return pltpu.make_async_remote_copy(
            src_ref=self.x.at[here, lane, pl.ds(0, count)], dst_ref=self.x.at[there, lane, pl.ds(count, count)],
            send_sem=self.ici_send.at[lane, pos, there], recv_sem=self.ici_recv.at[lane, pos, there],
            device_id=self.same[(lane + pos) % self.geo.nd], device_id_type=MESH)

    def piece(self, s, lane):
        width = self.geo.width
        return pltpu.make_async_remote_copy(
            src_ref=self.ownx.at[1, lax.rem(s, self.geo.rows), :, pl.ds(lane * width, width)],
            dst_ref=self.stage.at[parity(s), lane], send_sem=self.piece_send.at[lane, parity(s)],
            recv_sem=self.piece_recv.at[lane, parity(s)], device_id=self.sib, device_id_type=MESH)

    def inject(self, s, lane):
        geo = self.geo
        width = geo.width
        self.piece(s, lane).wait()
        mine = self.ownx[0, lax.rem(s, geo.rows), :, lane * width:(lane + 1) * width].astype(F32)
        theirs = self.stage[parity(s), lane].astype(F32)
        first = jnp.where(self.core == 0, mine, theirs)
        second = jnp.where(self.core == 0, theirs, mine)
        self.x[parity(s), lane, :geo.slab, :] = jnp.concatenate([first, second], axis=0).astype(BF16)

    def begin(self):
        geo = self.geo
        for lane in range(geo.nd):
            self.inject(0, lane)
            for pos in range(geo.nd):
                self.first(lane, pos).start()
            self.piece(1, lane).start()

    def begun(self):
        geo = self.geo
        for lane in range(geo.nd):
            for pos in range(geo.nd):
                self.first(lane, pos).wait_send()
            self.grant(lane)
        for lane in range(geo.nd):
            for pos in range(geo.nd):
                self.first(lane, pos).wait_recv()

    def first(self, lane, pos):
        geo = self.geo
        return pltpu.make_async_remote_copy(
            src_ref=self.x.at[0, lane, pl.ds(0, geo.slab)],
            dst_ref=self.x.at[1, lane, pl.ds((1 << pos) * geo.slab, geo.slab)],
            send_sem=self.ici_send.at[lane, pos, 1], recv_sem=self.ici_recv.at[lane, pos, 1],
            device_id=self.same[(lane + pos) % geo.nd], device_id_type=MESH)

    def arrive(self, s, lane, loss):
        geo = self.geo
        self.inject(s, lane)

        if loss:
            @pl.when(s > 1)
            def _():
                self.receive(s, lane)
        else:
            self.receive(s, lane)
        self.credits(lane)
        for pos in reversed(range(geo.nd)):
            self.ici(s, lane, pos).start()
        self.piece(s + 1, lane).start()

    def receive(self, s, lane):
        for pos in range(self.geo.nd):
            self.ici(s - 1, lane, pos).wait_recv()

    def credits(self, lane):
        pl.semaphore_wait(self.free_piece.at[lane], 1)
        for pos in range(self.geo.nd):
            pl.semaphore_wait(self.free_ici.at[lane, pos], 1)

    def grant(self, lane):
        geo = self.geo
        for pos in range(geo.nd):
            pl.semaphore_signal(self.free_ici.at[lane, pos], inc=1,
                                device_id=self.same[(lane + pos) % geo.nd], device_id_type=MESH)
        pl.semaphore_signal(self.free_piece.at[lane], inc=1, device_id=self.sib, device_id_type=MESH)

    def release(self, s, lane):
        for pos in range(self.geo.nd):
            self.ici(s, lane, pos).wait_send()
        self.grant(lane)

    def end(self, s):
        for lane in range(self.geo.nd):
            self.receive(s, lane)
            self.credits(lane)
            self.piece(s, lane).wait()

    def tokens(self, s, lane):
        geo = self.geo
        return jnp.concatenate([self.x[parity(s), lane, self.place(rel, lane), :] for rel in range(geo.chips)], axis=0)


def gather_scratch(geo):
    nd = geo.nd
    bufs = [pltpu.VMEM((2, nd, geo.tokens, geo.width), BF16), pltpu.VMEM((2, nd, geo.unit, geo.width), BF16),
            pltpu.VMEM((2, geo.rows, geo.unit, geo.half), BF16)]
    dma, reg = pltpu.SemaphoreType.DMA, pltpu.SemaphoreType.REGULAR
    sems = [dma((nd, nd, 2)), dma((nd, nd, 2)), dma((nd, 2)), dma((nd, 2)), reg((nd, nd)), reg((nd,))]
    return bufs, sems


def all_peers(geo, me):
    core = lax.rem(me, 2)
    found = [(0, 1 - core, geo.device(me, 0, 1 - core))]
    for rel in range(1, geo.chips):
        for other in PAIR:
            found.append((rel, other, geo.device(me, rel, other)))
    return found


def fused_kernel(geo, const, q_hbm, d_hbm, w_hbm, bias, mrow, tables, pick,
                 loss_ref, gw_hbm, gb_ref, gq_hbm, gd_hbm,
                 x, stage, ownx, wv, wt, acc, zo, zs, zr, dz, dzt, dsum, m1, m2, m3,
                 r1, r2, r3, r4, x2, x3, x4, ost, gout, early, last, gb, rep, rd, drd, mall, mt, sbuf, pall, gmine, gall,
                 lmine, lall,
                 own_sem, w_sem, wx_send, wx_recv, z_send, z_recv, dz_send, dz_recv, rs_send, rs_recv, fl_send, fl_recv,
                 out_send, out_recv, wout_sem, wo_send, wo_recv, hout_sem, ex_send, ex_recv, *sems):
    nd, slab, unit, width, steps, rows, first = (geo.nd, geo.slab, geo.unit, geo.width, geo.steps, geo.rows,
                                                 geo.first)
    n_q, n_d, lam_q, lam_d, tau, q_batch, d_batch = const
    slots, vocab = 2 * geo.chips, geo.vocab
    me = lax.axis_index("tp")
    net = Gather(geo, me, x, stage, ownx, sems)
    core, same = net.core, net.same
    docs = n_d * slots
    place, doc_place, target = tables.at[:slots], tables.at[pl.ds(slots, docs)], tables.at[pl.ds(slots + docs, n_q)]
    peers = all_peers(geo, me)
    half_at = [pl.multiple_of(core * geo.half, geo.half), pl.multiple_of((1 - core) * geo.half, geo.half)]

    n_dp = d_hbm.shape[0]
    own_loads = []
    for half in PAIR:
        cols = pl.ds(half_at[half], geo.half)
        own_loads.append(pltpu.make_async_copy(q_hbm.at[:, :, cols], ownx.at[half, pl.ds(0, n_q)],
                                               own_sem.at[2 * half]))
        own_loads.append(pltpu.make_async_copy(d_hbm.at[:, :, cols], ownx.at[half, pl.ds(n_q, n_dp)],
                                               own_sem.at[2 * half + 1]))
    w_loads, w_cross = [], []
    for lane in range(nd):
        here = pl.ds(pl.multiple_of(half_at[0] + lane * width, width), width)
        there = pl.ds(pl.multiple_of(half_at[1] + lane * width, width), width)
        w_loads.append(pltpu.make_async_copy(w_hbm.at[here, :], wv.at[lane, :, pl.ds(0, vocab)], w_sem.at[lane]))
        w_cross.append(pltpu.make_async_remote_copy(
            src_ref=w_hbm.at[there, :], dst_ref=wv.at[lane, :, pl.ds(vocab, vocab)], send_sem=wx_send.at[lane],
            recv_sem=wx_recv.at[lane], device_id=net.sib, device_id_type=MESH))
    for copy in own_loads + w_loads:
        copy.start()
    entry_barrier([device for _, _, device in peers])
    for copy in own_loads:
        copy.wait()
    for lane in range(nd):
        net.piece(0, lane).start()
    net.begin()

    def broadcast(kind, src_of, dst):
        return [pltpu.make_async_remote_copy(
            src_ref=src_of(2 * rel + other), dst_ref=dst.at[2 * rel + core],
            send_sem=ex_send.at[kind, i], recv_sem=ex_recv.at[kind, 2 * rel + core], device_id=device,
            device_id_type=MESH) for i, (rel, other, device) in enumerate(peers)]

    def arrivals(kind, dst):
        return [pltpu.make_async_remote_copy(
            src_ref=dst.at[2 * rel + other], dst_ref=dst.at[2 * rel + other],
            send_sem=ex_send.at[kind, i], recv_sem=ex_recv.at[kind, 2 * rel + other], device_id=device,
            device_id_type=MESH) for i, (rel, other, device) in enumerate(peers)]

    masks_out = broadcast(0, lambda slot: mrow, mall)
    for copy in masks_out:
        copy.start()
    mall[core] = mrow[...]
    for copy in w_cross:
        copy.start()
    gb[...] = jnp.zeros_like(gb)
    for ref in (dsum, m1, m2, m3, dz):
        ref[...] = jnp.zeros_like(ref)

    part = vocab // 2

    def z_copy(s, half):
        cols = pl.ds(half * part, part)
        return pltpu.make_async_remote_copy(
            src_ref=zs.at[parity(s), :, cols], dst_ref=zr.at[parity(s), :, cols], send_sem=z_send.at[parity(s), half],
            recv_sem=z_recv.at[parity(s), half], device_id=net.sib, device_id_type=MESH)

    def dz_copy(s, half, turned):
        here, there = pl.ds(half * part, part), pl.ds(vocab + half * part, part)
        src, dst = dzt.at[here], dzt.at[there]
        if not turned:
            src, dst = dz.at[parity(s), :, here], dz.at[parity(s), :, there]
        return pltpu.make_async_remote_copy(
            src_ref=src, dst_ref=dst, send_sem=dz_send.at[half, int(turned)], recv_sem=dz_recv.at[half, int(turned)],
            device_id=net.sib, device_id_type=MESH)

    def rs_copy(stage_no, lane, s):
        n_low = geo.tokens >> stage_no
        src = dsum.at[ring(s + 2), lane, pl.ds(n_low, n_low)]
        if stage_no > 1:
            src = (m1, m2, m3)[stage_no - 2].at[ring(s), lane, pl.ds(n_low, n_low)]
        dst = (r1, r2, r3, r4)[stage_no - 1].at[parity(s), lane]
        return pltpu.make_async_remote_copy(
            src_ref=src, dst_ref=dst, send_sem=rs_send.at[stage_no - 1, lane, parity(s)],
            recv_sem=rs_recv.at[stage_no - 1, lane, parity(s)],
            device_id=same[(lane + nd - stage_no) % nd], device_id_type=MESH)

    low = [geo.tokens >> k for k in range(5)]
    deep = (low[2] + low[4], low[2] + low[3], low[2] + low[3] + low[4])
    later = (2, 3, 4)
    tail, spare = (steps - 1) % 3, steps % 3

    def flush_copy(i, lane):
        src, dst, stage_no = (
            (dsum.at[tail, lane, pl.ds(low[2], low[2])], x2.at[lane], 2),
            (dsum.at[spare, lane, pl.ds(low[3], low[3])], x3.at[0, lane], 3),
            (dsum.at[tail, lane, pl.ds(low[3], low[3])], x3.at[1, lane], 3),
            (dsum.at[spare, lane, pl.ds(deep[0], low[4])], x4.at[0, lane], 4),
            (dsum.at[spare, lane, pl.ds(deep[2], low[4])], x4.at[1, lane], 4),
            (dsum.at[tail, lane, pl.ds(low[4], low[4])], x4.at[2, lane], 4))[i]
        return pltpu.make_async_remote_copy(
            src_ref=src, dst_ref=dst, send_sem=fl_send.at[i, lane], recv_sem=fl_recv.at[i, lane],
            device_id=same[(lane + nd - stage_no) % nd], device_id_type=MESH)

    def out_copy(s, at):
        return pltpu.make_async_remote_copy(
            src_ref=ost.at[at], dst_ref=gout.at[1, lax.rem(s - 9, rows)], send_sem=out_send.at[at],
            recv_sem=out_recv.at[at], device_id=net.sib, device_id_type=MESH)

    def emit(lane, s, total, at):
        cols = slice(lane * width, (lane + 1) * width)
        one, two = total[:unit], total[unit:slab]
        gout[0, lax.rem(s - 9, rows), :, cols] = jnp.where(core == 0, one, two).astype(BF16)
        ost[at, :, cols] = jnp.where(core == 0, two, one).astype(BF16)

    def merged(stage_no, lane, s, mine):
        got = (r1, r2, r3, r4)[stage_no - 1][parity(s + 1), lane].astype(F32)
        return got + mine.astype(F32)

    def merge_first(s):
        for lane in range(nd):
            rs_copy(1, lane, s - 1).wait()
        for lane in range(nd):
            m1[ring(s), lane] = merged(1, lane, s, dsum[ring(s), lane, :low[1]]).astype(BF16)

    def merge_rest(s):
        back = ring(s + 1)
        for lane in range(nd):
            for stage_no in later:
                rs_copy(stage_no, lane, s - 1).wait()
        for lane in range(nd):
            m2[ring(s), lane] = merged(2, lane, s, m1[back, lane, :low[2]]).astype(BF16)
            m3[ring(s), lane] = merged(3, lane, s, m2[back, lane, :low[3]]).astype(BF16)
            last[lane] = merged(4, lane, s, m3[back, lane, :low[4]])

    def finish(s):
        @pl.when((s >= first + 5) & (s < first + 9))
        def _():
            early[lax.rem(s - first - 5, nd)] = last[...]

        @pl.when(s >= first + 9)
        def _():
            for lane in range(nd):
                emit(lane, s, last[lane], parity(s))

        @pl.when(s >= first + 10)
        def _():
            out_copy(s - 1, parity(s + 1)).wait()

        @pl.when(s >= first + 9)
        def _():
            out_copy(s, parity(s)).start()

    def start_rest(s):
        for lane in range(nd):
            rs_copy(3, lane, s).start()
            rs_copy(4, lane, s).start()

    def logits_part(s, lane):
        tokens = net.tokens(s, lane)
        for ref, at in ((zs, vocab), (zo, 0)):
            part = jnp.dot(tokens, wv[lane, :, at:at + vocab], preferred_element_type=F32)
            if lane == 0:
                ref[parity(s)] = part
            else:
                ref[parity(s)] = ref[parity(s)] + part

    def reps(s):
        for half in PAIR:
            z_copy(s, half).wait()
        for rel in range(geo.chips):
            span = slice(rel * slab, (rel + 1) * slab)
            logits = zo[parity(s), span, :] + zr[parity(s), span, :] + bias[...]
            active = jnp.log1p(jnp.maximum(logits, 0.0))
            row = lax.rem(s - geo.hops(rel), rows)
            for cr in PAIR:
                at = 2 * rel + cr
                part = active[cr * unit:(cr + 1) * unit, :] * mt[row, :, at:at + 1]
                rep[at, pl.ds(row, 1), :] = sum_rows(part)

    def prepare(s):
        @pl.when(s == 1)
        def _():
            for copy in w_loads:
                copy.wait()
            for copy in arrivals(0, mall):
                copy.wait_recv()
            for copy in masks_out:
                copy.wait_send()
            table = jnp.concatenate([mall[i] for i in range(slots)], axis=0)
            table = jnp.concatenate([table, jnp.zeros((128 - slots, table.shape[1]), F32)], axis=0)
            mt[...] = table.T.reshape(mt.shape)

        @pl.when(s == 2)
        def _():
            for copy in w_cross:
                copy.wait()

        @pl.when((s >= 2) & (s < 2 + nd))
        def _():
            def turn(half, carry):
                span = pl.ds(pl.multiple_of(half * vocab, vocab), vocab)
                acc[s - 2, span, :] = jnp.zeros((vocab, width), F32)
                wt[s - 2, span, :] = wv[s - 2, :, span].T
                return carry

            lax.fori_loop(0, 2, turn, 0)

    def loss_step(s, carry):
        prepare(s)
        for lane in range(nd):
            if lane == nd - 1:
                net.release(s, 0)
            else:
                @pl.when(s > 1)
                def _():
                    net.release(s - 1, lane + 1)

            net.arrive(s, lane, True)

            @pl.when(s >= nd)
            def _():
                logits_part(s, lane)

            if lane == 1:
                @pl.when(s > nd)
                def _():
                    reps(s - 1)

        @pl.when(s >= nd)
        def _():
            for half in PAIR:
                z_copy(s, half).start()
        return carry

    def softmax():
        chunk = 16
        hq = n_q // 2
        shift = loss_ref.shape[1] // 2
        parts = slots // chunk
        pieces = rep[:, n_q:rows, :].reshape((slots * (rows - n_q), geo.vocab))
        rd[...] = exact_dot(pick[...], pieces)

        def score(c, q_sum):
            at = pl.ds(c * chunk, chunk)
            reps_c = rep[at, :n_q, :].reshape((chunk * n_q, geo.vocab))
            part = exact_dot(reps_c, rd[...], TURNED)
            part = exact_dot(part, doc_place[...])
            part = part.reshape((chunk, n_q, part.shape[1]))
            sbuf[at] = part[:, :hq] + pltpu.roll(part[:, hq:], shift, 2)
            return q_sum + sum_rows(reps_c)

        q_sum = lax.fori_loop(0, parts, score, jnp.zeros((1, geo.vocab), F32))
        scores_out = broadcast(1, lambda slot: sbuf.at[slot], pall)
        for copy in scores_out:
            copy.start()
        pall[core] = sbuf[core]
        q_mean = q_sum / q_batch
        d_mean = sum_rows(rd[...]) / d_batch
        reg = (lam_q * sum_lanes(q_mean * q_mean)
               + lam_d * sum_lanes(d_mean * d_mean))
        for copy in arrivals(1, pall):
            copy.wait_recv()
        total = pall[0]
        for i in range(1, slots):
            total = total + pall[i]
        scores = jnp.concatenate([total, pltpu.roll(total, shift, 1)], axis=0) / tau
        lane_no = lax.broadcasted_iota(jnp.int32, scores.shape, 1)
        masked = jnp.where(lane_no < d_batch, scores, -jnp.inf)
        top = jnp.max(masked, axis=1, keepdims=True)
        log_norm = jnp.log(sum_lanes(jnp.exp(masked - top))) + top
        hit = sum_lanes(target[...] * scores)
        mine = sum_rows(log_norm - hit) / q_batch + reg
        grad = (jnp.exp(masked - log_norm) - target[...]) / (q_batch * tau)
        gmine[...] = grad[:hq] + pltpu.roll(grad[hq:], shift, 1)
        lmine[...] = jnp.broadcast_to(mine, lmine.shape)
        grads_out = broadcast(2, lambda slot: gmine, gall)
        for copy in grads_out:
            copy.start()
        losses_out = broadcast(3, lambda slot: lmine, lall)
        for copy in losses_out:
            copy.start()
        gall[core] = gmine[...]
        lall[core] = lmine[...]
        drd[...] = jnp.broadcast_to((2.0 * lam_d / d_batch) * d_mean, drd.shape)
        for copy in arrivals(2, gall):
            copy.wait_recv()

        def back(c, carry):
            at = pl.ds(c * chunk, chunk)
            grad_c = gall[at]
            grad_c = jnp.concatenate([grad_c, pltpu.roll(grad_c, shift, 2)], axis=1).reshape((chunk * n_q, 2 * shift))
            grad_c = exact_dot(grad_c, doc_place[...], TURNED)
            reps_c = rep[at, :n_q, :].reshape((chunk * n_q, geo.vocab))
            drd[...] += exact_dot(grad_c, reps_c, FIRST)
            drq = exact_dot(grad_c, rd[...])
            drq = drq + (2.0 * lam_q / q_batch) * q_mean
            rep[at, :n_q, :] = drq.reshape((chunk, n_q, geo.vocab))
            return carry

        lax.fori_loop(0, parts, back, 0)
        spread = exact_dot(pick[...], drd[...], FIRST)
        rep[:, n_q:rows, :] = spread.reshape((slots, rows - n_q, geo.vocab))
        for copy in arrivals(3, lall):
            copy.wait_recv()
        by_device = jnp.zeros((1, place.shape[1]), F32)
        for i in range(slots):
            by_device = by_device + lall[i] * place[i:i + 1, :]
        loss_ref[...] = jnp.broadcast_to(sum_lanes(by_device), loss_ref.shape)
        for copy in scores_out + grads_out + losses_out:
            copy.wait_send()

    def logit_sum(s, at):
        total = jnp.dot(net.tokens(s, 0), wv[0, :, at:at + part], preferred_element_type=F32)
        for lane in range(1, nd):
            total += jnp.dot(net.tokens(s, lane), wv[lane, :, at:at + part], preferred_element_type=F32)
        return total

    def logits_grad(s, half):
        cols = slice(half * part, (half + 1) * part)
        total = gb[:, cols]
        for rel in range(geo.chips):
            span = slice(rel * slab, (rel + 1) * slab)
            logits = zo[parity(s), span, cols] + zr[parity(s), span, cols] + bias[:, cols]
            inverse = 1.0 / (1.0 + logits)
            row = lax.rem(s - geo.hops(rel), rows)
            parts = []
            for cr in PAIR:
                at = 2 * rel + cr
                tok = slice(cr * unit, (cr + 1) * unit)
                grad_row = rep[at, pl.ds(row, 1), cols] * inverse[tok, :]
                grad_row = jnp.where(logits[tok, :] > 0.0, grad_row, 0.0) * mt[row, :, at:at + 1]
                total = total + grad_row
                parts.append(grad_row)
            dz[parity(s), span, cols] = jnp.concatenate(parts, axis=0).astype(BF16)
        gb[:, cols] = total
        dzt[cols, :] = dz[parity(s), :, cols].T

    def accumulate(s, at, count):
        for lane in range(nd):
            acc[lane, at:at + count, :] += jnp.dot(dzt[at:at + count, :], net.tokens(s, lane),
                                                   preferred_element_type=F32)

    def hidden_grad(s, lane):
        block = jnp.dot(dz[parity(s)], wt[lane], preferred_element_type=F32).astype(BF16)
        for rel in range(geo.chips):
            dsum[ring(s), lane, net.place(rel, lane), :] = block[rel * slab:(rel + 1) * slab, :]

    def grad_step(s, carry):
        for lane in range(nd):
            net.arrive(s, lane, False)
        for half in PAIR:
            zs[parity(s), :, half * part:(half + 1) * part] = logit_sum(s, vocab + half * part)
            z_copy(s, half).start()
        hidden_grad(s - 1, 0)
        rs_copy(1, 0, s).start()
        zo[parity(s), :, :part] = logit_sum(s, 0)
        z_copy(s, 0).wait()
        logits_grad(s, 0)
        zo[parity(s), :, part:vocab] = logit_sum(s, part)
        dz_copy(s, 0, True).start()
        dz_copy(s, 0, False).start()
        z_copy(s, 1).wait()
        logits_grad(s, 1)
        accumulate(s, 0, part)
        dz_copy(s, 1, True).start()
        dz_copy(s, 1, False).start()
        hidden_grad(s - 1, 1)
        rs_copy(1, 1, s).start()
        merge_rest(s)
        accumulate(s, part, part)
        finish(s)
        start_rest(s)
        for half in PAIR:
            dz_copy(s, half, True).wait()
        merge_first(s)
        accumulate(s, vocab, vocab)
        for lane in range(nd):
            net.release(s, lane)
            rs_copy(2, lane, s).start()
        for lane in range(2, nd):
            hidden_grad(s - 1, lane)
            rs_copy(1, lane, s).start()
        for half in PAIR:
            dz_copy(s, half, False).wait()
        return carry

    def wout(lane):
        return pltpu.make_async_copy(
            wv.at[lane, :, pl.ds(0, vocab)],
            gw_hbm.at[pl.ds(pl.multiple_of(half_at[0] + lane * width, width), width), :], wout_sem.at[lane])

    def wout_cross(lane):
        return pltpu.make_async_remote_copy(
            src_ref=wv.at[lane, :, pl.ds(vocab, vocab)],
            dst_ref=gw_hbm.at[pl.ds(pl.multiple_of(half_at[0] + lane * width, width), width), :],
            send_sem=wo_send.at[lane], recv_sem=wo_recv.at[lane], device_id=net.sib, device_id_type=MESH)

    def store_weights(lane):
        for half in PAIR:
            span = slice(half * vocab, (half + 1) * vocab)
            wv[lane, :, span] = acc[lane, span, :].astype(BF16).T
        wout(lane).start()
        wout_cross(lane).start()

    def flush():
        end = steps
        for lane in range(nd):
            hidden_grad(end - 1, lane)
        merge_rest(end)
        for lane in range(nd):
            rs_copy(1, lane, end).start()
        start_rest(end)
        merge_first(end)
        for lane in range(nd):
            rs_copy(2, lane, end).start()
        finish(end)
        store_weights(0)

        end += 1
        merge_rest(end)
        finish(end)
        start_rest(end)
        merge_first(end)
        for lane in range(nd):
            rs_copy(2, lane, end).start()
            flush_copy(0, lane).start()

        end += 1
        for lane in range(nd):
            for stage_no in later:
                rs_copy(stage_no, lane, end - 1).wait()
            flush_copy(0, lane).wait()
        for lane in range(nd):
            m3[ring(end), lane] = merged(3, lane, end, m2[ring(end + 1), lane, :low[3]]).astype(BF16)
            m2[ring(end), lane] = merged(2, lane, end, m1[ring(end + 1), lane, :low[2]]).astype(BF16)
            last[lane] = merged(4, lane, end, m3[ring(end + 1), lane, :low[4]])
            dsum[spare, lane, :low[2], :] = (x2[lane].astype(F32)
                                          + m1[ring(end + 2), lane, :low[2]].astype(F32)).astype(BF16)
            rs_copy(3, lane, end).start()
            rs_copy(4, lane, end).start()
            flush_copy(1, lane).start()
            flush_copy(2, lane).start()
        finish(end)
        store_weights(1)

        end += 1
        for lane in range(nd):
            for stage_no in range(3, 5):
                rs_copy(stage_no, lane, end - 1).wait()
            flush_copy(1, lane).wait()
            flush_copy(2, lane).wait()
        for lane in range(nd):
            last[lane] = merged(4, lane, end, m3[ring(end + 1), lane, :low[4]])
            m3[ring(end), lane] = merged(3, lane, end, m2[ring(end + 1), lane, :low[3]]).astype(BF16)
            dsum[spare, lane, low[2]:deep[1], :] = (
                x3[0, lane].astype(F32) + m2[ring(end + 2), lane, :low[3]].astype(F32)).astype(BF16)
            dsum[spare, lane, deep[1]:low[1], :] = (
                x3[1, lane].astype(F32) + dsum[spare, lane, :low[3], :].astype(F32)).astype(BF16)
            rs_copy(4, lane, end).start()
            for i in range(3, 6):
                flush_copy(i, lane).start()
        finish(end)
        store_weights(2)

        end += 1
        for lane in range(nd):
            rs_copy(4, lane, end - 1).wait()
            for i in range(3, 6):
                flush_copy(i, lane).wait()
        for lane in range(nd):
            own3 = (m3[ring(end + 1), lane, :low[4]], m3[ring(end + 2), lane, :low[4]],
                    dsum[spare, lane, low[2]:deep[0], :],
                    dsum[spare, lane, deep[1]:deep[2], :])
            got4 = (r4[parity(end + 1), lane], x4[0, lane], x4[1, lane], x4[2, lane])
            for i in range(nd + 1):
                total = dsum[tail, lane, :low[4], :].astype(F32)
                if i < nd:
                    total = got4[i].astype(F32) + own3[i].astype(F32)
                if i > 0:
                    total = total + early[i - 1, lane]
                emit(lane, end + i, total, 2 + i)
        out_copy(end - 1, parity(end - 1)).wait()
        for i in range(nd + 1):
            out_copy(end + i, 2 + i).start()
        store_weights(3)
        net.end(steps)
        for i in range(nd + 1):
            out_copy(end + i, 2 + i).wait()

    net.begun()
    lax.fori_loop(1, first, loss_step, 0)
    for lane in range(1, nd):
        net.release(first - 1, lane)
    for lane in range(nd):
        for stage_no in range(1, 5):
            rs_copy(stage_no, lane, first - 1).start()
    reps(first - 1)
    softmax()
    lax.fori_loop(first, steps, grad_step, 0)
    flush()
    gb_ref[...] = sum_rows(gb[...])
    stores = []
    for half in PAIR:
        cols = pl.ds(half_at[half], geo.half)
        stores.append(pltpu.make_async_copy(gout.at[half, pl.ds(0, n_q)], gq_hbm.at[:, :, cols], hout_sem.at[half, 0]))
        stores.append(pltpu.make_async_copy(gout.at[half, pl.ds(n_q, n_dp)], gd_hbm.at[:, :, cols],
                                            hout_sem.at[half, 1]))
    for copy in stores:
        copy.start()
    for copy in stores:
        copy.wait()
    for lane in range(nd):
        wout(lane).wait()
        wout_cross(lane).wait()


def call_fused(geo, const, q_rows, d_rows, w_head, bias, mrow, tables, pick):
    bufs, sems = gather_scratch(geo)
    dma = pltpu.SemaphoreType.DMA
    nd, tok, width, vocab, rows = geo.nd, geo.tokens, geo.width, geo.vocab, geo.rows
    n_q, (docs, _), slots, lanes = const[0], pick.shape, 2 * geo.chips, tables.shape[1]
    hq = n_q // 2
    hbm, vmem = pl.BlockSpec(memory_space=pl.ANY), pl.BlockSpec(memory_space=pltpu.VMEM)
    logit = pltpu.VMEM((2, tok, vocab), F32)
    scratch = bufs + [
        pltpu.VMEM((nd, width, 2 * vocab), BF16), pltpu.VMEM((nd, 2 * vocab, width), BF16),
        pltpu.VMEM((nd, 2 * vocab, width), F32), logit, logit, logit,
        pltpu.VMEM((2, tok, 2 * vocab), BF16), pltpu.VMEM((2 * vocab, tok), BF16),
        pltpu.VMEM((3, nd, tok, width), BF16),
        pltpu.VMEM((3, nd, tok // 2, width), BF16), pltpu.VMEM((3, nd, tok // 4, width), BF16),
        pltpu.VMEM((3, nd, tok // 8, width), BF16),
        pltpu.VMEM((2, nd, tok // 2, width), BF16), pltpu.VMEM((2, nd, tok // 4, width), BF16),
        pltpu.VMEM((2, nd, tok // 8, width), BF16), pltpu.VMEM((2, nd, tok // 16, width), BF16),
        pltpu.VMEM((nd, tok // 4, width), BF16), pltpu.VMEM((2, nd, tok // 8, width), BF16),
        pltpu.VMEM((3, nd, tok // 16, width), BF16),
        pltpu.VMEM((nd + 3, geo.unit, geo.half), BF16), pltpu.VMEM((2, rows, geo.unit, geo.half), BF16),
        pltpu.VMEM((nd, nd, geo.slab, width), F32), pltpu.VMEM((nd, geo.slab, width), F32),
        pltpu.VMEM((geo.unit, vocab), F32),
        pltpu.VMEM((slots, rows, vocab), F32), pltpu.VMEM((docs, vocab), F32), pltpu.VMEM((docs, vocab), F32),
        pltpu.VMEM((slots,) + mrow.shape, F32), pltpu.VMEM((mrow.shape[1] // geo.unit, geo.unit, 128), F32),
        pltpu.VMEM((slots, hq, lanes), F32), pltpu.VMEM((slots, hq, lanes), F32),
        pltpu.VMEM((hq, lanes), F32), pltpu.VMEM((slots, hq, lanes), F32),
        pltpu.VMEM((1, lanes), F32), pltpu.VMEM((slots, 1, lanes), F32),
        dma((4,)), dma((nd,)), dma((nd,)), dma((nd,)), dma((2, 2)), dma((2, 2)), dma((2, 2)), dma((2, 2)),
        dma((4, nd, 2)), dma((4, nd, 2)), dma((6, nd)), dma((6, nd)), dma((nd + 3,)), dma((nd + 3,)), dma((nd,)), dma((nd,)),
        dma((nd,)), dma((2, 2)), dma((4, slots)), dma((4, slots))] + sems
    return pl.pallas_call(
        functools.partial(fused_kernel, geo, const),
        name="lexical_head",
        out_shape=[jax.ShapeDtypeStruct((1, lanes), F32), jax.ShapeDtypeStruct(w_head.shape, BF16),
                   jax.ShapeDtypeStruct((1, vocab), F32), jax.ShapeDtypeStruct(q_rows.shape, BF16),
                   jax.ShapeDtypeStruct(d_rows.shape, BF16)],
        in_specs=[hbm, hbm, hbm] + [vmem] * 4,
        out_specs=[vmem, hbm, vmem, hbm, hbm],
        scratch_shapes=scratch,
        compiler_params=pltpu.CompilerParams(collective_id=0, has_side_effects=True, vmem_limit_bytes=VMEM_LIMIT),
    )(q_rows, d_rows, w_head, bias, mrow, tables, pick)


def store_kernel(count, *refs):
    sources, results, holds = refs[:count], refs[count:2 * count], refs[2 * count:3 * count]
    read_sem, write_sem = refs[3 * count:]
    reads, writes = [], []
    for source, result, hold in zip(sources, results, holds):
        for piece in range(hold.shape[0]):
            span = pl.ds(piece * hold.shape[1], hold.shape[1])
            at = len(reads)
            reads.append(pltpu.make_async_copy(source.at[span], hold.at[piece], read_sem.at[at]))
            writes.append(pltpu.make_async_copy(hold.at[piece], result.at[span], write_sem.at[at]))
    for copy in reads:
        copy.start()
    for read, write in zip(reads, writes):
        read.wait()
        write.start()
    for copy in writes:
        copy.wait()


def call_store(geo, *arrays):
    pieces = [geo.chips // (1 + 3 * (x.ndim - 2)) for x in arrays]
    holds = [pltpu.VMEM((n, x.shape[0] // n) + x.shape[1:], x.dtype) for n, x in zip(pieces, arrays)]
    hbm = pl.BlockSpec(memory_space=pl.ANY)
    dma = pltpu.SemaphoreType.DMA((sum(pieces),))
    return pl.pallas_call(
        functools.partial(store_kernel, len(arrays)), name="store_results",
        out_shape=[jax.ShapeDtypeStruct(x.shape, x.dtype) for x in arrays],
        in_specs=[hbm] * len(arrays), out_specs=[hbm] * len(arrays), scratch_shapes=holds + [dma, dma],
        compiler_params=pltpu.CompilerParams(vmem_limit_bytes=VMEM_LIMIT),
    )(*arrays)


def solution(mesh):
    n_group = mesh.shape['tp']
    row_spec = P(('dp', 'tp'))
    mask_spec = P(('dp', 'tp'), None)
    hid_spec = P(('dp', 'tp'), None, None)

    def local_step(q_hidden, d_hidden, q_mask, d_mask, positive, w_head, b_head):
        hidden_size, vocab_loc = w_head.shape
        vocab_size = vocab_loc * n_group
        n_q, q_len, _ = q_hidden.shape
        n_d, d_len, _ = d_hidden.shape
        pieces = d_len // q_len
        q_batch, d_batch = n_q * n_group, n_d * n_group
        tau = q_len * math.sqrt(vocab_size * d_len) / 16.0
        lam_q = 4.0 / (vocab_size * q_len * q_len)
        lam_d = 4.0 / (vocab_size * d_len * d_len)
        rows = n_q + n_d * pieces
        geo = Geometry(n_group, rows, hidden_size, vocab_loc, q_len)
        side, slots = geo.side, 2 * geo.chips
        lanes = max(128, 2 * d_batch)

        me = lax.axis_index('tp')
        slot = jnp.arange(slots)
        chip, rel = me // 2, slot // 2
        step_x, step_y = rel % side, rel // side
        chip_of = (((chip // side) ^ step_y ^ (step_y >> 1)) * side + ((chip % side) ^ step_x ^ (step_x >> 1)))
        device_of = chip_of * 2 + slot % 2
        doc_of = jnp.add.outer(jnp.arange(n_d), device_of * n_d).reshape((n_d * slots,))
        tables = jax.nn.one_hot(jnp.concatenate([device_of, doc_of, positive]), lanes, dtype=F32)
        pick = np.concatenate([np.kron(np.eye(slots), np.repeat(row, pieces)) for row in np.eye(n_d)])

        own_mask = jnp.concatenate([q_mask.reshape((-1,)), d_mask.reshape((-1,))]).astype(F32)
        mrow = jnp.pad(own_mask, (0, -own_mask.shape[0] % 128)).reshape((1, -1))
        const = (n_q, n_d, lam_q, lam_d, tau, float(q_batch), float(d_batch))
        loss, grad_w, grad_b, grad_q, grad_d = call_fused(
            geo, const, q_hidden, d_hidden.reshape((n_d * pieces, q_len, hidden_size)), w_head,
            b_head.reshape((1, vocab_loc)), mrow, tables, jnp.asarray(pick, F32))
        grad_w, grad_q, grad_d = call_store(geo, grad_w, grad_q, grad_d)
        return (loss[0, 0:1], grad_w, grad_b.reshape((vocab_loc,)), grad_q, grad_d.reshape(d_hidden.shape))

    return jax.shard_map(local_step, mesh=mesh,
                         in_specs=(hid_spec, hid_spec, mask_spec, mask_spec, row_spec, P(None, 'tp'), P('tp')),
                         out_specs=(P('dp'), P('dp', 'tp'), row_spec, hid_spec, hid_spec),
                         check_vma=False)
```

```python
import functools
import math

import jax
import jax.numpy as jnp
import numpy as np
from jax import lax
from jax.experimental import pallas as pl
from jax.experimental.pallas import tpu as pltpu
from jax.sharding import PartitionSpec as P

MESH = pl.DeviceIdType.MESH
F32 = jnp.float32
BF16 = jnp.bfloat16
VMEM_LIMIT = 67043328
PAIR = range(2)
HIGHEST = lax.Precision.HIGHEST


def parity(s):
    return lax.rem(s, 2)


def ring(s):
    return lax.rem(s, 3)


def sum_rows(x):
    return jnp.sum(x, axis=0, keepdims=True)


def sum_lanes(x):
    return jnp.sum(x, axis=1, keepdims=True)


def exact_dot(a, b, dims=(((1,), (0,)), ((), ()))):
    return lax.dot_general(a, b, dims, precision=HIGHEST, preferred_element_type=F32)


TURNED = (((1,), (1,)), ((), ()))
FIRST = (((0,), (0,)), ((), ()))


class Geometry:
    def __init__(self, n_group, rows, hidden, vocab, unit):
        self.side = math.isqrt(n_group // 2)
        self.nd = 2 * (self.side.bit_length() - 1)
        self.chips = 1 << self.nd
        assert self.side == 4 and self.chips * 2 == n_group
        self.rows = rows
        self.first = self.nd + rows
        self.steps = self.first + rows
        self.unit = unit
        self.slab = 2 * unit
        self.tokens = self.slab * self.chips
        self.half = hidden // 2
        self.width = self.half // self.nd
        self.vocab = vocab

    def hops(self, rel):
        return bin(rel).count("1")

    def slot(self, rel, lane):
        return ((rel >> lane) | (rel << (self.nd - lane))) & (self.chips - 1)

    def device(self, me, rel, core):
        chip = lax.div(me, 2)
        x, y = lax.rem(chip, self.side), lax.div(chip, self.side)
        at = [x, y]
        for dim in range(self.nd):
            if rel >> dim & 1:
                axis, wide = divmod(dim, len(at))
                at[axis] = self.side - 1 - at[axis] if wide else at[axis] + 1 - 2 * lax.rem(at[axis], 2)
        x, y = at
        return {"tp": (y * self.side + x) * 2 + core}

    def peer(self, me, dim, core):
        return self.device(me, 1 << dim, core)


def entry_barrier(peers):
    barrier = pltpu.get_barrier_semaphore()
    for device in peers:
        pl.semaphore_signal(barrier, inc=1, device_id=device, device_id_type=MESH)
    pl.semaphore_wait(barrier, len(peers))


class Gather:
    def __init__(self, geo, me, x, stage, ownx, sems):
        (self.ici_send, self.ici_recv, self.piece_send, self.piece_recv, self.free_ici, self.free_piece) = sems
        self.geo, self.x, self.stage, self.ownx = geo, x, stage, ownx
        self.core = lax.rem(me, 2)
        self.sib = {"tp": me + 1 - 2 * self.core}
        dims = [geo.peer(me, dim, self.core)["tp"] for dim in range(geo.nd)]
        turn = geo.nd // 2
        self.same = [{"tp": dims[d] + self.core * (dims[(d + turn) % geo.nd] - dims[d])} for d in range(geo.nd)]

    def place(self, rel, lane):
        geo = self.geo
        one = geo.slot(rel, lane) * geo.slab
        two = geo.slot(rel, (lane + geo.nd // 2) % geo.nd) * geo.slab
        if one == two:
            return pl.ds(one, geo.slab)
        return pl.ds(pl.multiple_of(one + self.core * (two - one), geo.slab), geo.slab)

    def ici(self, s, lane, pos):
        count = (1 << pos) * self.geo.slab
        here, there = parity(s), parity(s + 1)
        return pltpu.make_async_remote_copy(
            src_ref=self.x.at[here, lane, pl.ds(0, count)], dst_ref=self.x.at[there, lane, pl.ds(count, count)],
            send_sem=self.ici_send.at[lane, pos, there], recv_sem=self.ici_recv.at[lane, pos, there],
            device_id=self.same[(lane + pos) % self.geo.nd], device_id_type=MESH)

    def piece(self, s, lane):
        width = self.geo.width
        return pltpu.make_async_remote_copy(
            src_ref=self.ownx.at[1, lax.rem(s, self.geo.rows), :, pl.ds(lane * width, width)],
            dst_ref=self.stage.at[parity(s), lane], send_sem=self.piece_send.at[lane, parity(s)],
            recv_sem=self.piece_recv.at[lane, parity(s)], device_id=self.sib, device_id_type=MESH)

    def inject(self, s, lane):
        geo = self.geo
        width = geo.width
        self.piece(s, lane).wait()
        mine = self.ownx[0, lax.rem(s, geo.rows), :, lane * width:(lane + 1) * width].astype(F32)
        theirs = self.stage[parity(s), lane].astype(F32)
        first = jnp.where(self.core == 0, mine, theirs)
        second = jnp.where(self.core == 0, theirs, mine)
        self.x[parity(s), lane, :geo.slab, :] = jnp.concatenate([first, second], axis=0).astype(BF16)

    def begin(self):
        geo = self.geo
        for lane in range(geo.nd):
            self.inject(0, lane)
            for pos in range(geo.nd):
                self.first(lane, pos).start()
            self.piece(1, lane).start()

    def begun(self):
        geo = self.geo
        for lane in range(geo.nd):
            for pos in range(geo.nd):
                self.first(lane, pos).wait_send()
            self.grant(lane)
        for lane in range(geo.nd):
            for pos in range(geo.nd):
                self.first(lane, pos).wait_recv()

    def first(self, lane, pos):
        geo = self.geo
        return pltpu.make_async_remote_copy(
            src_ref=self.x.at[0, lane, pl.ds(0, geo.slab)],
            dst_ref=self.x.at[1, lane, pl.ds((1 << pos) * geo.slab, geo.slab)],
            send_sem=self.ici_send.at[lane, pos, 1], recv_sem=self.ici_recv.at[lane, pos, 1],
            device_id=self.same[(lane + pos) % geo.nd], device_id_type=MESH)

    def arrive(self, s, lane, loss):
        geo = self.geo
        self.inject(s, lane)

        if loss:
            @pl.when(s > 1)
            def _():
                self.receive(s, lane)
        else:
            self.receive(s, lane)
        self.credits(lane)
        for pos in reversed(range(geo.nd)):
            self.ici(s, lane, pos).start()
        self.piece(s + 1, lane).start()

    def receive(self, s, lane):
        for pos in range(self.geo.nd):
            self.ici(s - 1, lane, pos).wait_recv()

    def credits(self, lane):
        pl.semaphore_wait(self.free_piece.at[lane], 1)
        for pos in range(self.geo.nd):
            pl.semaphore_wait(self.free_ici.at[lane, pos], 1)

    def grant(self, lane):
        geo = self.geo
        for pos in range(geo.nd):
            pl.semaphore_signal(self.free_ici.at[lane, pos], inc=1,
                                device_id=self.same[(lane + pos) % geo.nd], device_id_type=MESH)
        pl.semaphore_signal(self.free_piece.at[lane], inc=1, device_id=self.sib, device_id_type=MESH)

    def release(self, s, lane):
        for pos in range(self.geo.nd):
            self.ici(s, lane, pos).wait_send()
        self.grant(lane)

    def end(self, s):
        for lane in range(self.geo.nd):
            self.receive(s, lane)
            self.credits(lane)
            self.piece(s, lane).wait()

    def tokens(self, s, lane):
        geo = self.geo
        return jnp.concatenate([self.x[parity(s), lane, self.place(rel, lane), :] for rel in range(geo.chips)], axis=0)


def gather_scratch(geo):
    nd = geo.nd
    bufs = [pltpu.VMEM((2, nd, geo.tokens, geo.width), BF16), pltpu.VMEM((2, nd, geo.unit, geo.width), BF16),
            pltpu.VMEM((2, geo.rows, geo.unit, geo.half), BF16)]
    dma, reg = pltpu.SemaphoreType.DMA, pltpu.SemaphoreType.REGULAR
    sems = [dma((nd, nd, 2)), dma((nd, nd, 2)), dma((nd, 2)), dma((nd, 2)), reg((nd, nd)), reg((nd,))]
    return bufs, sems


def all_peers(geo, me):
    core = lax.rem(me, 2)
    found = [(0, 1 - core, geo.device(me, 0, 1 - core))]
    for rel in range(1, geo.chips):
        for other in PAIR:
            found.append((rel, other, geo.device(me, rel, other)))
    return found


def fused_kernel(geo, const, q_hbm, d_hbm, w_hbm, bias, mrow, tables, pick,
                 loss_ref, gw_hbm, gb_ref, gq_hbm, gd_hbm,
                 x, stage, ownx, wv, wt, acc, zo, zs, zr, dz, dzt, dsum, m1, m2, m3,
                 r1, r2, r3, r4, x2, x3, x4, ost, gout, early, last, gb, rep, rd, drd, mall, mt, sbuf, pall, gmine, gall,
                 lmine, lall,
                 own_sem, w_sem, wx_send, wx_recv, z_send, z_recv, dz_send, dz_recv, rs_send, rs_recv, fl_send, fl_recv,
                 out_send, out_recv, wout_sem, wo_send, wo_recv, hout_sem, ex_send, ex_recv, *sems):
    nd, slab, unit, width, steps, rows, first = (geo.nd, geo.slab, geo.unit, geo.width, geo.steps, geo.rows,
                                                 geo.first)
    n_q, n_d, lam_q, lam_d, tau, q_batch, d_batch = const
    slots, vocab = 2 * geo.chips, geo.vocab
    me = lax.axis_index("tp")
    net = Gather(geo, me, x, stage, ownx, sems)
    core, same = net.core, net.same
    docs = n_d * slots
    place, doc_place, target = tables.at[:slots], tables.at[pl.ds(slots, docs)], tables.at[pl.ds(slots + docs, n_q)]
    peers = all_peers(geo, me)
    half_at = [pl.multiple_of(core * geo.half, geo.half), pl.multiple_of((1 - core) * geo.half, geo.half)]

    n_dp = d_hbm.shape[0]
    own_loads = []
    for half in PAIR:
        cols = pl.ds(half_at[half], geo.half)
        own_loads.append(pltpu.make_async_copy(q_hbm.at[:, :, cols], ownx.at[half, pl.ds(0, n_q)],
                                               own_sem.at[2 * half]))
        own_loads.append(pltpu.make_async_copy(d_hbm.at[:, :, cols], ownx.at[half, pl.ds(n_q, n_dp)],
                                               own_sem.at[2 * half + 1]))
    w_loads, w_cross = [], []
    for lane in range(nd):
        here = pl.ds(pl.multiple_of(half_at[0] + lane * width, width), width)
        there = pl.ds(pl.multiple_of(half_at[1] + lane * width, width), width)
        w_loads.append(pltpu.make_async_copy(w_hbm.at[here, :], wv.at[lane, :, pl.ds(0, vocab)], w_sem.at[lane]))
        w_cross.append(pltpu.make_async_remote_copy(
            src_ref=w_hbm.at[there, :], dst_ref=wv.at[lane, :, pl.ds(vocab, vocab)], send_sem=wx_send.at[lane],
            recv_sem=wx_recv.at[lane], device_id=net.sib, device_id_type=MESH))
    for copy in own_loads + w_loads:
        copy.start()
    entry_barrier([device for _, _, device in peers])
    for copy in own_loads:
        copy.wait()
    for lane in range(nd):
        net.piece(0, lane).start()
    net.begin()

    def broadcast(kind, src_of, dst):
        return [pltpu.make_async_remote_copy(
            src_ref=src_of(2 * rel + other), dst_ref=dst.at[2 * rel + core],
            send_sem=ex_send.at[kind, i], recv_sem=ex_recv.at[kind, 2 * rel + core], device_id=device,
            device_id_type=MESH) for i, (rel, other, device) in enumerate(peers)]

    def arrivals(kind, dst):
        return [pltpu.make_async_remote_copy(
            src_ref=dst.at[2 * rel + other], dst_ref=dst.at[2 * rel + other],
            send_sem=ex_send.at[kind, i], recv_sem=ex_recv.at[kind, 2 * rel + other], device_id=device,
            device_id_type=MESH) for i, (rel, other, device) in enumerate(peers)]

    masks_out = broadcast(0, lambda slot: mrow, mall)
    for copy in masks_out:
        copy.start()
    mall[core] = mrow[...]
    for copy in w_cross:
        copy.start()
    gb[...] = jnp.zeros_like(gb)
    for ref in (dsum, m1, m2, m3, dz):
        ref[...] = jnp.zeros_like(ref)

    part = vocab // 2

    def z_copy(s, half):
        cols = pl.ds(half * part, part)
        return pltpu.make_async_remote_copy(
            src_ref=zs.at[parity(s), :, cols], dst_ref=zr.at[parity(s), :, cols], send_sem=z_send.at[parity(s), half],
            recv_sem=z_recv.at[parity(s), half], device_id=net.sib, device_id_type=MESH)

    def dz_copy(s, half, turned):
        here, there = pl.ds(half * part, part), pl.ds(vocab + half * part, part)
        src, dst = dzt.at[here], dzt.at[there]
        if not turned:
            src, dst = dz.at[parity(s), :, here], dz.at[parity(s), :, there]
        return pltpu.make_async_remote_copy(
            src_ref=src, dst_ref=dst, send_sem=dz_send.at[half, int(turned)], recv_sem=dz_recv.at[half, int(turned)],
            device_id=net.sib, device_id_type=MESH)

    def rs_copy(stage_no, lane, s):
        n_low = geo.tokens >> stage_no
        src = dsum.at[ring(s + 2), lane, pl.ds(n_low, n_low)]
        if stage_no > 1:
            src = (m1, m2, m3)[stage_no - 2].at[ring(s), lane, pl.ds(n_low, n_low)]
        dst = (r1, r2, r3, r4)[stage_no - 1].at[parity(s), lane]
        return pltpu.make_async_remote_copy(
            src_ref=src, dst_ref=dst, send_sem=rs_send.at[stage_no - 1, lane, parity(s)],
            recv_sem=rs_recv.at[stage_no - 1, lane, parity(s)],
            device_id=same[(lane + nd - stage_no) % nd], device_id_type=MESH)

    low = [geo.tokens >> k for k in range(5)]
    deep = (low[2] + low[4], low[2] + low[3], low[2] + low[3] + low[4])
    later = (2, 3, 4)
    tail, spare = (steps - 1) % 3, steps % 3

    def flush_copy(i, lane):
        src, dst, stage_no = (
            (dsum.at[tail, lane, pl.ds(low[2], low[2])], x2.at[lane], 2),
            (dsum.at[spare, lane, pl.ds(low[3], low[3])], x3.at[0, lane], 3),
            (dsum.at[tail, lane, pl.ds(low[3], low[3])], x3.at[1, lane], 3),
            (dsum.at[spare, lane, pl.ds(deep[0], low[4])], x4.at[0, lane], 4),
            (dsum.at[spare, lane, pl.ds(deep[2], low[4])], x4.at[1, lane], 4),
            (dsum.at[tail, lane, pl.ds(low[4], low[4])], x4.at[2, lane], 4))[i]
        return pltpu.make_async_remote_copy(
            src_ref=src, dst_ref=dst, send_sem=fl_send.at[i, lane], recv_sem=fl_recv.at[i, lane],
            device_id=same[(lane + nd - stage_no) % nd], device_id_type=MESH)

    def out_copy(s, at):
        return pltpu.make_async_remote_copy(
            src_ref=ost.at[at], dst_ref=gout.at[1, lax.rem(s - 9, rows)], send_sem=out_send.at[at],
            recv_sem=out_recv.at[at], device_id=net.sib, device_id_type=MESH)

    def emit(lane, s, total, at):
        cols = slice(lane * width, (lane + 1) * width)
        one, two = total[:unit], total[unit:slab]
        gout[0, lax.rem(s - 9, rows), :, cols] = jnp.where(core == 0, one, two).astype(BF16)
        ost[at, :, cols] = jnp.where(core == 0, two, one).astype(BF16)

    def merged(stage_no, lane, s, mine):
        got = (r1, r2, r3, r4)[stage_no - 1][parity(s + 1), lane].astype(F32)
        return got + mine.astype(F32)

    def merge_first(s):
        for lane in range(nd):
            rs_copy(1, lane, s - 1).wait()
        for lane in range(nd):
            m1[ring(s), lane] = merged(1, lane, s, dsum[ring(s), lane, :low[1]]).astype(BF16)

    def merge_rest(s):
        back = ring(s + 1)
        for lane in range(nd):
            for stage_no in later:
                rs_copy(stage_no, lane, s - 1).wait()
        for lane in range(nd):
            m2[ring(s), lane] = merged(2, lane, s, m1[back, lane, :low[2]]).astype(BF16)
            m3[ring(s), lane] = merged(3, lane, s, m2[back, lane, :low[3]]).astype(BF16)
            last[lane] = merged(4, lane, s, m3[back, lane, :low[4]])

    def finish(s):
        @pl.when((s >= first + 5) & (s < first + 9))
        def _():
            early[lax.rem(s - first - 5, nd)] = last[...]

        @pl.when(s >= first + 9)
        def _():
            for lane in range(nd):
                emit(lane, s, last[lane], parity(s))

        @pl.when(s >= first + 10)
        def _():
            out_copy(s - 1, parity(s + 1)).wait()

        @pl.when(s >= first + 9)
        def _():
            out_copy(s, parity(s)).start()

    def start_rest(s):
        for lane in range(nd):
            rs_copy(3, lane, s).start()
            rs_copy(4, lane, s).start()

    def logits_part(s, lane):
        tokens = net.tokens(s, lane)
        for ref, at in ((zs, vocab), (zo, 0)):
            part = jnp.dot(tokens, wv[lane, :, at:at + vocab], preferred_element_type=F32)
            if lane == 0:
                ref[parity(s)] = part
            else:
                ref[parity(s)] = ref[parity(s)] + part

    def reps(s):
        for half in PAIR:
            z_copy(s, half).wait()
        for rel in range(geo.chips):
            span = slice(rel * slab, (rel + 1) * slab)
            logits = zo[parity(s), span, :] + zr[parity(s), span, :] + bias[...]
            active = jnp.log1p(jnp.maximum(logits, 0.0))
            row = lax.rem(s - geo.hops(rel), rows)
            for cr in PAIR:
                at = 2 * rel + cr
                part = active[cr * unit:(cr + 1) * unit, :] * mt[row, :, at:at + 1]
                rep[at, pl.ds(row, 1), :] = sum_rows(part)

    def prepare(s):
        @pl.when(s == 1)
        def _():
            for copy in w_loads:
                copy.wait()
            for copy in arrivals(0, mall):
                copy.wait_recv()
            for copy in masks_out:
                copy.wait_send()
            table = jnp.concatenate([mall[i] for i in range(slots)], axis=0)
            table = jnp.concatenate([table, jnp.zeros((128 - slots, table.shape[1]), F32)], axis=0)
            mt[...] = table.T.reshape(mt.shape)

        @pl.when(s == 2)
        def _():
            for copy in w_cross:
                copy.wait()

        @pl.when((s >= 2) & (s < 2 + nd))
        def _():
            def turn(half, carry):
                span = pl.ds(pl.multiple_of(half * vocab, vocab), vocab)
                acc[s - 2, span, :] = jnp.zeros((vocab, width), F32)
                wt[s - 2, span, :] = wv[s - 2, :, span].T
                return carry

            lax.fori_loop(0, 2, turn, 0)

    def loss_step(s, carry):
        prepare(s)
        for lane in range(nd):
            if lane == nd - 1:
                net.release(s, 0)
            else:
                @pl.when(s > 1)
                def _():
                    net.release(s - 1, lane + 1)

            net.arrive(s, lane, True)

            @pl.when(s >= nd)
            def _():
                logits_part(s, lane)

            if lane == 1:
                @pl.when(s > nd)
                def _():
                    reps(s - 1)

        @pl.when(s >= nd)
        def _():
            for half in PAIR:
                z_copy(s, half).start()
        return carry

    def softmax():
        chunk = 16
        hq = n_q // 2
        shift = loss_ref.shape[1] // 2
        parts = slots // chunk
        pieces = rep[:, n_q:rows, :].reshape((slots * (rows - n_q), geo.vocab))
        rd[...] = exact_dot(pick[...], pieces)

        def score(c, q_sum):
            at = pl.ds(c * chunk, chunk)
            reps_c = rep[at, :n_q, :].reshape((chunk * n_q, geo.vocab))
            part = exact_dot(reps_c, rd[...], TURNED)
            part = exact_dot(part, doc_place[...])
            part = part.reshape((chunk, n_q, part.shape[1]))
            sbuf[at] = part[:, :hq] + pltpu.roll(part[:, hq:], shift, 2)
            return q_sum + sum_rows(reps_c)

        q_sum = lax.fori_loop(0, parts, score, jnp.zeros((1, geo.vocab), F32))
        scores_out = broadcast(1, lambda slot: sbuf.at[slot], pall)
        for copy in scores_out:
            copy.start()
        pall[core] = sbuf[core]
        q_mean = q_sum / q_batch
        d_mean = sum_rows(rd[...]) / d_batch
        reg = (lam_q * sum_lanes(q_mean * q_mean)
               + lam_d * sum_lanes(d_mean * d_mean))
        for copy in arrivals(1, pall):
            copy.wait_recv()
        total = pall[0]
        for i in range(1, slots):
            total = total + pall[i]
        scores = jnp.concatenate([total, pltpu.roll(total, shift, 1)], axis=0) / tau
        lane_no = lax.broadcasted_iota(jnp.int32, scores.shape, 1)
        masked = jnp.where(lane_no < d_batch, scores, -jnp.inf)
        top = jnp.max(masked, axis=1, keepdims=True)
        log_norm = jnp.log(sum_lanes(jnp.exp(masked - top))) + top
        hit = sum_lanes(target[...] * scores)
        mine = sum_rows(log_norm - hit) / q_batch + reg
        grad = (jnp.exp(masked - log_norm) - target[...]) / (q_batch * tau)
        gmine[...] = grad[:hq] + pltpu.roll(grad[hq:], shift, 1)
        lmine[...] = jnp.broadcast_to(mine, lmine.shape)
        grads_out = broadcast(2, lambda slot: gmine, gall)
        for copy in grads_out:
            copy.start()
        losses_out = broadcast(3, lambda slot: lmine, lall)
        for copy in losses_out:
            copy.start()
        gall[core] = gmine[...]
        lall[core] = lmine[...]
        drd[...] = jnp.broadcast_to((2.0 * lam_d / d_batch) * d_mean, drd.shape)
        for copy in arrivals(2, gall):
            copy.wait_recv()
        for lane in range(nd):
            net.arrive(first, lane, False)

        def back(c, carry):
            at = pl.ds(c * chunk, chunk)
            grad_c = gall[at]
            grad_c = jnp.concatenate([grad_c, pltpu.roll(grad_c, shift, 2)], axis=1).reshape((chunk * n_q, 2 * shift))
            grad_c = exact_dot(grad_c, doc_place[...], TURNED)
            reps_c = rep[at, :n_q, :].reshape((chunk * n_q, geo.vocab))
            drd[...] += exact_dot(grad_c, reps_c, FIRST)
            drq = exact_dot(grad_c, rd[...])
            drq = drq + (2.0 * lam_q / q_batch) * q_mean
            rep[at, :n_q, :] = drq.reshape((chunk, n_q, geo.vocab))
            return carry

        lax.fori_loop(0, parts, back, 0)
        spread = exact_dot(pick[...], drd[...], FIRST)
        rep[:, n_q:rows, :] = spread.reshape((slots, rows - n_q, geo.vocab))
        for copy in arrivals(3, lall):
            copy.wait_recv()
        by_device = jnp.zeros((1, place.shape[1]), F32)
        for i in range(slots):
            by_device = by_device + lall[i] * place[i:i + 1, :]
        loss_ref[...] = jnp.broadcast_to(sum_lanes(by_device), loss_ref.shape)
        for copy in scores_out + grads_out + losses_out:
            copy.wait_send()

    def logit_sum(s, at):
        total = jnp.dot(net.tokens(s, 0), wv[0, :, at:at + part], preferred_element_type=F32)
        for lane in range(1, nd):
            total += jnp.dot(net.tokens(s, lane), wv[lane, :, at:at + part], preferred_element_type=F32)
        return total

    def logits_grad(s, half):
        cols = slice(half * part, (half + 1) * part)
        total = gb[:, cols]
        for rel in range(geo.chips):
            span = slice(rel * slab, (rel + 1) * slab)
            logits = zo[parity(s), span, cols] + zr[parity(s), span, cols] + bias[:, cols]
            inverse = 1.0 / (1.0 + logits)
            row = lax.rem(s - geo.hops(rel), rows)
            parts = []
            for cr in PAIR:
                at = 2 * rel + cr
                tok = slice(cr * unit, (cr + 1) * unit)
                grad_row = rep[at, pl.ds(row, 1), cols] * inverse[tok, :]
                grad_row = jnp.where(logits[tok, :] > 0.0, grad_row, 0.0) * mt[row, :, at:at + 1]
                total = total + grad_row
                parts.append(grad_row)
            dz[parity(s), span, cols] = jnp.concatenate(parts, axis=0).astype(BF16)
        gb[:, cols] = total
        dzt[cols, :] = dz[parity(s), :, cols].T

    def accumulate(s, at, count):
        for lane in range(nd):
            acc[lane, at:at + count, :] += jnp.dot(dzt[at:at + count, :], net.tokens(s, lane),
                                                   preferred_element_type=F32)

    def hidden_grad(s, lane):
        block = jnp.dot(dz[parity(s)], wt[lane], preferred_element_type=F32).astype(BF16)
        for rel in range(geo.chips):
            dsum[ring(s), lane, net.place(rel, lane), :] = block[rel * slab:(rel + 1) * slab, :]

    def grad_step(s, carry):
        for half in PAIR:
            zs[parity(s), :, half * part:(half + 1) * part] = logit_sum(s, vocab + half * part)
            z_copy(s, half).start()
        hidden_grad(s - 1, 0)
        rs_copy(1, 0, s).start()
        zo[parity(s), :, :part] = logit_sum(s, 0)
        z_copy(s, 0).wait()
        logits_grad(s, 0)
        zo[parity(s), :, part:vocab] = logit_sum(s, part)
        dz_copy(s, 0, True).start()
        dz_copy(s, 0, False).start()
        z_copy(s, 1).wait()
        logits_grad(s, 1)
        accumulate(s, 0, part)
        dz_copy(s, 1, True).start()
        dz_copy(s, 1, False).start()
        hidden_grad(s - 1, 1)
        rs_copy(1, 1, s).start()
        merge_rest(s)
        accumulate(s, part, part)
        finish(s)
        start_rest(s)
        for half in PAIR:
            dz_copy(s, half, True).wait()
        merge_first(s)
        accumulate(s, vocab, vocab)
        for lane in range(nd):
            net.release(s, lane)
            rs_copy(2, lane, s).start()
        for lane in range(2, nd):
            hidden_grad(s - 1, lane)
            rs_copy(1, lane, s).start()
        for half in PAIR:
            dz_copy(s, half, False).wait()

        @pl.when(s < steps - 1)
        def _():
            for lane in range(nd):
                net.arrive(s + 1, lane, False)
        return carry

    def wout(lane):
        return pltpu.make_async_copy(
            wv.at[lane, :, pl.ds(0, vocab)],
            gw_hbm.at[pl.ds(pl.multiple_of(half_at[0] + lane * width, width), width), :], wout_sem.at[lane])

    def wout_cross(lane):
        return pltpu.make_async_remote_copy(
            src_ref=wv.at[lane, :, pl.ds(vocab, vocab)],
            dst_ref=gw_hbm.at[pl.ds(pl.multiple_of(half_at[0] + lane * width, width), width), :],
            send_sem=wo_send.at[lane], recv_sem=wo_recv.at[lane], device_id=net.sib, device_id_type=MESH)

    def store_weights(lane):
        for half in PAIR:
            span = slice(half * vocab, (half + 1) * vocab)
            wv[lane, :, span] = acc[lane, span, :].astype(BF16).T
        wout(lane).start()
        wout_cross(lane).start()

    def flush():
        end = steps
        for lane in range(nd):
            hidden_grad(end - 1, lane)
        merge_rest(end)
        for lane in range(nd):
            rs_copy(1, lane, end).start()
        start_rest(end)
        merge_first(end)
        for lane in range(nd):
            rs_copy(2, lane, end).start()
        finish(end)
        store_weights(0)

        end += 1
        merge_rest(end)
        finish(end)
        start_rest(end)
        merge_first(end)
        for lane in range(nd):
            rs_copy(2, lane, end).start()
            flush_copy(0, lane).start()

        end += 1
        for lane in range(nd):
            for stage_no in later:
                rs_copy(stage_no, lane, end - 1).wait()
            flush_copy(0, lane).wait()
        for lane in range(nd):
            m3[ring(end), lane] = merged(3, lane, end, m2[ring(end + 1), lane, :low[3]]).astype(BF16)
            m2[ring(end), lane] = merged(2, lane, end, m1[ring(end + 1), lane, :low[2]]).astype(BF16)
            last[lane] = merged(4, lane, end, m3[ring(end + 1), lane, :low[4]])
            dsum[spare, lane, :low[2], :] = (x2[lane].astype(F32)
                                          + m1[ring(end + 2), lane, :low[2]].astype(F32)).astype(BF16)
            rs_copy(3, lane, end).start()
            rs_copy(4, lane, end).start()
            flush_copy(1, lane).start()
            flush_copy(2, lane).start()
        finish(end)
        store_weights(1)

        end += 1
        for lane in range(nd):
            for stage_no in range(3, 5):
                rs_copy(stage_no, lane, end - 1).wait()
            flush_copy(1, lane).wait()
            flush_copy(2, lane).wait()
        for lane in range(nd):
            last[lane] = merged(4, lane, end, m3[ring(end + 1), lane, :low[4]])
            m3[ring(end), lane] = merged(3, lane, end, m2[ring(end + 1), lane, :low[3]]).astype(BF16)
            dsum[spare, lane, low[2]:deep[1], :] = (
                x3[0, lane].astype(F32) + m2[ring(end + 2), lane, :low[3]].astype(F32)).astype(BF16)
            dsum[spare, lane, deep[1]:low[1], :] = (
                x3[1, lane].astype(F32) + dsum[spare, lane, :low[3], :].astype(F32)).astype(BF16)
            rs_copy(4, lane, end).start()
            for i in range(3, 6):
                flush_copy(i, lane).start()
        finish(end)
        store_weights(2)

        end += 1
        for lane in range(nd):
            rs_copy(4, lane, end - 1).wait()
            for i in range(3, 6):
                flush_copy(i, lane).wait()
        for lane in range(nd):
            own3 = (m3[ring(end + 1), lane, :low[4]], m3[ring(end + 2), lane, :low[4]],
                    dsum[spare, lane, low[2]:deep[0], :],
                    dsum[spare, lane, deep[1]:deep[2], :])
            got4 = (r4[parity(end + 1), lane], x4[0, lane], x4[1, lane], x4[2, lane])
            for i in range(nd + 1):
                total = dsum[tail, lane, :low[4], :].astype(F32)
                if i < nd:
                    total = got4[i].astype(F32) + own3[i].astype(F32)
                if i > 0:
                    total = total + early[i - 1, lane]
                emit(lane, end + i, total, 2 + i)
        out_copy(end - 1, parity(end - 1)).wait()
        for i in range(nd + 1):
            out_copy(end + i, 2 + i).start()
        store_weights(3)
        net.end(steps)
        for i in range(nd + 1):
            out_copy(end + i, 2 + i).wait()

    net.begun()
    lax.fori_loop(1, first, loss_step, 0)
    for lane in range(1, nd):
        net.release(first - 1, lane)
    for lane in range(nd):
        for stage_no in range(1, 5):
            rs_copy(stage_no, lane, first - 1).start()
    reps(first - 1)
    softmax()
    lax.fori_loop(first, steps, grad_step, 0)
    flush()
    gb_ref[...] = sum_rows(gb[...])
    stores = []
    for half in PAIR:
        cols = pl.ds(half_at[half], geo.half)
        stores.append(pltpu.make_async_copy(gout.at[half, pl.ds(0, n_q)], gq_hbm.at[:, :, cols], hout_sem.at[half, 0]))
        stores.append(pltpu.make_async_copy(gout.at[half, pl.ds(n_q, n_dp)], gd_hbm.at[:, :, cols],
                                            hout_sem.at[half, 1]))
    for copy in stores:
        copy.start()
    for copy in stores:
        copy.wait()
    for lane in range(nd):
        wout(lane).wait()
        wout_cross(lane).wait()


def call_fused(geo, const, q_rows, d_rows, w_head, bias, mrow, tables, pick):
    bufs, sems = gather_scratch(geo)
    dma = pltpu.SemaphoreType.DMA
    nd, tok, width, vocab, rows = geo.nd, geo.tokens, geo.width, geo.vocab, geo.rows
    n_q, (docs, _), slots, lanes = const[0], pick.shape, 2 * geo.chips, tables.shape[1]
    hq = n_q // 2
    hbm, vmem = pl.BlockSpec(memory_space=pl.ANY), pl.BlockSpec(memory_space=pltpu.VMEM)
    logit = pltpu.VMEM((2, tok, vocab), F32)
    scratch = bufs + [
        pltpu.VMEM((nd, width, 2 * vocab), BF16), pltpu.VMEM((nd, 2 * vocab, width), BF16),
        pltpu.VMEM((nd, 2 * vocab, width), F32), logit, logit, logit,
        pltpu.VMEM((2, tok, 2 * vocab), BF16), pltpu.VMEM((2 * vocab, tok), BF16),
        pltpu.VMEM((3, nd, tok, width), BF16),
        pltpu.VMEM((3, nd, tok // 2, width), BF16), pltpu.VMEM((3, nd, tok // 4, width), BF16),
        pltpu.VMEM((3, nd, tok // 8, width), BF16),
        pltpu.VMEM((2, nd, tok // 2, width), BF16), pltpu.VMEM((2, nd, tok // 4, width), BF16),
        pltpu.VMEM((2, nd, tok // 8, width), BF16), pltpu.VMEM((2, nd, tok // 16, width), BF16),
        pltpu.VMEM((nd, tok // 4, width), BF16), pltpu.VMEM((2, nd, tok // 8, width), BF16),
        pltpu.VMEM((3, nd, tok // 16, width), BF16),
        pltpu.VMEM((nd + 3, geo.unit, geo.half), BF16), pltpu.VMEM((2, rows, geo.unit, geo.half), BF16),
        pltpu.VMEM((nd, nd, geo.slab, width), F32), pltpu.VMEM((nd, geo.slab, width), F32),
        pltpu.VMEM((geo.unit, vocab), F32),
        pltpu.VMEM((slots, rows, vocab), F32), pltpu.VMEM((docs, vocab), F32), pltpu.VMEM((docs, vocab), F32),
        pltpu.VMEM((slots,) + mrow.shape, F32), pltpu.VMEM((mrow.shape[1] // geo.unit, geo.unit, 128), F32),
        pltpu.VMEM((slots, hq, lanes), F32), pltpu.VMEM((slots, hq, lanes), F32),
        pltpu.VMEM((hq, lanes), F32), pltpu.VMEM((slots, hq, lanes), F32),
        pltpu.VMEM((1, lanes), F32), pltpu.VMEM((slots, 1, lanes), F32),
        dma((4,)), dma((nd,)), dma((nd,)), dma((nd,)), dma((2, 2)), dma((2, 2)), dma((2, 2)), dma((2, 2)),
        dma((4, nd, 2)), dma((4, nd, 2)), dma((6, nd)), dma((6, nd)), dma((nd + 3,)), dma((nd + 3,)), dma((nd,)), dma((nd,)),
        dma((nd,)), dma((2, 2)), dma((4, slots)), dma((4, slots))] + sems
    return pl.pallas_call(
        functools.partial(fused_kernel, geo, const),
        name="lexical_head",
        out_shape=[jax.ShapeDtypeStruct((1, lanes), F32), jax.ShapeDtypeStruct(w_head.shape, BF16),
                   jax.ShapeDtypeStruct((1, vocab), F32), jax.ShapeDtypeStruct(q_rows.shape, BF16),
                   jax.ShapeDtypeStruct(d_rows.shape, BF16)],
        in_specs=[hbm, hbm, hbm] + [vmem] * 4,
        out_specs=[vmem, hbm, vmem, hbm, hbm],
        scratch_shapes=scratch,
        compiler_params=pltpu.CompilerParams(collective_id=0, has_side_effects=True, vmem_limit_bytes=VMEM_LIMIT),
    )(q_rows, d_rows, w_head, bias, mrow, tables, pick)


def store_kernel(count, *refs):
    sources, results, holds = refs[:count], refs[count:2 * count], refs[2 * count:3 * count]
    read_sem, write_sem = refs[3 * count:]
    reads, writes = [], []
    for source, result, hold in zip(sources, results, holds):
        for piece in range(hold.shape[0]):
            span = pl.ds(piece * hold.shape[1], hold.shape[1])
            at = len(reads)
            reads.append(pltpu.make_async_copy(source.at[span], hold.at[piece], read_sem.at[at]))
            writes.append(pltpu.make_async_copy(hold.at[piece], result.at[span], write_sem.at[at]))
    for copy in reads:
        copy.start()
    for read, write in zip(reads, writes):
        read.wait()
        write.start()
    for copy in writes:
        copy.wait()


def call_store(geo, *arrays):
    pieces = [max(1, min(geo.chips, x.shape[0] // 2)) for x in arrays]
    holds = [pltpu.VMEM((n, x.shape[0] // n) + x.shape[1:], x.dtype) for n, x in zip(pieces, arrays)]
    hbm = pl.BlockSpec(memory_space=pl.ANY)
    dma = pltpu.SemaphoreType.DMA((sum(pieces),))
    return pl.pallas_call(
        functools.partial(store_kernel, len(arrays)), name="store_results",
        out_shape=[jax.ShapeDtypeStruct(x.shape, x.dtype) for x in arrays],
        in_specs=[hbm] * len(arrays), out_specs=[hbm] * len(arrays), scratch_shapes=holds + [dma, dma],
        compiler_params=pltpu.CompilerParams(vmem_limit_bytes=VMEM_LIMIT),
    )(*arrays)


def solution(mesh):
    n_group = mesh.shape['tp']
    row_spec = P(('dp', 'tp'))
    mask_spec = P(('dp', 'tp'), None)
    hid_spec = P(('dp', 'tp'), None, None)

    def local_step(q_hidden, d_hidden, q_mask, d_mask, positive, w_head, b_head):
        hidden_size, vocab_loc = w_head.shape
        vocab_size = vocab_loc * n_group
        n_q, q_len, _ = q_hidden.shape
        n_d, d_len, _ = d_hidden.shape
        pieces = d_len // q_len
        q_batch, d_batch = n_q * n_group, n_d * n_group
        tau = q_len * math.sqrt(vocab_size * d_len) / 16.0
        lam_q = 4.0 / (vocab_size * q_len * q_len)
        lam_d = 4.0 / (vocab_size * d_len * d_len)
        rows = n_q + n_d * pieces
        geo = Geometry(n_group, rows, hidden_size, vocab_loc, q_len)
        side, slots = geo.side, 2 * geo.chips
        lanes = max(128, 2 * d_batch)

        me = lax.axis_index('tp')
        slot = jnp.arange(slots)
        chip, rel = me // 2, slot // 2
        step_x, step_y = rel % side, rel // side
        chip_of = (((chip // side) ^ step_y ^ (step_y >> 1)) * side + ((chip % side) ^ step_x ^ (step_x >> 1)))
        device_of = chip_of * 2 + slot % 2
        doc_of = jnp.add.outer(jnp.arange(n_d), device_of * n_d).reshape((n_d * slots,))
        tables = jax.nn.one_hot(jnp.concatenate([device_of, doc_of, positive]), lanes, dtype=F32)
        pick = np.concatenate([np.kron(np.eye(slots), np.repeat(row, pieces)) for row in np.eye(n_d)])

        own_mask = jnp.concatenate([q_mask.reshape((-1,)), d_mask.reshape((-1,))]).astype(F32)
        mrow = jnp.pad(own_mask, (0, -own_mask.shape[0] % 128)).reshape((1, -1))
        const = (n_q, n_d, lam_q, lam_d, tau, float(q_batch), float(d_batch))
        loss, grad_w, grad_b, grad_q, grad_d = call_fused(
            geo, const, q_hidden, d_hidden.reshape((n_d * pieces, q_len, hidden_size)), w_head,
            b_head.reshape((1, vocab_loc)), mrow, tables, jnp.asarray(pick, F32))
        loss, grad_w, grad_b, grad_q, grad_d = call_store(geo, loss, grad_w, grad_b, grad_q, grad_d)
        return (loss[0, 0:1], grad_w, grad_b.reshape((vocab_loc,)), grad_q, grad_d.reshape(d_hidden.shape))

    return jax.shard_map(local_step, mesh=mesh,
                         in_specs=(hid_spec, hid_spec, mask_spec, mask_spec, row_spec, P(None, 'tp'), P('tp')),
                         out_specs=(P('dp'), P('dp', 'tp'), row_spec, hid_spec, hid_spec),
                         check_vma=False)
```
